32 devices in a mesh: grp: 4 (over y, x), sp: 8 (over z, core).
Axes of the slice: x: 2, y: 2, z: 4, core: 2. Of those that a mesh axis runs over, the one named last changes fastest.
Arguments:
- layer_input: bfloat16 [8192, 768], P(('grp', 'sp')), may hold values from -6 to 6
- block_order: int32 [4, 16], P('grp'), may hold values from 0 to 15, each once within a row
- ln1_gain: float32 [768], replicated, may hold values from 0.5 to 1.5
- ln1_bias: float32 [768], replicated, may hold values from -1.8 to 1.8
- w_query: bfloat16 [768, 768], replicated, may hold values from -0.4375 to 0.4375
- b_query: float32 [768], replicated, may hold values from -1.8 to 1.8
- w_keyval: bfloat16 [768, 128], replicated, may hold values from -0.21875 to 0.21875
- b_keyval: float32 [128], replicated, may hold values from -1.8 to 1.8
- w_attn_out: bfloat16 [768, 768], replicated, may hold values from -0.875 to 0.875
- b_attn_out: float32 [768], replicated, may hold values from -1.8 to 1.8
- ln2_gain: float32 [768], replicated, may hold values from 0.5 to 1.5
- ln2_bias: float32 [768], replicated, may hold values from -1.8 to 1.8
- w_fc: bfloat16 [768, 3072], replicated, may hold values from -0.21875 to 0.21875
- b_fc: float32 [3072], replicated, may hold values from -1.8 to 1.8
- w_proj: bfloat16 [3072, 768], replicated, may hold values from -0.15625 to 0.15625
- b_proj: float32 [768], replicated, may hold values from -1.8 to 1.8
- kv_grad: bfloat16 [8192, 128], P(('grp', 'sp')), may hold values from -6 to 6
- out_grad: bfloat16 [8192, 768], P(('grp', 'sp')), may hold values from -16 to 16
Outputs:
- layer_out: bfloat16 [8192, 768], P(('grp', 'sp'))
- input_grad: float32 [8192, 768], P(('grp', 'sp'))
- ln1_gain_grad: float32 [768], replicated
- ln1_bias_grad: float32 [768], replicated
- w_query_grad: float32 [768, 768], P('sp')
- b_query_grad: float32 [768], replicated
- w_keyval_grad: float32 [768, 128], P('sp')
- b_keyval_grad: float32 [128], replicated
- w_attn_out_grad: float32 [768, 768], P('sp')
- b_attn_out_grad: float32 [768], replicated
- ln2_gain_grad: float32 [768], replicated
- ln2_bias_grad: float32 [768], replicated
- w_fc_grad: float32 [768, 3072], P('sp')
- b_fc_grad: float32 [3072], replicated
- w_proj_grad: float32 [3072, 768], P('sp')
- b_proj_grad: float32 [768], replicated
The draws below stay inside these ranges and needn't reach their ends.
Inputs may be any that keep to these rules, and one draw needn't show every extreme that they name: `block_order`: each row names each of the 16 blocks of its sequence exactly once.
All inputs are finite; a program needn't handle non-finite values.
Results may differ from the reference program's by a relative error of at most 0.012.
The reference program's roundings to bfloat16 on the way count: a program that leaves them out, or rounds other values in their place, can miss the bound.
Values may be sent and summed in bfloat16 or wider, within the bound.
A program may use at most 128 MiB of HBM per device.

```python
import math
import jax
import jax.numpy as jnp
from jax import lax

D = 768
H = 12
HD = 64
ROT = 16
FF = 3072
SEQ_SHARD = 256
SEQS_G = 1
SEQ_LEN = 2048
BLOCK = 128
NBLK = 16
SEQS = 4
TOKENS = 8192
N_GRP = 4
N_SP = 8


def draw_out_grad(key, part):
    rows_rise = jnp.arange(TOKENS, dtype=jnp.float32)[:, None] / (TOKENS - 1)
    values = jax.random.truncated_normal(key, -4.0, 4.0, (TOKENS, D), jnp.float32)
    row_scale = 1.0 + 2.0 * rows_rise
    return (values * row_scale).astype(jnp.bfloat16)


def block_levels(own_key, extent, cuts, smallest, top_value):
    factor_of = 1.0
    for axis_at, shards_of in cuts:
        steps = jax.random.uniform(jax.random.fold_in(jax.random.fold_in(own_key, 6), axis_at), (shards_of,), jnp.float32, smallest / len(cuts), top_value / len(cuts))
        factor_of = factor_of * jnp.repeat(jnp.exp(steps), extent[axis_at] // shards_of).reshape((-1,) + (1,) * (len(extent) - 1 - axis_at))
    return factor_of


def normal_values(rng, extent, width, reach, pieces=(), kind=jnp.bfloat16):
    loudness = block_levels(rng, extent, pieces, -0.22, 0.18) if pieces else 1.0
    values = jax.random.normal(rng, extent, jnp.float32) * width * loudness
    return jnp.minimum(jnp.maximum(values, -reach), reach).astype(kind)


def setup_inputs(seed: int = 0) -> dict:
    keys = jax.random.split(jax.random.key(seed), 19)
    return {
        "layer_input": normal_values(keys[0], (TOKENS, D), 1.0, 6.0, ((0, 32),)),
        "block_order": jax.vmap(lambda own: jax.random.permutation(own, NBLK))(jax.random.split(keys[1], SEQS)).reshape((SEQS, NBLK)).astype(jnp.int32),
        "ln1_gain": jnp.clip(1.0 + 0.1 * jax.random.normal(keys[2], (D,), jnp.float32), 0.5, 1.5),
        "ln1_bias": normal_values(keys[3], (D,), 0.3, 1.8, (), jnp.float32),
        "w_query": normal_values(keys[4], (D, D), (D // 4) ** -0.5, 0.4375),
        "b_query": normal_values(keys[5], (D,), 0.3, 1.8, (), jnp.float32),
        "w_keyval": normal_values(keys[6], (D, 2 * HD), D ** -0.5, 0.21875),
        "b_keyval": normal_values(keys[7], (2 * HD,), 0.3, 1.8, (), jnp.float32),
        "w_attn_out": normal_values(keys[8], (D, D), (D // 16) ** -0.5, 0.875),
        "b_attn_out": normal_values(keys[9], (D,), 0.3, 1.8, (), jnp.float32),
        "ln2_gain": jnp.clip(1.0 + 0.1 * jax.random.normal(keys[10], (D,), jnp.float32), 0.5, 1.5),
        "ln2_bias": normal_values(keys[11], (D,), 0.3, 1.8, (), jnp.float32),
        "w_fc": normal_values(keys[12], (D, FF), D ** -0.5, 0.21875),
        "b_fc": normal_values(keys[13], (FF,), 0.3, 1.8, (), jnp.float32),
        "w_proj": normal_values(keys[14], (FF, D), (FF // 2) ** -0.5, 0.15625),
        "b_proj": normal_values(keys[15], (D,), 0.3, 1.8, (), jnp.float32),
        "kv_grad": normal_values(keys[16], (TOKENS, 2 * HD), 1.0, 6.0, ((0, 32),)),
        "out_grad": draw_out_grad(jax.random.fold_in(keys[18], 71), 0),
    }


@jax.custom_vjp
def low(v):
    return lax.optimization_barrier(v.astype(jnp.bfloat16)).astype(jnp.float32)

@jax.custom_vjp
def low_back(v):
    return v

def low_keep(v):
    return (low(v), None)

def low_pass(kept, grad):
    return (grad,)

def back_keep(v):
    return (v, None)

def back_low(kept, grad):
    return (low(grad),)
low.defvjp(low_keep, low_pass)
low_back.defvjp(back_keep, back_low)
norm_eps = 1e-05
half_root = 0.7071067811865476
masked_score = -1e+30
rotary_base_log = math.log(10000.0)

def matmul(left_side, right_side):
    return jnp.dot(left_side, right_side, precision=lax.Precision.HIGHEST, preferred_element_type=jnp.float32)

def layer_norm(values, gain_row, shift_row):
    centre = lax.optimization_barrier(jnp.mean(values, axis=-1, keepdims=True))
    centred = values - centre
    spread = lax.optimization_barrier(jnp.mean(centred * centred, axis=-1, keepdims=True))
    return centred * lax.rsqrt(spread + norm_eps) * gain_row + shift_row

def rotary_tables(position):
    half_rot = ROT // 2
    frequency = jnp.exp(jnp.arange(half_rot, dtype=jnp.float32) * (-2.0 * rotary_base_log / ROT))
    angles = position.astype(jnp.float32)[:, None] * 0.25 * frequency[None, :]
    return (jnp.cos(angles), jnp.sin(angles))

def rotate(values, cosine, sine_table):
    half_rot = ROT // 2
    cos_rows = cosine[:, None, :]
    sin_rows = sine_table[:, None, :]
    lower_half = values[..., :half_rot]
    upper_half = values[..., half_rot:ROT]
    return jnp.concatenate([lower_half * cos_rows - upper_half * sin_rows, upper_half * cos_rows + lower_half * sin_rows, values[..., ROT:]], axis=-1)

def attention(query_use, keyval_use, position):
    key_use = keyval_use[:, :HD]
    value_use = keyval_use[:, HD:]
    allowed = position[None, :] <= position[:, None]

    def one_head(query_head):
        scores = low_back(matmul(query_head, key_use.T) * 0.125)
        scores = jnp.where(allowed, scores, masked_score)
        weights = low(jax.nn.softmax(scores, axis=-1))
        return matmul(weights, value_use)
    per_head = lax.map(jax.checkpoint(one_head), jnp.transpose(query_use, (1, 0, 2)))
    return jnp.transpose(per_head, (1, 0, 2)).reshape(query_use.shape[0], H * HD)

def layer(params, layer_in, position):
    ln1_gain, ln1_bias, w_query, b_query, w_keyval, b_keyval, w_attn_out, b_attn_out, ln2_gain, ln2_bias, w_fc, b_fc, w_proj, b_proj = params
    length = layer_in.shape[0]
    cosine, sine_table = rotary_tables(position)
    first_in = low(layer_norm(layer_in, ln1_gain, ln1_bias))
    query_pre = low_back(matmul(first_in, w_query) + b_query)
    keyval_pre = low_back(matmul(first_in, w_keyval) + b_keyval)
    query_use = low(rotate(query_pre.reshape(length, H, HD), cosine, sine_table))
    key_rot = rotate(keyval_pre[:, None, :HD], cosine, sine_table)[:, 0, :]
    keyval_use = low(jnp.concatenate([key_rot, keyval_pre[:, HD:]], axis=1))
    heads = low(low_back(attention(query_use, keyval_use, position)))
    attn_branch = matmul(heads, w_attn_out) + b_attn_out
    second_in = low(layer_norm(layer_in, ln2_gain, ln2_bias))
    hidden = low_back(matmul(second_in, w_fc) + b_fc)
    activated = low(0.5 * hidden * (1.0 + lax.erf(hidden * half_root)))
    mlp_branch = matmul(activated, w_proj) + b_proj
    return (layer_in + attn_branch + mlp_branch, keyval_use)

def by_sequence(array):
    return array.reshape(N_GRP, N_SP, SEQS_G, SEQ_SHARD, -1).transpose(0, 2, 1, 3, 4).reshape(SEQS, SEQ_LEN, -1)

def to_stored(array):
    return array.reshape(N_GRP, SEQS_G, N_SP, SEQ_SHARD, -1).transpose(0, 2, 1, 3, 4).reshape(TOKENS, -1)

def reference(layer_input, block_order, ln1_gain, ln1_bias, w_query, b_query, w_keyval, b_keyval, w_attn_out, b_attn_out, ln2_gain, ln2_bias, w_fc, b_fc, w_proj, b_proj, kv_grad, out_grad):
    params = (ln1_gain, ln1_bias, w_query.astype(jnp.float32), b_query, w_keyval.astype(jnp.float32), b_keyval, w_attn_out.astype(jnp.float32), b_attn_out, ln2_gain, ln2_bias, w_fc.astype(jnp.float32), b_fc, w_proj.astype(jnp.float32), b_proj)
    offsets = jnp.arange(BLOCK, dtype=jnp.int32)
    positions = (block_order[:, :, None] * BLOCK + offsets[None, None, :]).reshape(SEQS, SEQ_LEN).astype(jnp.int32)
    inputs_all = (by_sequence(layer_input.astype(jnp.float32)), positions, by_sequence(kv_grad.astype(jnp.float32)), by_sequence(out_grad.astype(jnp.float32)))

    def one_sequence(totals, inputs):
        layer_in, position, keyval_cot, out_cot = inputs

        def apply_layer(weights_all, values_in):
            return layer(weights_all, values_in, position)
        (layer_out, shared_kv), pull_back = jax.vjp(apply_layer, params, layer_in)
        param_grads, input_grad = pull_back((out_cot, keyval_cot))
        totals = jax.tree.map(lambda held_sum, fresh_grad: held_sum + fresh_grad, totals, param_grads)
        return (totals, (layer_out, input_grad))
    start_totals = jax.tree.map(jnp.zeros_like, params)
    totals, (outs_all, grads_all) = lax.scan(one_sequence, start_totals, inputs_all)
    layer_out = to_stored(outs_all).astype(jnp.bfloat16)
    input_grad = to_stored(grads_all)
    return (layer_out, input_grad, totals[0], totals[1], totals[2], totals[3], totals[4], totals[5], totals[6], totals[7], totals[8], totals[9], totals[10], totals[11], totals[12], totals[13])
```

```python
import functools
import math

import jax
import jax.numpy as jnp
from jax import lax
from jax.experimental import pallas as pl
from jax.experimental.pallas import tpu as pltpu
from jax.sharding import PartitionSpec as P

H = 12
HD = 64
ROT = 16
MESH = pl.DeviceIdType.MESH
F32 = jnp.float32
BF16 = jnp.bfloat16
NN = (((1,), (0,)), ((), ()))
NT = (((1,), (1,)), ((), ()))
TN = (((0,), (0,)), ((), ()))


def mm(a, b, dims=NN):
    return lax.dot_general(a, b, dims, preferred_element_type=F32)

norm_eps = 1e-05
half_root = 0.7071067811865476
inv_root_tau = 0.3989422804014327
masked_score = -1e30
rotary_base_log = math.log(10000.0)
score_block = 512


def vec_rows(width, ff, pair):
    names = ("ln1_gain", "ln1_bias", "b_query", "b_keyval", "column", "ln2_gain", "ln2_bias", "b_fc")
    sizes = (width, width, width, pair, width, width, width, ff)
    at, rows = 0, {}
    for name, size in zip(names, sizes):
        rows[name] = (at, size // 128)
        at += size // 128
    return rows, at


def fused_kernel(
    dims,
    x_h,
    order_s,
    g1_h,
    b1_h,
    wq_h,
    bq_h,
    wkv_h,
    bkv_h,
    wo_h,
    bo_h,
    g2_h,
    b2_h,
    wfc_h,
    bfc_h,
    wpr_h,
    bpr_h,
    kvg_h,
    og_h,
    o_wp,
    o_wf,
    o_wo,
    o_wq,
    o_wkv,
    o_vec,
    o_lo,
    o_ig,
    vecs,
    bkv_v,
    bfc_v,
    x2,
    og2,
    fi2,
    si2,
    fit,
    sit,
    nrm,
    inv,
    wkv_v,
    wq_v,
    wo_v,
    wfc_v,
    wpr_v,
    kvg_v,
    act_s,
    hg_s,
    mlp_all,
    sec_all,
    mlp_r,
    sec_r,
    wp_part,
    rx_wp,
    wp_s1,
    ry_wp,
    zs_wp,
    rz_wp,
    fin_wp,
    wf_part,
    ry_wf,
    wf_s1,
    wf_own,
    rx_wf,
    zs_wf,
    rz_wf,
    fin_wf,
    kv_all,
    kvt,
    qo,
    bias,
    sbuf,
    dbuf,
    dsp,
    dkv,
    dkv_b,
    rdkv,
    oht,
    qgt,
    ht_r,
    qg2,
    wo_part,
    rx_wo,
    wo_s1,
    ry_wo,
    zs_wo,
    rz_wo,
    fin_wo,
    wq_part,
    ry_wq,
    wq_s1,
    rx_wq,
    zs_wq,
    rz_wq,
    fin_wq,
    vec,
    rvec,
    wkv_part,
    wkv_b,
    rkv,
    sm,
    fin_kv,
    fin_vec,
    lo_v,
    ig_v,
    ctab,
    stab,
    cost,
    sint,
    lsem,
    ssem,
    rsem,
):
    T, D, F, S, NSP, NG = dims
    NZ = NSP // 2
    Q = F // NSP
    R = D // NSP
    C2 = D // 2
    pair = 2 * HD
    g = lax.axis_index("grp")
    d = lax.axis_index("sp")
    c = lax.rem(d, 2)
    z = lax.div(d, 2)
    xx = lax.rem(g, 2)
    yy = lax.div(g, 2)
    partner = (g, d + 1 - 2 * c)
    xnb = (g + 1 - 2 * xx, d)
    ynb = (g + 2 - 4 * yy, d)

    def sp_peer(o):
        return (g, lax.rem(d + o, NSP))

    def z_peer(o):
        return (g, 2 * lax.rem(z + o, NZ) + c)

    def xy_peer(o, core):
        return (lax.rem(g + o, NG), 2 * z + core)

    base = {}
    used = [0]

    def take(name, n):
        base[name] = used[0]
        used[0] += n

    for name, n in (
        ("x", 1), ("og", 1), ("kv", NSP), ("mlp", 1), ("sec", 1),
        ("wpx", NZ), ("wpy", NZ), ("wpz", NZ), ("wpg", NG),
        ("wfy", 2), ("wfx", 1), ("wfz", NZ), ("wfg", 2 * NG),
        ("ht", NZ), ("qg", 1), ("dkv", NSP),
        ("wox", 1), ("woy", 1), ("woz", NZ), ("wog", NG),
        ("wqy", 1), ("wqx", 1), ("wqz", NZ), ("wqg", NG),
        ("wkv", NSP), ("vec", NSP), ("sm", NG), ("vg", NSP),
    ):
        take(name, n)

    def rc(name, i, src, dst, to):
        k = base[name] + i
        return pltpu.make_async_remote_copy(
            src_ref=src,
            dst_ref=dst,
            send_sem=ssem.at[k],
            recv_sem=rsem.at[k],
            device_id=to,
            device_id_type=MESH,
        )

    started = []

    def send(copy):
        copy.start()
        started.append(copy)

    lused = [0]

    def lc(src, dst):
        copy = pltpu.make_async_copy(src, dst, lsem.at[lused[0]])
        lused[0] += 1
        copy.start()
        return copy

    def chunk_of(j):
        far_y = lax.div(j, 2) == 0
        far_x = lax.rem(j, 2) == 0
        return 2 * jnp.where(far_y, 1 - yy, yy) + jnp.where(far_x, 1 - xx, xx)

    def chunk_in(j):
        far_y = lax.div(j, 2) == 0
        far_x = lax.rem(j, 2) == 0
        return 2 * jnp.where(far_y, 1 - yy, yy) + jnp.where(far_x, xx, 1 - xx)

    own = pl.ds(0, T)
    other = pl.ds(T, T)
    l_x = lc(x_h, x2.at[own])
    l_og = lc(og_h, og2.at[own])
    l_wkv = lc(wkv_h, wkv_v)
    l_vec = [
        lc(src, vecs.at[i]) for i, src in enumerate((g1_h, b1_h, g2_h, b2_h, bq_h, bo_h, bpr_h))
    ]
    l_bkv = lc(bkv_h, bkv_v.at[0])
    l_bfc = lc(bfc_h, bfc_v.at[0])
    l_mlp = []
    for j in range(NZ):
        q = chunk_of(j)
        cols = pl.ds(pl.multiple_of(Q * (2 * q + c), 128), Q)
        rows = pl.ds(pl.multiple_of(Q * (2 * q + c), 16), Q)
        l_mlp.append((lc(wfc_h.at[:, cols], wfc_v.at[q]), lc(wpr_h.at[rows, :], wpr_v.at[q])))
    l_wq = lc(wq_h, wq_v)
    l_wo = lc(wo_h, wo_v)
    l_kvg = lc(kvg_h, kvg_v)

    barrier = pltpu.get_barrier_semaphore()
    for o in range(1, NSP):
        pl.semaphore_signal(barrier, inc=1, device_id=sp_peer(o), device_id_type=MESH)
    for o in range(1, NG):
        for core in range(2):
            pl.semaphore_signal(barrier, inc=1, device_id=xy_peer(o, core), device_id_type=MESH)
    pl.semaphore_wait(barrier, NSP - 1 + 2 * (NG - 1))

    s_x = rc("x", 0, x_h, x2.at[other], partner)
    send(s_x)
    s_og = rc("og", 0, og_h, og2.at[other], partner)
    send(s_og)

    lane = lax.broadcasted_iota(jnp.int32, (8, T), 1)
    half = lax.broadcasted_iota(jnp.int32, (8, T), 0).astype(F32)
    block = T // 2
    first_block = order_s[0, 2 * d]
    second_block = order_s[0, 2 * d + 1]
    own_pos = jnp.where(
        lane < block, first_block * block + lane, second_block * block + (lane - block)
    )
    frequency = jnp.exp(half * (-2.0 * rotary_base_log / ROT))
    angle = own_pos.astype(F32) * 0.25 * frequency
    cosine, sine = jnp.cos(angle), jnp.sin(angle)
    cost[...] = cosine
    sint[...] = sine
    ones = jnp.ones((HD - ROT, T), F32)
    zeros = jnp.zeros((HD - ROT, T), F32)
    ctab[...] = jnp.concatenate([cosine, cosine, ones] * 2, axis=0).T
    stab[...] = jnp.concatenate([-sine, sine, zeros] * 2, axis=0).T
    lanes = lax.broadcasted_iota(jnp.int32, (128, pair), 1)
    low_half = lax.rem(lanes, HD) < ROT // 2

    def turn(tile, rows, sign):
        mixed = jnp.where(low_half, pltpu.roll(tile, pair - ROT // 2, 1), pltpu.roll(tile, ROT // 2, 1))
        return tile * ctab[rows, :] + (sign * mixed) * stab[rows, :]

    for copy in l_vec:
        copy.wait()
    l_bkv.wait()
    l_bfc.wait()
    g1, b1, g2, b2 = (vecs[i : i + 1, :] for i in range(4))
    vec[...] = jnp.zeros_like(vec)

    def norms(at, keep):
        for i in range(T // 128):
            rows = pl.ds(at + 128 * i, 128)
            v = x2[rows, :].astype(F32)
            centred = v - jnp.mean(v, axis=-1, keepdims=True)
            r = lax.rsqrt(jnp.mean(centred * centred, axis=-1, keepdims=True) + norm_eps)
            n = centred * r
            first = (n * g1 + b1).astype(BF16)
            second = (n * g2 + b2).astype(BF16)
            fi2[rows, :] = first
            si2[rows, :] = second
            fit[:, rows] = first.T
            sit[:, rows] = second.T
            if keep:
                nrm[rows, :] = n
                inv[rows, :] = jnp.broadcast_to(r, (128, 128))

    l_x.wait()
    norms(0, True)

    l_wkv.wait()
    for i in range(T // 128):
        rows = pl.ds(128 * i, 128)
        kv = mm(fi2[rows, :], wkv_v[...]) + bkv_v[...]
        kv = jnp.where(lanes < HD, turn(kv, rows, 1.0), kv)
        kv_all[pl.ds(pl.multiple_of(d * T + 128 * i, 128), 128), :] = kv.astype(BF16)
    mine = pl.ds(pl.multiple_of(d * T, T), T)
    s_kv = [rc("kv", o, kv_all.at[mine], kv_all.at[mine], sp_peer(o)) for o in range(1, NSP)]
    for copy in s_kv:
        send(copy)

    s_x.wait_recv()
    norms(T, False)
    l_og.wait()
    s_og.wait_recv()

    rows_v, _ = vec_rows(D, F, pair)
    for pair_of_copies in l_mlp:
        for copy in pair_of_copies:
            copy.wait()

    def x_half(q):
        far = pl.ds(pl.multiple_of(Q // 2 * (1 - xx), 16), Q // 2)
        return rc("wpx", q, wp_part.at[q, far, :], rx_wp.at[q], xnb)

    def y_chunk(q):
        side = lax.rem(q, 2)
        return rc("wfy", side, wf_part.at[q], ry_wf.at[side], ynb)

    def mlp_chunk(j, carry):
        q = chunk_of(j)
        at = pl.ds(pl.multiple_of(Q * (2 * q + c), 128), Q)
        shift = bfc_v[:, at]
        total = jnp.zeros((1, Q), F32)
        for i in range(2 * T // 128):
            rows = pl.ds(128 * i, 128)
            hidden = mm(si2[rows, :], wfc_v[q]) + shift
            erf_part = 1.0 + lax.erf(hidden * half_root)
            act_s[q, rows, :] = (0.5 * hidden * erf_part).astype(BF16)
            slope = 0.5 * erf_part + hidden * jnp.exp(-0.5 * hidden * hidden) * inv_root_tau
            act_grad = mm(og2[rows, :], wpr_v[q], NT)
            hidden_grad = (act_grad * slope).astype(BF16)
            hg_s[q, rows, :] = hidden_grad
            total = total + jnp.sum(hidden_grad.astype(F32), axis=0, keepdims=True)
        for i in range(Q // 128):
            cols = pl.ds(128 * i, 128)
            wp_part[q, cols, :] = mm(act_s[q, :, cols], og2[...], TN).astype(BF16)
        x_half(q).start()
        for i in range(D // 128):
            rows = pl.ds(128 * i, 128)
            wf_part[q, rows, :] = mm(sit[rows, :], hg_s[q]).astype(BF16)

        @pl.when(j < 2)
        def _():
            y_chunk(q).start()

        at_row = rows_v["b_fc"][0] + Q // 128 * (2 * q + c)
        for i in range(Q // 128):
            vec[pl.ds(at_row + i, 1), :] = total[:, 128 * i : 128 * (i + 1)]
        return carry

    lax.fori_loop(0, NZ, mlp_chunk, 0)

    def mlp_sums(i, carry):
        at = lax.rem(i + T // 128, 2 * T // 128) * 128
        rows = pl.ds(pl.multiple_of(at, 128), 128)
        out = mm(act_s[0, rows, :], wpr_v[0])
        back = mm(hg_s[0, rows, :], wfc_v[0], NT)
        for q in range(1, NZ):
            out = out + mm(act_s[q, rows, :], wpr_v[q])
            back = back + mm(hg_s[q, rows, :], wfc_v[q], NT)
        mlp_all[rows, :] = out
        sec_all[rows, :] = back
        return carry

    lax.fori_loop(0, 2 * T // 128, mlp_sums, 0)
    s_mlp = rc("mlp", 0, mlp_all.at[other], mlp_r, partner)
    send(s_mlp)
    s_sec = rc("sec", 0, sec_all.at[other], sec_r, partner)
    send(s_sec)

    l_wq.wait()
    l_wo.wait()
    for i in range(T // 128):
        rows = pl.ds(128 * i, 128)
        query = mm(fi2[rows, :], wq_v[...]) + vecs[4:5, :]
        grads = mm(og2[rows, :], wo_v[...], NT)
        for t in range(D // pair):
            q_tile = turn(query[:, pair * t : pair * (t + 1)], rows, 1.0).astype(BF16).astype(F32) * 0.125
            o_tile = grads[:, pair * t : pair * (t + 1)]
            low = lanes < HD
            qo[2 * t, rows, :] = jnp.where(low, q_tile, 0.0).astype(BF16)
            qo[2 * t + 1, rows, :] = jnp.where(low, pltpu.roll(q_tile, HD, 1), 0.0).astype(BF16)
            late = pl.ds(T + 128 * i, 128)
            qo[2 * t, late, :] = jnp.where(low, 0.0, pltpu.roll(o_tile, HD, 1)).astype(BF16)
            qo[2 * t + 1, late, :] = jnp.where(low, 0.0, o_tile).astype(BF16)

    row_in = lax.broadcasted_iota(jnp.int32, (block, T), 0)
    query_pos = jnp.broadcast_to(own_pos[0:1, :], (block, T))
    for j in range(S // block):
        key_pos = order_s[0, j] * block + row_in
        bias[pl.ds(block * j, block), :] = jnp.where(key_pos <= query_pos, 0.0, masked_score)

    for copy in s_kv:
        copy.wait_recv()
    for j in range(S // 256):
        rows = pl.ds(256 * j, 256)
        kvt[:, rows] = kv_all[rows, :].T
        dkv[rows, :] = jnp.zeros((256, pair), F32)

    near_x = pl.ds(pl.multiple_of(Q // 2 * xx, 16), Q // 2)
    near_y = pl.ds(pl.multiple_of(Q // 4 * yy, 16), Q // 4)
    far_y = pl.ds(pl.multiple_of(Q // 4 * (1 - yy), 16), Q // 4)

    def wp_y(q):
        return rc("wpy", q, wp_s1.at[q, far_y, :], ry_wp.at[q], ynb)

    def wp_first(j):
        q = chunk_in(j)
        x_half(q).wait_recv()
        wp_s1[q] = (wp_part[q, near_x, :].astype(F32) + rx_wp[q].astype(F32)).astype(BF16)
        wp_y(q).start()

    def wp_z(o):
        return rc("wpz", o, zs_wp.at[lax.rem(z + o, NZ)], rz_wp.at[o], z_peer(o))

    def wp_second():
        for q in range(NZ):
            wp_y(q).wait_recv()
            zs_wp[q] = (wp_s1[q, near_y, :].astype(F32) + ry_wp[q].astype(F32)).astype(BF16)
        for o in range(1, NZ):
            wp_z(o).start()

    slot_wp = 2 * xx + yy

    def wp_g(o):
        return rc("wpg", o, fin_wp, o_wp.at[slot_wp], xy_peer(o, c))

    l_fin = []

    def wp_third():
        total = zs_wp[z].astype(F32)
        for o in range(1, NZ):
            wp_z(o).wait_recv()
            total = total + rz_wp[o].astype(F32)
        fin_wp[...] = total.astype(BF16)
        for o in range(1, NG):
            wp_g(o).start()
        l_fin.append(lc(fin_wp, o_wp.at[slot_wp]))

    wf_x = rc("wfx", 0, wf_s1, rx_wf, xnb)

    def wf_first():
        q = 2 * yy + 1 - xx
        y_chunk(2 * (1 - yy) + 1 - xx).wait_recv()
        wf_s1[...] = (wf_part[q].astype(F32) + ry_wf[1 - xx].astype(F32)).astype(BF16)
        wf_x.start()

    def wf_second():
        q = 2 * yy + xx
        y_chunk(2 * (1 - yy) + xx).wait_recv()
        wf_own[...] = (wf_part[q].astype(F32) + ry_wf[xx].astype(F32)).astype(BF16)

    def wf_z(o):
        rows = pl.ds(pl.multiple_of(2 * R * lax.rem(z + o, NZ), 16), 2 * R)
        return rc("wfz", o, zs_wf.at[rows, :], rz_wf.at[o], z_peer(o))

    def wf_third():
        wf_x.wait_recv()
        zs_wf[...] = (wf_own[...].astype(F32) + rx_wf[...].astype(F32)).astype(BF16)
        for o in range(1, NZ):
            wf_z(o).start()

    slot_wf = 2 * yy + xx

    def wf_g(o, core):
        to = c + core - 2 * c * core
        rows = pl.ds(pl.multiple_of(R * to, 16), R)
        return rc("wfg", 2 * o + core, fin_wf.at[rows, :], o_wf.at[slot_wf, c], xy_peer(o, to))

    def wf_fourth():
        total = zs_wf[pl.ds(pl.multiple_of(2 * R * z, 16), 2 * R), :].astype(F32)
        for o in range(1, NZ):
            wf_z(o).wait_recv()
            total = total + rz_wf[o].astype(F32)
        fin_wf[...] = total.astype(BF16)
        for o in range(NG):
            for core in range(2):
                if o or core:
                    wf_g(o, core).start()
        l_fin.append(lc(fin_wf.at[pl.ds(pl.multiple_of(R * c, 16), R), :], o_wf.at[slot_wf, c]))

    def at_head(h):
        for when, what in EVENTS:
            pl.when(h == when)(functools.partial(run_event, what))

    def run_event(what):
        {
            "wp0": lambda: wp_first(0),
            "wp1": lambda: wp_first(1),
            "wp2": lambda: wp_first(2),
            "wp3": lambda: wp_first(3),
            "wp_second": wp_second,
            "wf_first": wf_first,
            "wf_second": wf_second,
            "wf_third": wf_third,
        }[what]()

    KC = 256

    def head(h, carry):
        at_head(h)
        both = qo[h]
        top = jnp.full((8, T), -3e38, F32)
        for k in range(S // KC):
            rows = pl.ds(KC * k, KC)
            sd = mm(kv_all[rows, :], both, NT)
            score = sd[:, :T] + bias[rows, :]
            sbuf[rows, :] = score
            dbuf[rows, :] = sd[:, T:]
            top = jnp.maximum(top, jnp.max(score.reshape(KC // 8, 8, T), axis=0))
        top = jnp.max(top, axis=0, keepdims=True)
        norm = jnp.zeros((8, T), F32)
        delta = jnp.zeros((8, T), F32)
        for k in range(S // KC):
            rows = pl.ds(KC * k, KC)
            e = jnp.exp(sbuf[rows, :] - top)
            sbuf[rows, :] = e
            norm = norm + jnp.sum(e.reshape(KC // 8, 8, T), axis=0)
            delta = delta + jnp.sum((e * dbuf[rows, :]).reshape(KC // 8, 8, T), axis=0)
        scale = 1.0 / jnp.sum(norm, axis=0, keepdims=True)
        delta = jnp.sum(delta, axis=0, keepdims=True) * scale
        for k in range(S // KC):
            rows = pl.ds(KC * k, KC)
            p = sbuf[rows, :] * scale
            dsp[rows, :T] = (p * (dbuf[rows, :] - delta)).astype(BF16)
            dsp[rows, T:] = p.astype(BF16)
        for k in range(S // KC):
            rows = pl.ds(KC * k, KC)
            dkv[rows, :] += mm(dsp[rows, :], both)
        result = mm(kvt[...], dsp[...])
        rows = pl.ds(pl.multiple_of(HD * h, HD), HD)
        oht[rows, :] = result[HD:, T:].astype(BF16)
        back = result[:HD, :T] * 0.125
        a, b, rest = back[: ROT // 2], back[ROT // 2 : ROT], back[ROT:]
        ct, st = cost[...], sint[...]
        qgt[rows, :] = jnp.concatenate([a * ct + b * st, b * ct - a * st, rest], axis=0).astype(BF16)
        return carry

    lax.fori_loop(0, H, head, 0)

    dkv_b[...] = dkv[...].astype(BF16)
    s_dkv = []
    for o in range(1, NSP):
        rows = pl.ds(pl.multiple_of(lax.rem(d + o, NSP) * T, T), T)
        s_dkv.append(rc("dkv", o, dkv_b.at[rows, :], rdkv.at[o], sp_peer(o)))
        send(s_dkv[-1])

    s_ht = []
    for k in range(NZ):
        rows = pl.ds(pl.multiple_of(2 * R * k + R * (1 - c), 16), R)
        s_ht.append(rc("ht", k, oht.at[rows, :], ht_r.at[k], partner))
        send(s_ht[-1])
    qg2[own, :] = qgt[...].T
    s_qg = rc("qg", 0, qg2.at[own], qg2.at[other], partner)
    send(s_qg)

    wf_fourth()
    wp_third()

    def put(name, row):
        at, count = rows_v[name]
        for i in range(count):
            vec[at + i : at + i + 1, :] = row[:, 128 * i : 128 * (i + 1)]

    s_mlp.wait_recv()
    for i in range(T // 128):
        rows = pl.ds(128 * i, 128)
        branch = mm(oht[:, rows], wo_v[...], TN) + vecs[5:6, :]
        mlp = (mlp_all[rows, :] + mlp_r[rows, :]) + vecs[6:7, :]
        lo_v[rows, :] = ((x2[rows, :].astype(F32) + branch) + mlp).astype(BF16)
    l_lo = lc(lo_v, o_lo)

    for copy in s_ht:
        copy.wait_recv()
    for k in range(NZ):
        rows = pl.ds(pl.multiple_of(2 * R * k + R * c, 16), R)
        wo_part[k] = (mm(oht[rows, :], og2[own, :]) + mm(ht_r[k], og2[other, :])).astype(BF16)
    far_rx = pl.ds(pl.multiple_of(R // 2 * (1 - xx), 16), R // 2)
    far_ry = pl.ds(pl.multiple_of(R // 2 * (1 - yy), 16), R // 2)
    near_rx = pl.ds(pl.multiple_of(R // 2 * xx, 16), R // 2)
    near_ry = pl.ds(pl.multiple_of(R // 2 * yy, 16), R // 2)
    far_cx = pl.ds(pl.multiple_of(C2 * (1 - xx), 128), C2)
    far_cy = pl.ds(pl.multiple_of(C2 * (1 - yy), 128), C2)
    near_cx = pl.ds(pl.multiple_of(C2 * xx, 128), C2)
    near_cy = pl.ds(pl.multiple_of(C2 * yy, 128), C2)
    s_wox = rc("wox", 0, wo_part.at[:, far_rx, :], rx_wo, xnb)
    send(s_wox)
    s_qg.wait_recv()
    for k in range(NZ):
        rows = pl.ds(pl.multiple_of(2 * R * k + R * c, 16), R)
        wq_part[k] = mm(fit[rows, :], qg2[...]).astype(BF16)
    s_wqy = rc("wqy", 0, wq_part.at[:, far_ry, :], ry_wq, ynb)
    send(s_wqy)

    l_kvg.wait()
    for copy in s_dkv:
        copy.wait_recv()
    kv_grads = []
    for i in range(T // 128):
        rows = pl.ds(128 * i, 128)
        total = dkv[pl.ds(pl.multiple_of(d * T + 128 * i, 128), 128), :]
        for o in range(1, NSP):
            total = total + rdkv[o, rows, :].astype(F32)
        total = total + kvg_v[rows, :].astype(F32)
        kv_grads.append(jnp.where(lanes < HD, turn(total, rows, -1.0), total).astype(BF16))
    kv_grad = jnp.concatenate(kv_grads, axis=0)
    put("b_keyval", jnp.sum(kv_grad.astype(F32), axis=0, keepdims=True))
    wkv_part[...] = mm(fit[:, own], kv_grad)
    wkv_b[...] = wkv_part[...].astype(BF16)
    s_wkv = []
    for o in range(1, NSP):
        rows = pl.ds(pl.multiple_of(lax.rem(d + o, NSP) * R, 16), R)
        s_wkv.append(rc("wkv", o, wkv_b.at[rows, :], rkv.at[o], sp_peer(o)))
        send(s_wkv[-1])

    s_sec.wait_recv()
    sums = [jnp.zeros((1, D), F32) for _ in range(6)]
    for i in range(T // 128):
        rows = pl.ds(128 * i, 128)
        first_grad = mm(qg2[rows, :], wq_v[...], NT) + mm(kv_grads[i], wkv_v[...], NT)
        second_grad = sec_all[rows, :] + sec_r[rows, :]
        n = nrm[rows, :]
        up = og2[rows, :].astype(F32)
        u = first_grad * g1 + second_grad * g2
        back = u - jnp.mean(u, axis=-1, keepdims=True) - n * jnp.mean(u * n, axis=-1, keepdims=True)
        ig_v[rows, :] = up + inv[rows, 0:1] * back
        for k, value in enumerate(
            (first_grad * n, first_grad, qg2[rows, :].astype(F32), up, second_grad * n, second_grad)
        ):
            sums[k] = sums[k] + jnp.sum(value, axis=0, keepdims=True)
    l_ig = lc(ig_v, o_ig)
    for name, row in zip(("ln1_gain", "ln1_bias", "b_query", "column", "ln2_gain", "ln2_bias"), sums):
        put(name, row)
    s_vec = []
    for o in range(1, NSP):
        rows = pl.ds(pl.multiple_of(lax.rem(d + o, NSP) * 8, 8), 8)
        s_vec.append(rc("vec", o, vec.at[rows, :], rvec.at[o], sp_peer(o)))
        send(s_vec[-1])

    s_wox.wait_recv()
    wo_s1[...] = (wo_part[:, near_rx, :].astype(F32) + rx_wo[...].astype(F32)).astype(BF16)
    s_woy = rc("woy", 0, wo_s1.at[:, :, far_cy], ry_wo, ynb)
    send(s_woy)
    s_wqy.wait_recv()
    wq_s1[...] = (wq_part[:, near_ry, :].astype(F32) + ry_wq[...].astype(F32)).astype(BF16)
    s_wqx = rc("wqx", 0, wq_s1.at[:, :, far_cx], rx_wq, xnb)
    send(s_wqx)

    for copy in s_wkv:
        copy.wait_recv()
    total = wkv_part[pl.ds(pl.multiple_of(d * R, 8), R), :]
    for o in range(1, NSP):
        total = total + rkv[o].astype(F32)
    sm[g, :R, :] = total
    for copy in s_vec:
        copy.wait_recv()
    total = vec[pl.ds(pl.multiple_of(d * 8, 8), 8), :]
    for o in range(1, NSP):
        total = total + rvec[o]
    sm[g, R:, :] = total
    s_sm = [rc("sm", o, sm.at[g], sm.at[g], xy_peer(o, c)) for o in range(1, NG)]
    for copy in s_sm:
        send(copy)

    s_woy.wait_recv()
    zs_wo[...] = (wo_s1[:, :, near_cy].astype(F32) + ry_wo[...].astype(F32)).astype(BF16)
    s_woz = []
    for o in range(1, NZ):
        s_woz.append(rc("woz", o, zs_wo.at[lax.rem(z + o, NZ)], rz_wo.at[o], z_peer(o)))
        send(s_woz[-1])
    s_wqx.wait_recv()
    zs_wq[...] = (wq_s1[:, :, near_cx].astype(F32) + rx_wq[...].astype(F32)).astype(BF16)
    s_wqz = []
    for o in range(1, NZ):
        s_wqz.append(rc("wqz", o, zs_wq.at[lax.rem(z + o, NZ)], rz_wq.at[o], z_peer(o)))
        send(s_wqz[-1])

    for copy in s_sm:
        copy.wait_recv()
    total = sm[0]
    for k in range(1, NG):
        total = total + sm[k]
    fin_kv[...] = total[:R]
    fin_vec[...] = total[R:]
    l_kv = lc(fin_kv, o_wkv)
    mine8 = pl.ds(pl.multiple_of(d * 8, 8), 8)
    s_vg = [rc("vg", o, fin_vec, o_vec.at[mine8, :], sp_peer(o)) for o in range(1, NSP)]
    for copy in s_vg:
        send(copy)
    l_vg = lc(fin_vec, o_vec.at[mine8, :])

    total = zs_wo[z].astype(F32)
    for o in range(1, NZ):
        s_woz[o - 1].wait_recv()
        total = total + rz_wo[o].astype(F32)
    fin_wo[...] = total.astype(BF16)
    s_wog = [rc("wog", o, fin_wo, o_wo.at[xx, yy], xy_peer(o, c)) for o in range(1, NG)]
    for copy in s_wog:
        send(copy)
    l_fo = lc(fin_wo, o_wo.at[xx, yy])
    total = zs_wq[z].astype(F32)
    for o in range(1, NZ):
        s_wqz[o - 1].wait_recv()
        total = total + rz_wq[o].astype(F32)
    fin_wq[...] = total.astype(BF16)
    s_wqg = [rc("wqg", o, fin_wq, o_wq.at[yy, xx], xy_peer(o, c)) for o in range(1, NG)]
    for copy in s_wqg:
        send(copy)
    l_fq = lc(fin_wq, o_wq.at[yy, xx])

    for o in range(1, NG):
        wp_g(o).wait_recv()
    for o in range(NG):
        for core in range(2):
            if o or core:
                wf_g(o, core).wait_recv()
    for copy in s_wog + s_wqg + s_vg:
        copy.wait_recv()
    for copy in started:
        copy.wait_send()
    for q in range(NZ):
        x_half(q).wait_send()
        wp_y(q).wait_send()
    for k in range(2):
        y_chunk(2 * (1 - yy) + k).wait_send()
    wf_x.wait_send()
    for o in range(1, NZ):
        wp_z(o).wait_send()
        wf_z(o).wait_send()
    for o in range(1, NG):
        wp_g(o).wait_send()
    for o in range(NG):
        for core in range(2):
            if o or core:
                wf_g(o, core).wait_send()
    for copy in l_fin + [l_lo, l_ig, l_kv, l_vg, l_fo, l_fq]:
        copy.wait()


EVENTS = (
    (0, "wp0"),
    (2, "wp1"),
    (2, "wf_first"),
    (5, "wp2"),
    (7, "wp3"),
    (7, "wf_second"),
    (9, "wp_second"),
    (10, "wf_third"),
)


def finish_kernel(
    dims, wp, wf, wo, wq, wkv, vec, lo, ig,
    layer_out, input_grad, ln1_gain, ln1_bias, w_query, b_query, w_keyval, b_keyval,
    w_attn_out, b_attn_out, ln2_gain, ln2_bias, w_fc, b_fc, w_proj, b_proj,
):
    T, D, F, S, NSP, NG = dims
    Q, R, C2 = F // NSP, D // NSP, D // 2
    layer_out[...] = lo[...]
    input_grad[...] = ig[...]
    for k in range(NG):
        w_proj[Q // NG * k : Q // NG * (k + 1), :] = wp[k].astype(F32)
        for core in range(2):
            at = Q * (2 * k + core)
            w_fc[:, at : at + Q] = wf[k, core].astype(F32)
    for a in range(2):
        for b in range(2):
            rows = slice(R // 2 * a, R // 2 * (a + 1))
            cols = slice(C2 * b, C2 * (b + 1))
            w_attn_out[rows, cols] = wo[a, b].astype(F32)
            w_query[rows, cols] = wq[a, b].astype(F32)
    w_keyval[...] = wkv[...]
    rows_v, _ = vec_rows(D, F, 2 * HD)
    for name, out in (
        ("ln1_gain", ln1_gain), ("ln1_bias", ln1_bias), ("b_query", b_query), ("b_keyval", b_keyval),
        ("column", b_attn_out), ("column", b_proj), ("ln2_gain", ln2_gain), ("ln2_bias", ln2_bias),
        ("b_fc", b_fc),
    ):
        at, count = rows_v[name]
        out[...] = jnp.concatenate([vec[at + i : at + i + 1, :] for i in range(count)], axis=1).reshape(
            128 * count
        )


def fused_local(n_grp, n_sp, *args):
    layer_input, block_order = args[0], args[1]
    T, D = layer_input.shape
    F = args[12].shape[1]
    S = T * n_sp
    NZ, NG, NSP = n_sp // 2, n_grp, n_sp
    Q, R, C2, pair = F // n_sp, D // n_sp, D // 2, 2 * HD
    dims = (T, D, F, S, NSP, NG)
    V = pltpu.VMEM
    scratch = [
        V((8, D), F32), V((1, pair), F32), V((1, F), F32),
        V((2 * T, D), BF16), V((2 * T, D), BF16), V((2 * T, D), BF16), V((2 * T, D), BF16),
        V((D, 2 * T), BF16), V((D, 2 * T), BF16), V((T, D), F32), V((T, 128), F32),
        V((D, pair), BF16), V((D, D), BF16), V((D, D), BF16), V((NZ, D, Q), BF16), V((NZ, Q, D), BF16),
        V((T, pair), BF16), V((NZ, 2 * T, Q), BF16), V((NZ, 2 * T, Q), BF16),
        V((2 * T, D), F32), V((2 * T, D), F32), V((T, D), F32), V((T, D), F32),
        V((NZ, Q, D), BF16), V((NZ, Q // 2, D), BF16), V((NZ, Q // 2, D), BF16), V((NZ, Q // 4, D), BF16),
        V((NZ, Q // 4, D), BF16), V((NZ, Q // 4, D), BF16), V((Q // 4, D), BF16),
        V((NZ, D, Q), BF16), V((2, D, Q), BF16), V((D, Q), BF16), V((D, Q), BF16), V((D, Q), BF16),
        V((D, Q), BF16), V((NZ, 2 * R, Q), BF16), V((2 * R, Q), BF16),
        V((S, pair), BF16), V((pair, S), BF16), V((H, 2 * T, pair), BF16), V((S, T), F32), V((S, T), F32),
        V((S, T), F32), V((S, 2 * T), BF16), V((S, pair), F32), V((S, pair), BF16), V((NSP, T, pair), BF16),
        V((D, T), BF16), V((D, T), BF16), V((NZ, R, T), BF16), V((2 * T, D), BF16),
        V((NZ, R, D), BF16), V((NZ, R // 2, D), BF16), V((NZ, R // 2, D), BF16), V((NZ, R // 2, C2), BF16),
        V((NZ, R // 2, C2), BF16), V((NZ, R // 2, C2), BF16), V((R // 2, C2), BF16),
        V((NZ, R, D), BF16), V((NZ, R // 2, D), BF16), V((NZ, R // 2, D), BF16), V((NZ, R // 2, C2), BF16),
        V((NZ, R // 2, C2), BF16), V((NZ, R // 2, C2), BF16), V((R // 2, C2), BF16),
        V((8 * NSP, 128), F32), V((NSP, 8, 128), F32), V((D, pair), F32), V((D, pair), BF16),
        V((NSP, R, pair), BF16), V((NG, R + 8, 128), F32), V((R, 128), F32), V((8, 128), F32),
        V((T, D), BF16), V((T, D), F32), V((T, pair), F32), V((T, pair), F32), V((8, T), F32), V((8, T), F32),
        pltpu.SemaphoreType.DMA((40,)), pltpu.SemaphoreType.DMA((128,)), pltpu.SemaphoreType.DMA((128,)),
    ]
    any_spec = pl.BlockSpec(memory_space=pl.ANY)
    shape = jax.ShapeDtypeStruct
    held = pl.pallas_call(
        functools.partial(fused_kernel, dims),
        out_shape=(
            shape((NG, Q // 4, D), BF16),
            shape((NG, 2, R, Q), BF16),
            shape((2, 2, R // 2, C2), BF16),
            shape((2, 2, R // 2, C2), BF16),
            shape((R, pair), F32),
            shape((8 * NSP, 128), F32),
            shape((T, D), BF16),
            shape((T, D), F32),
        ),
        in_specs=[any_spec, pl.BlockSpec(memory_space=pltpu.SMEM)] + [any_spec] * 16,
        out_specs=(any_spec,) * 8,
        scratch_shapes=scratch,
        compiler_params=pltpu.CompilerParams(
            collective_id=0, has_side_effects=True, vmem_limit_bytes=67043328
        ),
        name="fused_layer",
    )(*args)
    vmem_spec = pl.BlockSpec(memory_space=pltpu.VMEM)
    row = shape((D,), F32)
    return pl.pallas_call(
        functools.partial(finish_kernel, dims),
        out_shape=(
            shape((T, D), BF16), shape((T, D), F32), row, row, shape((R, D), F32), row, shape((R, pair), F32),
            shape((pair,), F32), shape((R, D), F32), row, row, row, shape((R, F), F32), shape((F,), F32),
            shape((Q, D), F32), row,
        ),
        in_specs=[vmem_spec] * 8,
        out_specs=(vmem_spec,) * 16,
        compiler_params=pltpu.CompilerParams(vmem_limit_bytes=48 << 20),
        name="finish",
    )(*held)


def fits(mesh, args):
    n_grp, n_sp = mesh.shape["grp"], mesh.shape["sp"]
    tokens, width = args[0].shape
    seqs, blocks = args[1].shape
    ff = args[12].shape[1]
    rows = tokens // (n_grp * n_sp)
    return (
        n_grp == 4
        and n_sp == 2 * n_grp
        and seqs == n_grp
        and blocks == 2 * n_sp
        and rows == 2 * 128
        and width == H * HD
        and width % (32 * n_sp) == 0
        and ff % (128 * n_sp) == 0
        and sum(count for _, count in vec_rows(width, ff, 2 * HD)[0].values()) <= 8 * n_sp
    )


def layer_norm(values, gain_row, shift_row):
    centre = jnp.mean(values, axis=-1, keepdims=True)
    centred = values - centre
    spread = jnp.mean(centred * centred, axis=-1, keepdims=True)
    inverse_dev = lax.rsqrt(spread + norm_eps)
    normed = centred * inverse_dev
    return (normed * gain_row + shift_row, normed, inverse_dev)


def norm_back(upstream, normed, inverse_dev, gain_row):
    scaled = upstream * gain_row
    return inverse_dev * (
        scaled
        - jnp.mean(scaled, axis=-1, keepdims=True)
        - normed * jnp.mean(scaled * normed, axis=-1, keepdims=True)
    )


def rotary_tables(position):
    half_rot = ROT // 2
    frequency = jnp.exp(jnp.arange(half_rot, dtype=jnp.float32) * (-2.0 * rotary_base_log / ROT))
    angles = position.astype(jnp.float32)[:, None] * 0.25 * frequency[None, :]
    return (jnp.cos(angles), jnp.sin(angles))


def rotate(values, cosine, sine_table):
    half_rot = ROT // 2
    cos_rows = cosine[:, None, :]
    sin_rows = sine_table[:, None, :]
    lower_half = values[..., :half_rot]
    upper_half = values[..., half_rot:ROT]
    return jnp.concatenate(
        [
            lower_half * cos_rows - upper_half * sin_rows,
            upper_half * cos_rows + lower_half * sin_rows,
            values[..., ROT:],
        ],
        axis=-1,
    )


def rotate_back(values, cosine, sine_table):
    half_rot = ROT // 2
    cos_rows = cosine[:, None, :]
    sin_rows = sine_table[:, None, :]
    lower_half = values[..., :half_rot]
    upper_half = values[..., half_rot:ROT]
    return jnp.concatenate(
        [
            lower_half * cos_rows + upper_half * sin_rows,
            upper_half * cos_rows - lower_half * sin_rows,
            values[..., ROT:],
        ],
        axis=-1,
    )


def key_scores(query_rows, row_pos, kv_sequence, block_index, block_rows):
    key_start = block_index * block_rows
    key_slice = lax.dynamic_slice_in_dim(kv_sequence, key_start, block_rows, 0)
    raw_scores = (
        jnp.einsum("rd,kd->rk", query_rows, key_slice[:, :HD], preferred_element_type=jnp.float32)
        * 0.125
    )
    key_pos = key_start + lax.broadcasted_iota(jnp.int32, (1, block_rows), 1)
    return (jnp.where(key_pos <= row_pos[:, None], raw_scores, masked_score), key_slice)


def attention_forward(query_tiles, tile_pos, kv_sorted):
    pair_count = query_tiles.shape[0]
    pairs_per_seq = pair_count // kv_sorted.shape[0]
    block_rows = min(score_block, kv_sorted.shape[1])

    def one_pair(inputs):
        query_rows, row_pos, pair_index = inputs
        kv_sequence = kv_sorted[pair_index // pairs_per_seq]
        key_blocks = jnp.max(row_pos) // block_rows + 1
        row_count = query_rows.shape[0]

        def max_pass(block_index, carried):
            running_max, running_sum = carried
            masked, key_slice = key_scores(
                query_rows, row_pos, kv_sequence, block_index, block_rows
            )
            new_max = jnp.maximum(running_max, jnp.max(masked, axis=1, keepdims=True))
            running_sum = running_sum * jnp.exp(running_max - new_max) + jnp.sum(
                jnp.exp(masked - new_max), axis=1, keepdims=True
            )
            return (new_max, running_sum)

        start_max = jnp.full((row_count, 1), masked_score, jnp.float32)
        running_max, running_sum = lax.fori_loop(
            0, key_blocks, max_pass, (start_max, jnp.zeros((row_count, 1), jnp.float32))
        )
        log_total = running_max + jnp.log(running_sum)

        def value_pass(block_index, output):
            masked, key_slice = key_scores(
                query_rows, row_pos, kv_sequence, block_index, block_rows
            )
            weights = jnp.exp(masked - log_total).astype(jnp.bfloat16)
            return output + jnp.dot(weights, key_slice[:, HD:], preferred_element_type=jnp.float32)

        output = lax.fori_loop(0, key_blocks, value_pass, jnp.zeros((row_count, HD), jnp.float32))
        return (output, log_total)

    return lax.map(one_pair, (query_tiles, tile_pos, jnp.arange(pair_count, dtype=jnp.int32)))


def attention_backward(query_tiles, tile_pos, grad_tiles, log_totals, kv_sorted):
    pair_count = query_tiles.shape[0]
    pairs_per_seq = pair_count // kv_sorted.shape[0]
    block_rows = min(score_block, kv_sorted.shape[1])
    pair_width = kv_sorted.shape[2]

    def one_pair(key_grads, inputs):
        query_rows, row_pos, grad_rows, log_total, pair_index = inputs
        sequence = pair_index // pairs_per_seq
        kv_sequence = kv_sorted[sequence]
        key_blocks = jnp.max(row_pos) // block_rows + 1
        row_count = query_rows.shape[0]

        def pass_terms(block_index):
            masked, key_slice = key_scores(
                query_rows, row_pos, kv_sequence, block_index, block_rows
            )
            weights = jnp.exp(masked - log_total)
            weight_grads = jnp.einsum(
                "rd,kd->rk", grad_rows, key_slice[:, HD:], preferred_element_type=jnp.float32
            )
            return (weights, weight_grads, key_slice)

        def delta_pass(block_index, row_delta):
            weights, weight_grads, unused_slice = pass_terms(block_index)
            return row_delta + jnp.sum(weights * weight_grads, axis=1, keepdims=True)

        row_delta = lax.fori_loop(0, key_blocks, delta_pass, jnp.zeros((row_count, 1), jnp.float32))

        def grad_pass(block_index, carried):
            query_grad, sequence_grads = carried
            weights, weight_grads, key_slice = pass_terms(block_index)
            score_grad = (weights * (weight_grads - row_delta)).astype(jnp.bfloat16)
            query_grad = (
                query_grad
                + jnp.dot(score_grad, key_slice[:, :HD], preferred_element_type=jnp.float32) * 0.125
            )
            key_part = (
                jnp.einsum("rk,rd->kd", score_grad, query_rows, preferred_element_type=jnp.float32)
                * 0.125
            )
            value_part = jnp.einsum(
                "rk,rd->kd",
                weights.astype(jnp.bfloat16),
                grad_rows,
                preferred_element_type=jnp.float32,
            )
            key_start = block_index * block_rows
            previous = lax.dynamic_slice(
                sequence_grads, (sequence, key_start, 0), (1, block_rows, pair_width)
            )
            updated = previous + jnp.concatenate([key_part, value_part], axis=1)[None]
            return (
                query_grad,
                lax.dynamic_update_slice(sequence_grads, updated, (sequence, key_start, 0)),
            )

        query_grad, key_grads = lax.fori_loop(
            0, key_blocks, grad_pass, (jnp.zeros((row_count, HD), jnp.float32), key_grads)
        )
        return (key_grads, query_grad)

    start_grads = jnp.zeros(kv_sorted.shape, jnp.float32)
    key_grads, query_grads = lax.scan(
        one_pair,
        start_grads,
        (query_tiles, tile_pos, grad_tiles, log_totals, jnp.arange(pair_count, dtype=jnp.int32)),
    )
    return (query_grads, key_grads)


def local(
    layer_input,
    block_order,
    ln1_gain,
    ln1_bias,
    w_query,
    b_query,
    w_keyval,
    b_keyval,
    w_attn_out,
    b_attn_out,
    ln2_gain,
    ln2_bias,
    w_fc,
    b_fc,
    w_proj,
    b_proj,
    kv_grad,
    out_grad,
):
    my_rank = lax.axis_index("sp")
    seq_count = block_order.shape[0]
    block_count = block_order.shape[1]
    token_count = layer_input.shape[0]
    shard_len = token_count // seq_count
    block_len = shard_len // 2
    model_width = layer_input.shape[1]
    pair_width = 2 * HD
    pair_count = 2 * seq_count
    input_float = layer_input.astype(jnp.float32)
    first_in, first_hat, first_inv = layer_norm(input_float, ln1_gain, ln1_bias)
    first_low = first_in.astype(jnp.bfloat16)
    query_pre = jnp.dot(first_low, w_query, preferred_element_type=jnp.float32) + b_query
    keyval_pre = jnp.dot(first_low, w_keyval, preferred_element_type=jnp.float32) + b_keyval
    offsets = jnp.arange(block_len, dtype=jnp.int32)
    own_blocks = lax.dynamic_slice_in_dim(block_order, 2 * my_rank, 2, 1)
    own_pos = (own_blocks[:, :, None] * block_len + offsets[None, None, :]).reshape(token_count)
    cosine, sine_table = rotary_tables(own_pos)
    query_use = (
        rotate(query_pre.reshape(token_count, H, HD), cosine, sine_table)
        .reshape(token_count, model_width)
        .astype(jnp.bfloat16)
    )
    key_rot = rotate(keyval_pre[:, None, :HD], cosine, sine_table)[:, 0, :]
    keyval_use = jnp.concatenate([key_rot, keyval_pre[:, HD:]], axis=1).astype(jnp.bfloat16)
    gathered = lax.all_gather(
        keyval_use.reshape(seq_count, shard_len, pair_width), "sp", axis=1, tiled=True
    )
    seq_len = gathered.shape[1]
    block_sorter = jnp.argsort(block_order, axis=1)
    kv_sorted = jnp.take_along_axis(
        gathered.reshape(seq_count, block_count, block_len, pair_width),
        block_sorter[:, :, None, None],
        axis=1,
    ).reshape(seq_count, seq_len, pair_width)
    row_pos = own_pos.reshape(seq_count, shard_len)
    query_rows = query_use.reshape(seq_count, shard_len, model_width)
    query_tiles = query_rows.reshape(pair_count, block_len * H, HD)
    tile_pos = jnp.repeat(row_pos.reshape(pair_count, block_len), H, axis=1)
    head_rows, log_totals = attention_forward(query_tiles, tile_pos, kv_sorted)
    heads_sorted = head_rows.reshape(seq_count, shard_len, model_width).astype(jnp.bfloat16)
    heads_local = heads_sorted.reshape(token_count, model_width)
    attn_branch = jnp.dot(heads_local, w_attn_out, preferred_element_type=jnp.float32) + b_attn_out
    second_in, second_hat, second_inv = layer_norm(input_float, ln2_gain, ln2_bias)
    second_low = second_in.astype(jnp.bfloat16)
    hidden = jnp.dot(second_low, w_fc, preferred_element_type=jnp.float32) + b_fc
    erf_part = 1.0 + lax.erf(hidden * half_root)
    activated = (0.5 * hidden * erf_part).astype(jnp.bfloat16)
    mlp_branch = jnp.dot(activated, w_proj, preferred_element_type=jnp.float32) + b_proj
    layer_out = (input_float + attn_branch + mlp_branch).astype(jnp.bfloat16)
    upstream = out_grad.astype(jnp.float32)
    column_sum = jnp.sum(upstream, axis=0)
    w_proj_grad = jnp.einsum("tf,td->fd", activated, out_grad, preferred_element_type=jnp.float32)
    act_grad = jnp.einsum("td,fd->tf", out_grad, w_proj, preferred_element_type=jnp.float32)
    gelu_slope = 0.5 * erf_part + hidden * jnp.exp(-0.5 * hidden * hidden) * inv_root_tau
    hidden_grad = (act_grad * gelu_slope).astype(jnp.bfloat16)
    w_fc_grad = jnp.einsum("td,tf->df", second_low, hidden_grad, preferred_element_type=jnp.float32)
    b_fc_grad = jnp.sum(hidden_grad.astype(jnp.float32), axis=0)
    second_grad = jnp.einsum("tf,df->td", hidden_grad, w_fc, preferred_element_type=jnp.float32)
    w_attn_out_grad = jnp.einsum(
        "te,td->ed", heads_local, out_grad, preferred_element_type=jnp.float32
    )
    heads_grad = jnp.einsum(
        "td,ed->te", out_grad, w_attn_out, preferred_element_type=jnp.float32
    ).astype(jnp.bfloat16)
    grad_rows = heads_grad.reshape(seq_count, shard_len, model_width)
    grad_tiles = grad_rows.reshape(pair_count, block_len * H, HD)
    query_tile_grads, sorted_kv_grads = attention_backward(
        query_tiles, tile_pos, grad_tiles, log_totals, kv_sorted
    )
    query_rot_rows = query_tile_grads.reshape(seq_count, shard_len, model_width)
    query_rot_grad = query_rot_rows.reshape(token_count, model_width)
    query_grad = (
        rotate_back(query_rot_grad.reshape(token_count, H, HD), cosine, sine_table)
        .reshape(token_count, model_width)
        .astype(jnp.bfloat16)
    )
    stored_kv_grads = jnp.take_along_axis(
        sorted_kv_grads.reshape(seq_count, block_count, block_len, pair_width),
        block_order[:, :, None, None],
        axis=1,
    ).reshape(seq_count, seq_len, pair_width)
    own_kv_grad = lax.psum_scatter(stored_kv_grads, "sp", scatter_dimension=1, tiled=True).reshape(
        token_count, pair_width
    ) + kv_grad.astype(jnp.float32)
    key_pre_grad = rotate_back(own_kv_grad[:, None, :HD], cosine, sine_table)[:, 0, :]
    keyval_grad = jnp.concatenate([key_pre_grad, own_kv_grad[:, HD:]], axis=1).astype(jnp.bfloat16)
    w_query_grad = jnp.einsum(
        "td,te->de", first_low, query_grad, preferred_element_type=jnp.float32
    )
    b_query_grad = jnp.sum(query_grad.astype(jnp.float32), axis=0)
    w_keyval_grad = jnp.einsum(
        "td,te->de", first_low, keyval_grad, preferred_element_type=jnp.float32
    )
    b_keyval_grad = jnp.sum(keyval_grad.astype(jnp.float32), axis=0)
    first_grad = jnp.einsum(
        "te,de->td", query_grad, w_query, preferred_element_type=jnp.float32
    ) + jnp.einsum("te,de->td", keyval_grad, w_keyval, preferred_element_type=jnp.float32)
    first_back = norm_back(first_grad, first_hat, first_inv, ln1_gain)
    second_back = norm_back(second_grad, second_hat, second_inv, ln2_gain)
    input_grad = upstream + first_back + second_back
    (
        ln1_gain_grad,
        ln1_bias_grad,
        b_query_total,
        b_keyval_total,
        bias_out_total,
        ln2_gain_grad,
        ln2_bias_grad,
        b_fc_total,
    ) = lax.psum(
        (
            jnp.sum(first_grad * first_hat, axis=0),
            jnp.sum(first_grad, axis=0),
            b_query_grad,
            b_keyval_grad,
            column_sum,
            jnp.sum(second_grad * second_hat, axis=0),
            jnp.sum(second_grad, axis=0),
            b_fc_grad,
        ),
        ("grp", "sp"),
    )
    query_share, keyval_share, out_share, fc_share, proj_share = (
        lax.psum_scatter(w_query_grad, "sp", scatter_dimension=0, tiled=True),
        lax.psum_scatter(w_keyval_grad, "sp", scatter_dimension=0, tiled=True),
        lax.psum_scatter(w_attn_out_grad, "sp", scatter_dimension=0, tiled=True),
        lax.psum_scatter(w_fc_grad, "sp", scatter_dimension=0, tiled=True),
        lax.psum_scatter(w_proj_grad, "sp", scatter_dimension=0, tiled=True),
    )
    query_total, keyval_total, out_total, fc_total, proj_total = lax.psum(
        (query_share, keyval_share, out_share, fc_share, proj_share), "grp"
    )
    return (
        layer_out,
        input_grad,
        ln1_gain_grad,
        ln1_bias_grad,
        query_total,
        b_query_total,
        keyval_total,
        b_keyval_total,
        out_total,
        bias_out_total,
        ln2_gain_grad,
        ln2_bias_grad,
        fc_total,
        b_fc_total,
        proj_total,
        bias_out_total,
    )


def solution(mesh):
    placed = (
        P(("grp", "sp"), None),
        P("grp", None),
        P(),
        P(),
        P(),
        P(),
        P(),
        P(),
        P(),
        P(),
        P(),
        P(),
        P(),
        P(),
        P(),
        P(),
        P(("grp", "sp"), None),
        P(("grp", "sp"), None),
    )
    def step(*args):
        if fits(mesh, args):
            body = functools.partial(fused_local, mesh.shape["grp"], mesh.shape["sp"])
        else:
            body = local
        return spread(body)(*args)

    def spread(body):
        return jax.shard_map(
            body,
            mesh=mesh,
            in_specs=placed,
            out_specs=(
                P(("grp", "sp"), None),
                P(("grp", "sp"), None),
                P(),
                P(),
                P("sp", None),
                P(),
                P("sp", None),
                P(),
                P("sp", None),
                P(),
                P(),
                P(),
                P("sp", None),
                P(),
                P("sp", None),
                P(),
            ),
            check_vma=False,
        )

    return step
```

```python
import functools
import math

import jax
import jax.numpy as jnp
from jax import lax
from jax.experimental import pallas as pl
from jax.experimental.pallas import tpu as pltpu
from jax.sharding import PartitionSpec as P

H = 12
HD = 64
ROT = 16
MESH = pl.DeviceIdType.MESH
F32 = jnp.float32
BF16 = jnp.bfloat16
NN = (((1,), (0,)), ((), ()))
NT = (((1,), (1,)), ((), ()))
TN = (((0,), (0,)), ((), ()))


def mm(a, b, dims=NN):
    return lax.dot_general(a, b, dims, preferred_element_type=F32)

norm_eps = 1e-05
half_root = 0.7071067811865476
inv_root_tau = 0.3989422804014327
masked_score = -1e30
rotary_base_log = math.log(10000.0)
score_block = 512


def vec_rows(width, ff, pair):
    names = ("ln1_gain", "ln1_bias", "b_query", "b_keyval", "column", "ln2_gain", "ln2_bias", "b_fc")
    sizes = (width, width, width, pair, width, width, width, ff)
    at, rows = 0, {}
    for name, size in zip(names, sizes):
        rows[name] = (at, size // 128)
        at += size // 128
    return rows, at


def fused_kernel(
    dims,
    x_h,
    order_s,
    g1_h,
    b1_h,
    wq_h,
    bq_h,
    wkv_h,
    bkv_h,
    wo_h,
    bo_h,
    g2_h,
    b2_h,
    wfc_h,
    bfc_h,
    wpr_h,
    bpr_h,
    kvg_h,
    og_h,
    o_wp,
    o_wf,
    o_wo,
    o_wq,
    o_wkv,
    o_vec,
    o_lo,
    o_ig,
    vecs,
    bkv_v,
    bfc_v,
    x2,
    og2,
    fi2,
    si2,
    fit,
    sit,
    nrm,
    inv,
    wkv_v,
    wq_v,
    wo_v,
    wfc_v,
    wpr_v,
    kvg_v,
    act_s,
    hg_s,
    mlp_all,
    sec_all,
    mlp_r,
    sec_r,
    wp_part,
    rx_wp,
    wp_s1,
    ry_wp,
    zs_wp,
    rz_wp,
    rzf,
    zf_s0,
    rx_zf,
    zf_s1,
    ry_zf,
    fin_wp,
    wf_part,
    ry_wf,
    rx_wf,
    wf_s1,
    wf_own,
    wf_in,
    zs_wf,
    rz_wf,
    fin_wf,
    kv_all,
    kvt,
    qo,
    bias,
    sbuf,
    dbuf,
    dsp,
    dkv,
    dkv_b,
    rdk,
    dks,
    rdkv,
    kvg2,
    oht,
    qgt,
    ht_r,
    qg2,
    wo_part,
    rx_wo,
    wo_s1,
    ry_wo,
    zs_wo,
    rz_wo,
    fin_wo,
    wq_part,
    ry_wq,
    wq_s1,
    rx_wq,
    zs_wq,
    rz_wq,
    fin_wq,
    vec,
    rvec,
    wkv_part,
    wkv_b,
    rkv,
    sm,
    fin_kv,
    fin_vec,
    lo_v,
    ig_v,
    ctab,
    stab,
    cost,
    sint,
    lsem,
    ssem,
    rsem,
):
    T, D, F, S, NSP, NG = dims
    NZ = NSP // 2
    D2 = D // 2
    Q = F // NSP
    QH = Q // 2
    R = D // NSP
    C2 = D // 2
    pair = 2 * HD
    g = lax.axis_index("grp")
    d = lax.axis_index("sp")
    c = lax.rem(d, 2)
    z = lax.div(d, 2)
    xx = lax.rem(g, 2)
    yy = lax.div(g, 2)
    partner = (g, d + 1 - 2 * c)
    xnb = (g + 1 - 2 * xx, d)
    ynb = (g + 2 - 4 * yy, d)

    def sp_peer(o):
        return (g, lax.rem(d + o, NSP))

    def z_peer(o):
        return (g, 2 * lax.rem(z + o, NZ) + c)

    def xy_peer(o, core):
        return (lax.rem(g + o, NG), 2 * z + core)

    base = {}
    used = [0]

    def take(name, n):
        base[name] = used[0]
        used[0] += n

    for name, n in (
        ("x", 1), ("og", 1), ("kv", NSP), ("mlp", 1), ("sec", 1),
        ("wpx", NZ), ("wpy", NZ), ("wpz", NZ), ("wpg", NG),
        ("wpf", NZ), ("zfx", 1), ("zfy", 1),
        ("wfy", 2), ("wfx", 2), ("wfs", 2), ("wfz", NZ), ("wfg", 2 * NG),
        ("ht", NZ), ("qg", 1), ("dk", NZ), ("dkv", NZ), ("kvg", 1),
        ("wox", 1), ("woy", 1), ("woz", NZ), ("wog", NG),
        ("wqy", 1), ("wqx", 1), ("wqz", NZ), ("wqg", NG),
        ("wkv", NZ), ("vec", NSP), ("sm", NG), ("vg", NSP),
    ):
        take(name, n)

    def rc(name, i, src, dst, to):
        k = base[name] + i
        return pltpu.make_async_remote_copy(
            src_ref=src,
            dst_ref=dst,
            send_sem=ssem.at[k],
            recv_sem=rsem.at[k],
            device_id=to,
            device_id_type=MESH,
        )

    started = []

    def send(copy):
        copy.start()
        started.append(copy)

    lused = [0]

    def lc(src, dst):
        copy = pltpu.make_async_copy(src, dst, lsem.at[lused[0]])
        lused[0] += 1
        copy.start()
        return copy

    def chunk_of(j):
        far_y = lax.div(j, 2) == 0
        far_x = lax.rem(j, 2) == 0
        return 2 * jnp.where(far_y, 1 - yy, yy) + jnp.where(far_x, 1 - xx, xx)

    def chunk_in(j):
        far_y = lax.div(j, 2) == 0
        far_x = lax.rem(j, 2) == 0
        return 2 * jnp.where(far_y, 1 - yy, yy) + jnp.where(far_x, xx, 1 - xx)

    own = pl.ds(0, T)
    other = pl.ds(T, T)
    l_x = lc(x_h, x2.at[own])
    l_og = lc(og_h, og2.at[own])
    l_wkv = lc(wkv_h, wkv_v)
    l_vec = [
        lc(src, vecs.at[i]) for i, src in enumerate((g1_h, b1_h, g2_h, b2_h, bq_h, bo_h, bpr_h))
    ]
    l_bkv = lc(bkv_h, bkv_v.at[0])
    l_bfc = lc(bfc_h, bfc_v.at[0])
    l_mlp = []
    for j in range(NZ):
        q = chunk_of(j)
        cols = pl.ds(pl.multiple_of(Q * (2 * q + c), 128), Q)
        rows = pl.ds(pl.multiple_of(Q * (2 * q + c), 16), Q)
        l_mlp.append((lc(wfc_h.at[:, cols], wfc_v.at[q]), lc(wpr_h.at[rows, :], wpr_v.at[q])))
    l_wq = lc(wq_h, wq_v)
    l_wo = lc(wo_h, wo_v)
    l_kvg = lc(kvg_h, kvg_v)

    barrier = pltpu.get_barrier_semaphore()
    for o in range(1, NSP):
        pl.semaphore_signal(barrier, inc=1, device_id=sp_peer(o), device_id_type=MESH)
    for o in range(1, NG):
        for core in range(2):
            pl.semaphore_signal(barrier, inc=1, device_id=xy_peer(o, core), device_id_type=MESH)
    pl.semaphore_wait(barrier, NSP - 1 + 2 * (NG - 1))

    s_x = rc("x", 0, x_h, x2.at[other], partner)
    send(s_x)
    s_og = rc("og", 0, og_h, og2.at[other], partner)
    send(s_og)

    lane = lax.broadcasted_iota(jnp.int32, (8, T), 1)
    half = lax.broadcasted_iota(jnp.int32, (8, T), 0).astype(F32)
    block = T // 2
    first_block = order_s[0, 2 * d]
    second_block = order_s[0, 2 * d + 1]
    own_pos = jnp.where(
        lane < block, first_block * block + lane, second_block * block + (lane - block)
    )
    frequency = jnp.exp(half * (-2.0 * rotary_base_log / ROT))
    angle = own_pos.astype(F32) * 0.25 * frequency
    cosine, sine = jnp.cos(angle), jnp.sin(angle)
    cost[...] = cosine
    sint[...] = sine
    ones = jnp.ones((HD - ROT, T), F32)
    zeros = jnp.zeros((HD - ROT, T), F32)
    ctab[...] = jnp.concatenate([cosine, cosine, ones] * 2, axis=0).T
    stab[...] = jnp.concatenate([-sine, sine, zeros] * 2, axis=0).T
    lanes = lax.broadcasted_iota(jnp.int32, (128, pair), 1)
    low_half = lax.rem(lanes, HD) < ROT // 2

    def turn(tile, rows, sign):
        mixed = jnp.where(low_half, pltpu.roll(tile, pair - ROT // 2, 1), pltpu.roll(tile, ROT // 2, 1))
        return tile * ctab[rows, :] + (sign * mixed) * stab[rows, :]

    for copy in l_vec:
        copy.wait()
    l_bkv.wait()
    l_bfc.wait()
    g1, b1, g2, b2 = (vecs[i : i + 1, :] for i in range(4))
    vec[...] = jnp.zeros_like(vec)

    def norms(at, keep):
        for i in range(T // 128):
            rows = pl.ds(at + 128 * i, 128)
            v = x2[rows, :].astype(F32)
            centred = v - jnp.mean(v, axis=-1, keepdims=True)
            r = lax.rsqrt(jnp.mean(centred * centred, axis=-1, keepdims=True) + norm_eps)
            n = centred * r
            first = (n * g1 + b1).astype(BF16)
            second = (n * g2 + b2).astype(BF16)
            fi2[rows, :] = first
            si2[rows, :] = second
            fit[:, rows] = first.T
            sit[:, rows] = second.T
            if keep:
                nrm[rows, :] = n
                inv[rows, :] = jnp.broadcast_to(r, (128, 128))

    l_x.wait()
    norms(0, True)

    l_wkv.wait()
    for i in range(T // 128):
        rows = pl.ds(128 * i, 128)
        kv = mm(fi2[rows, :], wkv_v[...]) + bkv_v[...]
        kv = jnp.where(lanes < HD, turn(kv, rows, 1.0), kv)
        kv_all[pl.ds(pl.multiple_of(d * T + 128 * i, 128), 128), :] = kv.astype(BF16)
    mine = pl.ds(pl.multiple_of(d * T, T), T)
    s_kv = [rc("kv", o, kv_all.at[mine], kv_all.at[mine], sp_peer(o)) for o in range(1, NSP)]
    for copy in s_kv:
        send(copy)

    s_x.wait_recv()
    norms(T, False)
    l_og.wait()
    s_og.wait_recv()

    rows_v, _ = vec_rows(D, F, pair)
    for pair_of_copies in l_mlp:
        for copy in pair_of_copies:
            copy.wait()

    def x_half(q):
        far = pl.ds(pl.multiple_of(QH // 2 * (1 - xx), 16), QH // 2)
        return rc("wpx", q, wp_part.at[q, far, :], rx_wp.at[q], xnb)

    def z_half(o):
        q = lax.rem(z + o, NZ)
        return rc("wpf", o, wp_part.at[q, pl.ds(QH, QH), :], rzf.at[o], z_peer(o))

    def y_chunk(q):
        side = lax.rem(q, 2)
        return rc("wfy", side, wf_part.at[q, pl.ds(0, D2), :], ry_wf.at[side], ynb)

    def x_chunk(q):
        side = lax.div(q, 2)
        return rc("wfx", side, wf_part.at[q, pl.ds(D2, D2), :], rx_wf.at[side], xnb)

    def start_z_half(o):
        z_half(o).start()

    def mlp_chunk(j, carry):
        q = chunk_of(j)
        at = pl.ds(pl.multiple_of(Q * (2 * q + c), 128), Q)
        shift = bfc_v[:, at]
        total = jnp.zeros((1, Q), F32)
        for i in range(2 * T // 128):
            rows = pl.ds(128 * i, 128)
            hidden = mm(si2[rows, :], wfc_v[q]) + shift
            erf_part = 1.0 + lax.erf(hidden * half_root)
            act_s[q, rows, :] = (0.5 * hidden * erf_part).astype(BF16)
            slope = 0.5 * erf_part + hidden * jnp.exp(-0.5 * hidden * hidden) * inv_root_tau
            act_grad = mm(og2[rows, :], wpr_v[q], NT)
            hidden_grad = (act_grad * slope).astype(BF16)
            hg_s[q, rows, :] = hidden_grad
            total = total + jnp.sum(hidden_grad.astype(F32), axis=0, keepdims=True)
        for i in range(Q // 128):
            cols = pl.ds(128 * i, 128)
            wp_part[q, cols, :] = mm(act_s[q, :, cols], og2[...], TN).astype(BF16)
        x_half(q).start()
        for o in range(1, NZ):
            pl.when(lax.rem(z + o, NZ) == q)(functools.partial(start_z_half, o))
        for i in range(D // 128):
            rows = pl.ds(128 * i, 128)
            wf_part[q, rows, :] = mm(sit[rows, :], hg_s[q]).astype(BF16)

        @pl.when(j < 2)
        def _():
            y_chunk(q).start()

        @pl.when(lax.rem(j, 2) == 0)
        def _():
            x_chunk(q).start()

        at_row = rows_v["b_fc"][0] + Q // 128 * (2 * q + c)
        for i in range(Q // 128):
            vec[pl.ds(at_row + i, 1), :] = total[:, 128 * i : 128 * (i + 1)]
        return carry

    lax.fori_loop(0, NZ, mlp_chunk, 0)

    def mlp_sums(i, carry):
        at = lax.rem(i + T // 128, 2 * T // 128) * 128
        rows = pl.ds(pl.multiple_of(at, 128), 128)
        out = mm(act_s[0, rows, :], wpr_v[0])
        back = mm(hg_s[0, rows, :], wfc_v[0], NT)
        for q in range(1, NZ):
            out = out + mm(act_s[q, rows, :], wpr_v[q])
            back = back + mm(hg_s[q, rows, :], wfc_v[q], NT)
        mlp_all[rows, :] = out
        sec_all[rows, :] = back
        return carry

    lax.fori_loop(0, 2 * T // 128, mlp_sums, 0)
    s_mlp = rc("mlp", 0, mlp_all.at[other], mlp_r, partner)
    send(s_mlp)
    s_sec = rc("sec", 0, sec_all.at[other], sec_r, partner)
    send(s_sec)

    l_wq.wait()
    l_wo.wait()
    for i in range(T // 128):
        rows = pl.ds(128 * i, 128)
        query = mm(fi2[rows, :], wq_v[...]) + vecs[4:5, :]
        grads = mm(og2[rows, :], wo_v[...], NT)
        for t in range(D // pair):
            q_tile = turn(query[:, pair * t : pair * (t + 1)], rows, 1.0).astype(BF16).astype(F32) * 0.125
            o_tile = grads[:, pair * t : pair * (t + 1)]
            low = lanes < HD
            qo[2 * t, rows, :] = jnp.where(low, q_tile, 0.0).astype(BF16)
            qo[2 * t + 1, rows, :] = jnp.where(low, pltpu.roll(q_tile, HD, 1), 0.0).astype(BF16)
            late = pl.ds(T + 128 * i, 128)
            qo[2 * t, late, :] = jnp.where(low, 0.0, pltpu.roll(o_tile, HD, 1)).astype(BF16)
            qo[2 * t + 1, late, :] = jnp.where(low, 0.0, o_tile).astype(BF16)

    row_in = lax.broadcasted_iota(jnp.int32, (block, T), 0)
    query_pos = jnp.broadcast_to(own_pos[0:1, :], (block, T))
    for j in range(S // block):
        key_pos = order_s[0, j] * block + row_in
        bias[pl.ds(block * j, block), :] = jnp.where(key_pos <= query_pos, 0.0, masked_score)

    for copy in s_kv:
        copy.wait_recv()
    for j in range(S // 256):
        rows = pl.ds(256 * j, 256)
        kvt[:, rows] = kv_all[rows, :].T
        dkv[rows, :] = jnp.zeros((256, pair), F32)

    near_x = pl.ds(pl.multiple_of(QH // 2 * xx, 16), QH // 2)
    near_y = pl.ds(pl.multiple_of(QH // 4 * yy, 16), QH // 4)
    far_y = pl.ds(pl.multiple_of(QH // 4 * (1 - yy), 16), QH // 4)

    def wp_y(q):
        return rc("wpy", q, wp_s1.at[q, far_y, :], ry_wp.at[q], ynb)

    def wp_first(j):
        q = chunk_in(j)
        x_half(q).wait_recv()
        wp_s1[q] = (wp_part[q, near_x, :].astype(F32) + rx_wp[q].astype(F32)).astype(BF16)
        wp_y(q).start()

    def wp_z(o):
        return rc("wpz", o, zs_wp.at[lax.rem(z + o, NZ)], rz_wp.at[o], z_peer(o))

    def wp_second():
        for q in range(NZ):
            wp_y(q).wait_recv()
            zs_wp[q] = (wp_s1[q, near_y, :].astype(F32) + ry_wp[q].astype(F32)).astype(BF16)
        for o in range(1, NZ):
            wp_z(o).start()

    slot_wp = 2 * xx + yy

    def wp_g(o):
        return rc("wpg", o, fin_wp, o_wp.at[slot_wp], xy_peer(o, c))

    l_fin = []

    far_zx = pl.ds(pl.multiple_of(QH // 2 * (1 - xx), 16), QH // 2)
    zf_x = rc("zfx", 0, zf_s0.at[far_zx, :], rx_zf, xnb)
    zf_y = rc("zfy", 0, zf_s1.at[far_y, :], ry_zf, ynb)

    def zf_first():
        total = wp_part[z, QH:, :].astype(F32)
        for o in range(1, NZ):
            z_half(o).wait_recv()
            total = total + rzf[o].astype(F32)
        zf_s0[...] = total.astype(BF16)
        zf_x.start()

    def zf_second():
        zf_x.wait_recv()
        zf_s1[...] = (zf_s0[near_x, :].astype(F32) + rx_zf[...].astype(F32)).astype(BF16)
        zf_y.start()

    def zf_third():
        zf_y.wait_recv()
        fin_wp[1] = (zf_s1[near_y, :].astype(F32) + ry_zf[...].astype(F32)).astype(BF16)

    def wp_third():
        total = zs_wp[z].astype(F32)
        for o in range(1, NZ):
            wp_z(o).wait_recv()
            total = total + rz_wp[o].astype(F32)
        fin_wp[0] = total.astype(BF16)
        for o in range(1, NG):
            wp_g(o).start()
        l_fin.append(lc(fin_wp, o_wp.at[slot_wp]))

    def wf_second_send(part):
        return rc("wfs", part, wf_s1.at[part], wf_in.at[part], ynb if part else xnb)

    def wf_first(part):
        if part:
            q = 2 * (1 - yy) + xx
            x_chunk(2 * (1 - yy) + 1 - xx).wait_recv()
            got = rx_wf[1 - yy]
        else:
            q = 2 * yy + 1 - xx
            y_chunk(2 * (1 - yy) + 1 - xx).wait_recv()
            got = ry_wf[1 - xx]
        wf_s1[part] = (wf_part[q, D2 * part : D2 * (part + 1), :].astype(F32) + got.astype(F32)).astype(BF16)
        wf_second_send(part).start()

    def wf_second(part):
        q = 2 * yy + xx
        if part:
            x_chunk(2 * yy + 1 - xx).wait_recv()
            got = rx_wf[yy]
        else:
            y_chunk(2 * (1 - yy) + xx).wait_recv()
            got = ry_wf[xx]
        wf_own[part] = (wf_part[q, D2 * part : D2 * (part + 1), :].astype(F32) + got.astype(F32)).astype(BF16)

    def wf_z(o):
        rows = pl.ds(pl.multiple_of(2 * R * lax.rem(z + o, NZ), 16), 2 * R)
        return rc("wfz", o, zs_wf.at[rows, :], rz_wf.at[o], z_peer(o))

    def start_wf_z(o):
        wf_z(o).start()

    def wf_third(part):
        wf_second_send(part).wait_recv()
        zs_wf[D2 * part : D2 * (part + 1), :] = (
            wf_own[part].astype(F32) + wf_in[part].astype(F32)
        ).astype(BF16)
        for o in range(1, NZ):
            pl.when(lax.div(lax.rem(z + o, NZ), NZ // 2) == part)(functools.partial(start_wf_z, o))

    slot_wf = 2 * yy + xx

    def wf_g(o, core):
        to = c + core - 2 * c * core
        rows = pl.ds(pl.multiple_of(R * to, 16), R)
        return rc("wfg", 2 * o + core, fin_wf.at[rows, :], o_wf.at[slot_wf, c], xy_peer(o, to))

    def wf_fourth():
        total = zs_wf[pl.ds(pl.multiple_of(2 * R * z, 16), 2 * R), :].astype(F32)
        for o in range(1, NZ):
            wf_z(o).wait_recv()
            total = total + rz_wf[o].astype(F32)
        fin_wf[...] = total.astype(BF16)
        for o in range(NG):
            for core in range(2):
                if o or core:
                    wf_g(o, core).start()
        l_fin.append(lc(fin_wf.at[pl.ds(pl.multiple_of(R * c, 16), R), :], o_wf.at[slot_wf, c]))

    def at_head(h):
        for when, what in EVENTS:
            pl.when(h == when)(functools.partial(run_event, what))

    def run_event(what):
        {
            "wp0": lambda: wp_first(0),
            "wp1": lambda: wp_first(1),
            "wp2": lambda: wp_first(2),
            "wp3": lambda: wp_first(3),
            "wp_second": wp_second,
            "zf_first": zf_first,
            "zf_second": zf_second,
            "zf_third": zf_third,
            "wf_first0": lambda: wf_first(0),
            "wf_second0": lambda: wf_second(0),
            "wf_third0": lambda: wf_third(0),
            "wf_first1": lambda: wf_first(1),
            "wf_second1": lambda: wf_second(1),
            "wf_third1": lambda: wf_third(1),
        }[what]()

    KC = 256

    def head(h, carry):
        at_head(h)
        both = qo[h]
        top = jnp.full((8, T), -3e38, F32)
        for k in range(S // KC):
            rows = pl.ds(KC * k, KC)
            sd = mm(kv_all[rows, :], both, NT)
            score = sd[:, :T] + bias[rows, :]
            sbuf[rows, :] = score
            dbuf[rows, :] = sd[:, T:]
            top = jnp.maximum(top, jnp.max(score.reshape(KC // 8, 8, T), axis=0))
        top = jnp.max(top, axis=0, keepdims=True)
        norm = jnp.zeros((8, T), F32)
        delta = jnp.zeros((8, T), F32)
        for k in range(S // KC):
            rows = pl.ds(KC * k, KC)
            e = jnp.exp(sbuf[rows, :] - top)
            sbuf[rows, :] = e
            norm = norm + jnp.sum(e.reshape(KC // 8, 8, T), axis=0)
            delta = delta + jnp.sum((e * dbuf[rows, :]).reshape(KC // 8, 8, T), axis=0)
        scale = 1.0 / jnp.sum(norm, axis=0, keepdims=True)
        delta = jnp.sum(delta, axis=0, keepdims=True) * scale
        for k in range(S // KC):
            rows = pl.ds(KC * k, KC)
            p = sbuf[rows, :] * scale
            dsp[rows, :T] = (p * (dbuf[rows, :] - delta)).astype(BF16)
            dsp[rows, T:] = p.astype(BF16)
        for k in range(S // KC):
            rows = pl.ds(KC * k, KC)
            dkv[rows, :] += mm(dsp[rows, :], both)
        result = mm(kvt[...], dsp[...])
        rows = pl.ds(pl.multiple_of(HD * h, HD), HD)
        oht[rows, :] = result[HD:, T:].astype(BF16)
        back = result[:HD, :T] * 0.125
        a, b, rest = back[: ROT // 2], back[ROT // 2 : ROT], back[ROT:]
        ct, st = cost[...], sint[...]
        qgt[rows, :] = jnp.concatenate([a * ct + b * st, b * ct - a * st, rest], axis=0).astype(BF16)
        return carry

    lax.fori_loop(0, H, head, 0)

    def block_rows(k, core):
        return pl.ds(pl.multiple_of((2 * k + core) * T, T), T)

    dkv_b[...] = dkv[...].astype(BF16)
    s_dk = []
    for k in range(NZ):
        s_dk.append(rc("dk", k, dkv_b.at[block_rows(k, 1 - c), :], rdk.at[k], partner))
        send(s_dk[-1])

    s_ht = []
    for k in range(NZ):
        rows = pl.ds(pl.multiple_of(2 * R * k + R * (1 - c), 16), R)
        s_ht.append(rc("ht", k, oht.at[rows, :], ht_r.at[k], partner))
        send(s_ht[-1])
    qg2[own, :] = qgt[...].T
    s_qg = rc("qg", 0, qg2.at[own], qg2.at[other], partner)
    send(s_qg)

    for copy in s_dk:
        copy.wait_recv()
    s_dkv = []
    for o in range(1, NZ):
        k = lax.rem(z + o, NZ)
        dks[o] = (dkv[block_rows(k, c), :] + rdk[k].astype(F32)).astype(BF16)
        s_dkv.append(rc("dkv", o, dks.at[o], rdkv.at[o], z_peer(o)))
        send(s_dkv[-1])

    def put(name, row):
        at, count = rows_v[name]
        for i in range(count):
            vec[at + i : at + i + 1, :] = row[:, 128 * i : 128 * (i + 1)]

    for copy in s_ht:
        copy.wait_recv()
    for k in range(NZ):
        rows = pl.ds(pl.multiple_of(2 * R * k + R * c, 16), R)
        wo_part[k] = (mm(oht[rows, :], og2[own, :]) + mm(ht_r[k], og2[other, :])).astype(BF16)
    far_rx = pl.ds(pl.multiple_of(R // 2 * (1 - xx), 16), R // 2)
    far_ry = pl.ds(pl.multiple_of(R // 2 * (1 - yy), 16), R // 2)
    near_rx = pl.ds(pl.multiple_of(R // 2 * xx, 16), R // 2)
    near_ry = pl.ds(pl.multiple_of(R // 2 * yy, 16), R // 2)
    far_cx = pl.ds(pl.multiple_of(C2 * (1 - xx), 128), C2)
    far_cy = pl.ds(pl.multiple_of(C2 * (1 - yy), 128), C2)
    near_cx = pl.ds(pl.multiple_of(C2 * xx, 128), C2)
    near_cy = pl.ds(pl.multiple_of(C2 * yy, 128), C2)
    s_wox = rc("wox", 0, wo_part.at[:, far_rx, :], rx_wo, xnb)
    send(s_wox)
    s_qg.wait_recv()
    for k in range(NZ):
        rows = pl.ds(pl.multiple_of(2 * R * k + R * c, 16), R)
        wq_part[k] = mm(fit[rows, :], qg2[...]).astype(BF16)
    s_wqy = rc("wqy", 0, wq_part.at[:, far_ry, :], ry_wq, ynb)
    send(s_wqy)

    zf_third()

    s_mlp.wait_recv()
    for i in range(T // 128):
        rows = pl.ds(128 * i, 128)
        branch = mm(oht[:, rows], wo_v[...], TN) + vecs[5:6, :]
        mlp = (mlp_all[rows, :] + mlp_r[rows, :]) + vecs[6:7, :]
        lo_v[rows, :] = ((x2[rows, :].astype(F32) + branch) + mlp).astype(BF16)
    l_lo = lc(lo_v, o_lo)

    s_wox.wait_recv()
    wo_s1[...] = (wo_part[:, near_rx, :].astype(F32) + rx_wo[...].astype(F32)).astype(BF16)
    s_woy = rc("woy", 0, wo_s1.at[:, :, far_cy], ry_wo, ynb)
    send(s_woy)
    s_wqy.wait_recv()
    wq_s1[...] = (wq_part[:, near_ry, :].astype(F32) + ry_wq[...].astype(F32)).astype(BF16)
    s_wqx = rc("wqx", 0, wq_s1.at[:, :, far_cx], rx_wq, xnb)
    send(s_wqx)

    s_woy.wait_recv()
    zs_wo[...] = (wo_s1[:, :, near_cy].astype(F32) + ry_wo[...].astype(F32)).astype(BF16)
    s_woz = []
    for o in range(1, NZ):
        s_woz.append(rc("woz", o, zs_wo.at[lax.rem(z + o, NZ)], rz_wo.at[o], z_peer(o)))
        send(s_woz[-1])
    s_wqx.wait_recv()
    zs_wq[...] = (wq_s1[:, :, near_cx].astype(F32) + rx_wq[...].astype(F32)).astype(BF16)
    s_wqz = []
    for o in range(1, NZ):
        s_wqz.append(rc("wqz", o, zs_wq.at[lax.rem(z + o, NZ)], rz_wq.at[o], z_peer(o)))
        send(s_wqz[-1])

    wp_third()
    wf_fourth()

    l_kvg.wait()
    for copy in s_dkv:
        copy.wait_recv()
    kv_grads = []
    for i in range(T // 128):
        rows = pl.ds(128 * i, 128)
        total = dkv[pl.ds(pl.multiple_of(d * T + 128 * i, 128), 128), :] + rdk[z, rows, :].astype(F32)
        for o in range(1, NZ):
            total = total + rdkv[o, rows, :].astype(F32)
        total = total + kvg_v[rows, :].astype(F32)
        kv_grads.append(jnp.where(lanes < HD, turn(total, rows, -1.0), total).astype(BF16))
        kvg2[rows, :] = kv_grads[-1]
    s_kvg = rc("kvg", 0, kvg2.at[own], kvg2.at[other], partner)
    send(s_kvg)
    put("b_keyval", jnp.sum(jnp.concatenate(kv_grads, axis=0).astype(F32), axis=0, keepdims=True))

    s_sec.wait_recv()
    sums = [jnp.zeros((1, D), F32) for _ in range(6)]
    for i in range(T // 128):
        rows = pl.ds(128 * i, 128)
        first_grad = mm(qg2[rows, :], wq_v[...], NT) + mm(kv_grads[i], wkv_v[...], NT)
        second_grad = sec_all[rows, :] + sec_r[rows, :]
        n = nrm[rows, :]
        up = og2[rows, :].astype(F32)
        u = first_grad * g1 + second_grad * g2
        back = u - jnp.mean(u, axis=-1, keepdims=True) - n * jnp.mean(u * n, axis=-1, keepdims=True)
        ig_v[rows, :] = up + inv[rows, 0:1] * back
        for k, value in enumerate(
            (first_grad * n, first_grad, qg2[rows, :].astype(F32), up, second_grad * n, second_grad)
        ):
            sums[k] = sums[k] + jnp.sum(value, axis=0, keepdims=True)
    l_ig = lc(ig_v, o_ig)
    for name, row in zip(("ln1_gain", "ln1_bias", "b_query", "column", "ln2_gain", "ln2_bias"), sums):
        put(name, row)
    s_vec = []
    for o in range(1, NSP):
        rows = pl.ds(pl.multiple_of(lax.rem(d + o, NSP) * 8, 8), 8)
        s_vec.append(rc("vec", o, vec.at[rows, :], rvec.at[o], sp_peer(o)))
        send(s_vec[-1])

    s_kvg.wait_recv()
    s_wkv = []
    for k in range(NZ):
        rows = pl.ds(pl.multiple_of(2 * R * k + R * c, 16), R)
        wkv_part[k] = mm(fit[rows, :], kvg2[...])
        wkv_b[k] = wkv_part[k].astype(BF16)
    for o in range(1, NZ):
        s_wkv.append(rc("wkv", o, wkv_b.at[lax.rem(z + o, NZ)], rkv.at[o], z_peer(o)))
        send(s_wkv[-1])

    for copy in s_wkv:
        copy.wait_recv()
    total = wkv_part[z]
    for o in range(1, NZ):
        total = total + rkv[o].astype(F32)
    sm[g, :R, :] = total
    for copy in s_vec:
        copy.wait_recv()
    total = vec[pl.ds(pl.multiple_of(d * 8, 8), 8), :]
    for o in range(1, NSP):
        total = total + rvec[o]
    sm[g, R:, :] = total
    s_sm = [rc("sm", o, sm.at[g], sm.at[g], xy_peer(o, c)) for o in range(1, NG)]
    for copy in s_sm:
        send(copy)

    total = zs_wo[z].astype(F32)
    for o in range(1, NZ):
        s_woz[o - 1].wait_recv()
        total = total + rz_wo[o].astype(F32)
    fin_wo[...] = total.astype(BF16)
    s_wog = [rc("wog", o, fin_wo, o_wo.at[xx, yy], xy_peer(o, c)) for o in range(1, NG)]
    for copy in s_wog:
        send(copy)
    l_fo = lc(fin_wo, o_wo.at[xx, yy])
    total = zs_wq[z].astype(F32)
    for o in range(1, NZ):
        s_wqz[o - 1].wait_recv()
        total = total + rz_wq[o].astype(F32)
    fin_wq[...] = total.astype(BF16)
    s_wqg = [rc("wqg", o, fin_wq, o_wq.at[yy, xx], xy_peer(o, c)) for o in range(1, NG)]
    for copy in s_wqg:
        send(copy)
    l_fq = lc(fin_wq, o_wq.at[yy, xx])

    for copy in s_sm:
        copy.wait_recv()
    total = sm[0]
    for k in range(1, NG):
        total = total + sm[k]
    fin_kv[...] = total[:R]
    fin_vec[...] = total[R:]
    l_kv = lc(fin_kv, o_wkv)
    mine8 = pl.ds(pl.multiple_of(d * 8, 8), 8)
    s_vg = [rc("vg", o, fin_vec, o_vec.at[mine8, :], sp_peer(o)) for o in range(1, NSP)]
    for copy in s_vg:
        send(copy)
    l_vg = lc(fin_vec, o_vec.at[mine8, :])

    for o in range(1, NG):
        wp_g(o).wait_recv()
    for o in range(NG):
        for core in range(2):
            if o or core:
                wf_g(o, core).wait_recv()
    for copy in s_wog + s_wqg + s_vg:
        copy.wait_recv()
    for copy in started:
        copy.wait_send()
    for q in range(NZ):
        x_half(q).wait_send()
        wp_y(q).wait_send()
    for k in range(2):
        y_chunk(2 * (1 - yy) + k).wait_send()
        x_chunk(2 * k + 1 - xx).wait_send()
        wf_second_send(k).wait_send()
    zf_x.wait_send()
    zf_y.wait_send()
    for o in range(1, NZ):
        z_half(o).wait_send()
        wp_z(o).wait_send()
        wf_z(o).wait_send()
    for o in range(1, NG):
        wp_g(o).wait_send()
    for o in range(NG):
        for core in range(2):
            if o or core:
                wf_g(o, core).wait_send()
    for copy in l_fin + [l_lo, l_ig, l_kv, l_vg, l_fo, l_fq]:
        copy.wait()


EVENTS = (
    (0, "wp0"),
    (1, "wf_first0"),
    (1, "wf_first1"),
    (1, "wp1"),
    (2, "wf_second0"),
    (3, "wp2"),
    (5, "wf_second1"),
    (5, "wp3"),
    (6, "wf_third1"),
    (7, "wp_second"),
    (8, "wf_third0"),
    (9, "zf_first"),
    (11, "zf_second"),
)


def finish_kernel(
    dims, wp_h, wf_h, wo_h, wq_h, wkv_h, vec_h, lo_h, ig_h,
    layer_out, input_grad, ln1_gain, ln1_bias, w_query, b_query, w_keyval, b_keyval,
    w_attn_out, b_attn_out, ln2_gain, ln2_bias, w_fc, b_fc, w_proj, b_proj,
    wp, wf, wo, wq, wkv, vec, lo, ig, fc_v, proj_v, out_v, query_v, isem, osem,
):
    T, D, F, S, NSP, NG = dims
    Q, R, C2 = F // NSP, D // NSP, D // 2
    arrive = {}
    for i, (name, src, dst) in enumerate(
        (("wf", wf_h, wf), ("wp", wp_h, wp), ("ig", ig_h, ig), ("lo", lo_h, lo), ("vec", vec_h, vec),
         ("wo", wo_h, wo), ("wq", wq_h, wq), ("wkv", wkv_h, wkv))
    ):
        arrive[name] = pltpu.make_async_copy(src, dst, isem.at[i])
        arrive[name].start()
    leave = []

    def put_out(src, dst):
        leave.append(pltpu.make_async_copy(src, dst, osem.at[len(leave)]))
        leave[-1].start()

    arrive["wf"].wait()
    for k in range(NG):
        for core in range(2):
            at = Q * (2 * k + core)
            fc_v[:, at : at + Q] = wf[k, core].astype(F32)
    put_out(fc_v, w_fc)
    arrive["wp"].wait()
    rows = Q // 2 // NG
    for k in range(NG):
        for part in range(2):
            at = Q // 2 * part + rows * k
            proj_v[at : at + rows, :] = wp[k, part].astype(F32)
    put_out(proj_v, w_proj)
    arrive["ig"].wait()
    put_out(ig, input_grad)
    arrive["lo"].wait()
    put_out(lo, layer_out)
    arrive["wo"].wait()
    arrive["wq"].wait()
    for a in range(2):
        for b in range(2):
            rows = slice(R // 2 * a, R // 2 * (a + 1))
            cols = slice(C2 * b, C2 * (b + 1))
            out_v[rows, cols] = wo[a, b].astype(F32)
            query_v[rows, cols] = wq[a, b].astype(F32)
    put_out(out_v, w_attn_out)
    put_out(query_v, w_query)
    arrive["wkv"].wait()
    put_out(wkv, w_keyval)
    arrive["vec"].wait()
    rows_v, _ = vec_rows(D, F, 2 * HD)
    for name, out in (
        ("ln1_gain", ln1_gain), ("ln1_bias", ln1_bias), ("b_query", b_query), ("b_keyval", b_keyval),
        ("column", b_attn_out), ("column", b_proj), ("ln2_gain", ln2_gain), ("ln2_bias", ln2_bias),
        ("b_fc", b_fc),
    ):
        at, count = rows_v[name]
        out[...] = jnp.concatenate([vec[at + i : at + i + 1, :] for i in range(count)], axis=1).reshape(
            128 * count
        )
    for copy in leave:
        copy.wait()


def fused_local(n_grp, n_sp, *args):
    layer_input, block_order = args[0], args[1]
    T, D = layer_input.shape
    F = args[12].shape[1]
    S = T * n_sp
    NZ, NG, NSP = n_sp // 2, n_grp, n_sp
    Q, R, C2, pair = F // n_sp, D // n_sp, D // 2, 2 * HD
    dims = (T, D, F, S, NSP, NG)
    V = pltpu.VMEM
    scratch = [
        V((8, D), F32), V((1, pair), F32), V((1, F), F32),
        V((2 * T, D), BF16), V((2 * T, D), BF16), V((2 * T, D), BF16), V((2 * T, D), BF16),
        V((D, 2 * T), BF16), V((D, 2 * T), BF16), V((T, D), F32), V((T, 128), F32),
        V((D, pair), BF16), V((D, D), BF16), V((D, D), BF16), V((NZ, D, Q), BF16), V((NZ, Q, D), BF16),
        V((T, pair), BF16), V((NZ, 2 * T, Q), BF16), V((NZ, 2 * T, Q), BF16),
        V((2 * T, D), F32), V((2 * T, D), F32), V((T, D), F32), V((T, D), F32),
        V((NZ, Q, D), BF16), V((NZ, Q // 4, D), BF16), V((NZ, Q // 4, D), BF16), V((NZ, Q // 8, D), BF16),
        V((NZ, Q // 8, D), BF16), V((NZ, Q // 8, D), BF16), V((NZ, Q // 2, D), BF16), V((Q // 2, D), BF16),
        V((Q // 4, D), BF16), V((Q // 4, D), BF16), V((Q // 8, D), BF16), V((2, Q // 8, D), BF16),
        V((NZ, D, Q), BF16), V((2, D // 2, Q), BF16), V((2, D // 2, Q), BF16), V((2, D // 2, Q), BF16),
        V((2, D // 2, Q), BF16), V((2, D // 2, Q), BF16), V((D, Q), BF16), V((NZ, 2 * R, Q), BF16), V((2 * R, Q), BF16),
        V((S, pair), BF16), V((pair, S), BF16), V((H, 2 * T, pair), BF16), V((S, T), F32), V((S, T), F32),
        V((S, T), F32), V((S, 2 * T), BF16), V((S, pair), F32), V((S, pair), BF16), V((NZ, T, pair), BF16),
        V((NZ, T, pair), BF16), V((NZ, T, pair), BF16), V((2 * T, pair), BF16),
        V((D, T), BF16), V((D, T), BF16), V((NZ, R, T), BF16), V((2 * T, D), BF16),
        V((NZ, R, D), BF16), V((NZ, R // 2, D), BF16), V((NZ, R // 2, D), BF16), V((NZ, R // 2, C2), BF16),
        V((NZ, R // 2, C2), BF16), V((NZ, R // 2, C2), BF16), V((R // 2, C2), BF16),
        V((NZ, R, D), BF16), V((NZ, R // 2, D), BF16), V((NZ, R // 2, D), BF16), V((NZ, R // 2, C2), BF16),
        V((NZ, R // 2, C2), BF16), V((NZ, R // 2, C2), BF16), V((R // 2, C2), BF16),
        V((8 * NSP, 128), F32), V((NSP, 8, 128), F32), V((NZ, R, pair), F32), V((NZ, R, pair), BF16),
        V((NZ, R, pair), BF16), V((NG, R + 8, 128), F32), V((R, 128), F32), V((8, 128), F32),
        V((T, D), BF16), V((T, D), F32), V((T, pair), F32), V((T, pair), F32), V((8, T), F32), V((8, T), F32),
        pltpu.SemaphoreType.DMA((40,)), pltpu.SemaphoreType.DMA((128,)), pltpu.SemaphoreType.DMA((128,)),
    ]
    any_spec = pl.BlockSpec(memory_space=pl.ANY)
    shape = jax.ShapeDtypeStruct
    held = pl.pallas_call(
        functools.partial(fused_kernel, dims),
        out_shape=(
            shape((NG, 2, Q // 8, D), BF16),
            shape((NG, 2, R, Q), BF16),
            shape((2, 2, R // 2, C2), BF16),
            shape((2, 2, R // 2, C2), BF16),
            shape((R, pair), F32),
            shape((8 * NSP, 128), F32),
            shape((T, D), BF16),
            shape((T, D), F32),
        ),
        in_specs=[any_spec, pl.BlockSpec(memory_space=pltpu.SMEM)] + [any_spec] * 16,
        out_specs=(any_spec,) * 8,
        scratch_shapes=scratch,
        compiler_params=pltpu.CompilerParams(
            collective_id=0, has_side_effects=True, vmem_limit_bytes=67043328
        ),
        name="fused_layer",
    )(*args)
    vmem_spec = pl.BlockSpec(memory_space=pltpu.VMEM)
    row = shape((D,), F32)
    return pl.pallas_call(
        functools.partial(finish_kernel, dims),
        out_shape=(
            shape((T, D), BF16), shape((T, D), F32), row, row, shape((R, D), F32), row, shape((R, pair), F32),
            shape((pair,), F32), shape((R, D), F32), row, row, row, shape((R, F), F32), shape((F,), F32),
            shape((Q, D), F32), row,
        ),
        in_specs=[any_spec] * 8,
        out_specs=tuple(any_spec if k in (0, 1, 4, 6, 8, 12, 14) else vmem_spec for k in range(16)),
        scratch_shapes=[
            V((NG, 2, Q // 8, D), BF16), V((NG, 2, R, Q), BF16), V((2, 2, R // 2, C2), BF16),
            V((2, 2, R // 2, C2), BF16), V((R, pair), F32), V((8 * NSP, 128), F32), V((T, D), BF16), V((T, D), F32),
            V((R, F), F32), V((Q, D), F32), V((R, D), F32), V((R, D), F32),
            pltpu.SemaphoreType.DMA((8,)), pltpu.SemaphoreType.DMA((8,)),
        ],
        compiler_params=pltpu.CompilerParams(vmem_limit_bytes=64000000),
        name="finish",
    )(*held)


def fits(mesh, args):
    n_grp, n_sp = mesh.shape["grp"], mesh.shape["sp"]
    tokens, width = args[0].shape
    seqs, blocks = args[1].shape
    ff = args[12].shape[1]
    rows = tokens // (n_grp * n_sp)
    return (
        n_grp == 4
        and n_sp == 2 * n_grp
        and seqs == n_grp
        and blocks == 2 * n_sp
        and rows == 2 * 128
        and width == H * HD
        and width % (32 * n_sp) == 0
        and ff % (128 * n_sp) == 0
        and width % 128 == 0
        and sum(count for _, count in vec_rows(width, ff, 2 * HD)[0].values()) <= 8 * n_sp
    )


def layer_norm(values, gain_row, shift_row):
    centre = jnp.mean(values, axis=-1, keepdims=True)
    centred = values - centre
    spread = jnp.mean(centred * centred, axis=-1, keepdims=True)
    inverse_dev = lax.rsqrt(spread + norm_eps)
    normed = centred * inverse_dev
    return (normed * gain_row + shift_row, normed, inverse_dev)


def norm_back(upstream, normed, inverse_dev, gain_row):
    scaled = upstream * gain_row
    return inverse_dev * (
        scaled
        - jnp.mean(scaled, axis=-1, keepdims=True)
        - normed * jnp.mean(scaled * normed, axis=-1, keepdims=True)
    )


def rotary_tables(position):
    half_rot = ROT // 2
    frequency = jnp.exp(jnp.arange(half_rot, dtype=jnp.float32) * (-2.0 * rotary_base_log / ROT))
    angles = position.astype(jnp.float32)[:, None] * 0.25 * frequency[None, :]
    return (jnp.cos(angles), jnp.sin(angles))


def rotate(values, cosine, sine_table):
    half_rot = ROT // 2
    cos_rows = cosine[:, None, :]
    sin_rows = sine_table[:, None, :]
    lower_half = values[..., :half_rot]
    upper_half = values[..., half_rot:ROT]
    return jnp.concatenate(
        [
            lower_half * cos_rows - upper_half * sin_rows,
            upper_half * cos_rows + lower_half * sin_rows,
            values[..., ROT:],
        ],
        axis=-1,
    )


def rotate_back(values, cosine, sine_table):
    half_rot = ROT // 2
    cos_rows = cosine[:, None, :]
    sin_rows = sine_table[:, None, :]
    lower_half = values[..., :half_rot]
    upper_half = values[..., half_rot:ROT]
    return jnp.concatenate(
        [
            lower_half * cos_rows + upper_half * sin_rows,
            upper_half * cos_rows - lower_half * sin_rows,
            values[..., ROT:],
        ],
        axis=-1,
    )


def key_scores(query_rows, row_pos, kv_sequence, block_index, block_rows):
    key_start = block_index * block_rows
    key_slice = lax.dynamic_slice_in_dim(kv_sequence, key_start, block_rows, 0)
    raw_scores = (
        jnp.einsum("rd,kd->rk", query_rows, key_slice[:, :HD], preferred_element_type=jnp.float32)
        * 0.125
    )
    key_pos = key_start + lax.broadcasted_iota(jnp.int32, (1, block_rows), 1)
    return (jnp.where(key_pos <= row_pos[:, None], raw_scores, masked_score), key_slice)


def attention_forward(query_tiles, tile_pos, kv_sorted):
    pair_count = query_tiles.shape[0]
    pairs_per_seq = pair_count // kv_sorted.shape[0]
    block_rows = min(score_block, kv_sorted.shape[1])

    def one_pair(inputs):
        query_rows, row_pos, pair_index = inputs
        kv_sequence = kv_sorted[pair_index // pairs_per_seq]
        key_blocks = jnp.max(row_pos) // block_rows + 1
        row_count = query_rows.shape[0]

        def max_pass(block_index, carried):
            running_max, running_sum = carried
            masked, key_slice = key_scores(
                query_rows, row_pos, kv_sequence, block_index, block_rows
            )
            new_max = jnp.maximum(running_max, jnp.max(masked, axis=1, keepdims=True))
            running_sum = running_sum * jnp.exp(running_max - new_max) + jnp.sum(
                jnp.exp(masked - new_max), axis=1, keepdims=True
            )
            return (new_max, running_sum)

        start_max = jnp.full((row_count, 1), masked_score, jnp.float32)
        running_max, running_sum = lax.fori_loop(
            0, key_blocks, max_pass, (start_max, jnp.zeros((row_count, 1), jnp.float32))
        )
        log_total = running_max + jnp.log(running_sum)

        def value_pass(block_index, output):
            masked, key_slice = key_scores(
                query_rows, row_pos, kv_sequence, block_index, block_rows
            )
            weights = jnp.exp(masked - log_total).astype(jnp.bfloat16)
            return output + jnp.dot(weights, key_slice[:, HD:], preferred_element_type=jnp.float32)

        output = lax.fori_loop(0, key_blocks, value_pass, jnp.zeros((row_count, HD), jnp.float32))
        return (output, log_total)

    return lax.map(one_pair, (query_tiles, tile_pos, jnp.arange(pair_count, dtype=jnp.int32)))


def attention_backward(query_tiles, tile_pos, grad_tiles, log_totals, kv_sorted):
    pair_count = query_tiles.shape[0]
    pairs_per_seq = pair_count // kv_sorted.shape[0]
    block_rows = min(score_block, kv_sorted.shape[1])
    pair_width = kv_sorted.shape[2]

    def one_pair(key_grads, inputs):
        query_rows, row_pos, grad_rows, log_total, pair_index = inputs
        sequence = pair_index // pairs_per_seq
        kv_sequence = kv_sorted[sequence]
        key_blocks = jnp.max(row_pos) // block_rows + 1
        row_count = query_rows.shape[0]

        def pass_terms(block_index):
            masked, key_slice = key_scores(
                query_rows, row_pos, kv_sequence, block_index, block_rows
            )
            weights = jnp.exp(masked - log_total)
            weight_grads = jnp.einsum(
                "rd,kd->rk", grad_rows, key_slice[:, HD:], preferred_element_type=jnp.float32
            )
            return (weights, weight_grads, key_slice)

        def delta_pass(block_index, row_delta):
            weights, weight_grads, unused_slice = pass_terms(block_index)
            return row_delta + jnp.sum(weights * weight_grads, axis=1, keepdims=True)

        row_delta = lax.fori_loop(0, key_blocks, delta_pass, jnp.zeros((row_count, 1), jnp.float32))

        def grad_pass(block_index, carried):
            query_grad, sequence_grads = carried
            weights, weight_grads, key_slice = pass_terms(block_index)
            score_grad = (weights * (weight_grads - row_delta)).astype(jnp.bfloat16)
            query_grad = (
                query_grad
                + jnp.dot(score_grad, key_slice[:, :HD], preferred_element_type=jnp.float32) * 0.125
            )
            key_part = (
                jnp.einsum("rk,rd->kd", score_grad, query_rows, preferred_element_type=jnp.float32)
                * 0.125
            )
            value_part = jnp.einsum(
                "rk,rd->kd",
                weights.astype(jnp.bfloat16),
                grad_rows,
                preferred_element_type=jnp.float32,
            )
            key_start = block_index * block_rows
            previous = lax.dynamic_slice(
                sequence_grads, (sequence, key_start, 0), (1, block_rows, pair_width)
            )
            updated = previous + jnp.concatenate([key_part, value_part], axis=1)[None]
            return (
                query_grad,
                lax.dynamic_update_slice(sequence_grads, updated, (sequence, key_start, 0)),
            )

        query_grad, key_grads = lax.fori_loop(
            0, key_blocks, grad_pass, (jnp.zeros((row_count, HD), jnp.float32), key_grads)
        )
        return (key_grads, query_grad)

    start_grads = jnp.zeros(kv_sorted.shape, jnp.float32)
    key_grads, query_grads = lax.scan(
        one_pair,
        start_grads,
        (query_tiles, tile_pos, grad_tiles, log_totals, jnp.arange(pair_count, dtype=jnp.int32)),
    )
    return (query_grads, key_grads)


def local(
    layer_input,
    block_order,
    ln1_gain,
    ln1_bias,
    w_query,
    b_query,
    w_keyval,
    b_keyval,
    w_attn_out,
    b_attn_out,
    ln2_gain,
    ln2_bias,
    w_fc,
    b_fc,
    w_proj,
    b_proj,
    kv_grad,
    out_grad,
):
    my_rank = lax.axis_index("sp")
    seq_count = block_order.shape[0]
    block_count = block_order.shape[1]
    token_count = layer_input.shape[0]
    shard_len = token_count // seq_count
    block_len = shard_len // 2
    model_width = layer_input.shape[1]
    pair_width = 2 * HD
    pair_count = 2 * seq_count
    input_float = layer_input.astype(jnp.float32)
    first_in, first_hat, first_inv = layer_norm(input_float, ln1_gain, ln1_bias)
    first_low = first_in.astype(jnp.bfloat16)
    query_pre = jnp.dot(first_low, w_query, preferred_element_type=jnp.float32) + b_query
    keyval_pre = jnp.dot(first_low, w_keyval, preferred_element_type=jnp.float32) + b_keyval
    offsets = jnp.arange(block_len, dtype=jnp.int32)
    own_blocks = lax.dynamic_slice_in_dim(block_order, 2 * my_rank, 2, 1)
    own_pos = (own_blocks[:, :, None] * block_len + offsets[None, None, :]).reshape(token_count)
    cosine, sine_table = rotary_tables(own_pos)
    query_use = (
        rotate(query_pre.reshape(token_count, H, HD), cosine, sine_table)
        .reshape(token_count, model_width)
        .astype(jnp.bfloat16)
    )
    key_rot = rotate(keyval_pre[:, None, :HD], cosine, sine_table)[:, 0, :]
    keyval_use = jnp.concatenate([key_rot, keyval_pre[:, HD:]], axis=1).astype(jnp.bfloat16)
    gathered = lax.all_gather(
        keyval_use.reshape(seq_count, shard_len, pair_width), "sp", axis=1, tiled=True
    )
    seq_len = gathered.shape[1]
    block_sorter = jnp.argsort(block_order, axis=1)
    kv_sorted = jnp.take_along_axis(
        gathered.reshape(seq_count, block_count, block_len, pair_width),
        block_sorter[:, :, None, None],
        axis=1,
    ).reshape(seq_count, seq_len, pair_width)
    row_pos = own_pos.reshape(seq_count, shard_len)
    query_rows = query_use.reshape(seq_count, shard_len, model_width)
    query_tiles = query_rows.reshape(pair_count, block_len * H, HD)
    tile_pos = jnp.repeat(row_pos.reshape(pair_count, block_len), H, axis=1)
    head_rows, log_totals = attention_forward(query_tiles, tile_pos, kv_sorted)
    heads_sorted = head_rows.reshape(seq_count, shard_len, model_width).astype(jnp.bfloat16)
    heads_local = heads_sorted.reshape(token_count, model_width)
    attn_branch = jnp.dot(heads_local, w_attn_out, preferred_element_type=jnp.float32) + b_attn_out
    second_in, second_hat, second_inv = layer_norm(input_float, ln2_gain, ln2_bias)
    second_low = second_in.astype(jnp.bfloat16)
    hidden = jnp.dot(second_low, w_fc, preferred_element_type=jnp.float32) + b_fc
    erf_part = 1.0 + lax.erf(hidden * half_root)
    activated = (0.5 * hidden * erf_part).astype(jnp.bfloat16)
    mlp_branch = jnp.dot(activated, w_proj, preferred_element_type=jnp.float32) + b_proj
    layer_out = (input_float + attn_branch + mlp_branch).astype(jnp.bfloat16)
    upstream = out_grad.astype(jnp.float32)
    column_sum = jnp.sum(upstream, axis=0)
    w_proj_grad = jnp.einsum("tf,td->fd", activated, out_grad, preferred_element_type=jnp.float32)
    act_grad = jnp.einsum("td,fd->tf", out_grad, w_proj, preferred_element_type=jnp.float32)
    gelu_slope = 0.5 * erf_part + hidden * jnp.exp(-0.5 * hidden * hidden) * inv_root_tau
    hidden_grad = (act_grad * gelu_slope).astype(jnp.bfloat16)
    w_fc_grad = jnp.einsum("td,tf->df", second_low, hidden_grad, preferred_element_type=jnp.float32)
    b_fc_grad = jnp.sum(hidden_grad.astype(jnp.float32), axis=0)
    second_grad = jnp.einsum("tf,df->td", hidden_grad, w_fc, preferred_element_type=jnp.float32)
    w_attn_out_grad = jnp.einsum(
        "te,td->ed", heads_local, out_grad, preferred_element_type=jnp.float32
    )
    heads_grad = jnp.einsum(
        "td,ed->te", out_grad, w_attn_out, preferred_element_type=jnp.float32
    ).astype(jnp.bfloat16)
    grad_rows = heads_grad.reshape(seq_count, shard_len, model_width)
    grad_tiles = grad_rows.reshape(pair_count, block_len * H, HD)
    query_tile_grads, sorted_kv_grads = attention_backward(
        query_tiles, tile_pos, grad_tiles, log_totals, kv_sorted
    )
    query_rot_rows = query_tile_grads.reshape(seq_count, shard_len, model_width)
    query_rot_grad = query_rot_rows.reshape(token_count, model_width)
    query_grad = (
        rotate_back(query_rot_grad.reshape(token_count, H, HD), cosine, sine_table)
        .reshape(token_count, model_width)
        .astype(jnp.bfloat16)
    )
    stored_kv_grads = jnp.take_along_axis(
        sorted_kv_grads.reshape(seq_count, block_count, block_len, pair_width),
        block_order[:, :, None, None],
        axis=1,
    ).reshape(seq_count, seq_len, pair_width)
    own_kv_grad = lax.psum_scatter(stored_kv_grads, "sp", scatter_dimension=1, tiled=True).reshape(
        token_count, pair_width
    ) + kv_grad.astype(jnp.float32)
    key_pre_grad = rotate_back(own_kv_grad[:, None, :HD], cosine, sine_table)[:, 0, :]
    keyval_grad = jnp.concatenate([key_pre_grad, own_kv_grad[:, HD:]], axis=1).astype(jnp.bfloat16)
    w_query_grad = jnp.einsum(
        "td,te->de", first_low, query_grad, preferred_element_type=jnp.float32
    )
    b_query_grad = jnp.sum(query_grad.astype(jnp.float32), axis=0)
    w_keyval_grad = jnp.einsum(
        "td,te->de", first_low, keyval_grad, preferred_element_type=jnp.float32
    )
    b_keyval_grad = jnp.sum(keyval_grad.astype(jnp.float32), axis=0)
    first_grad = jnp.einsum(
        "te,de->td", query_grad, w_query, preferred_element_type=jnp.float32
    ) + jnp.einsum("te,de->td", keyval_grad, w_keyval, preferred_element_type=jnp.float32)
    first_back = norm_back(first_grad, first_hat, first_inv, ln1_gain)
    second_back = norm_back(second_grad, second_hat, second_inv, ln2_gain)
    input_grad = upstream + first_back + second_back
    (
        ln1_gain_grad,
        ln1_bias_grad,
        b_query_total,
        b_keyval_total,
        bias_out_total,
        ln2_gain_grad,
        ln2_bias_grad,
        b_fc_total,
    ) = lax.psum(
        (
            jnp.sum(first_grad * first_hat, axis=0),
            jnp.sum(first_grad, axis=0),
            b_query_grad,
            b_keyval_grad,
            column_sum,
            jnp.sum(second_grad * second_hat, axis=0),
            jnp.sum(second_grad, axis=0),
            b_fc_grad,
        ),
        ("grp", "sp"),
    )
    query_share, keyval_share, out_share, fc_share, proj_share = (
        lax.psum_scatter(w_query_grad, "sp", scatter_dimension=0, tiled=True),
        lax.psum_scatter(w_keyval_grad, "sp", scatter_dimension=0, tiled=True),
        lax.psum_scatter(w_attn_out_grad, "sp", scatter_dimension=0, tiled=True),
        lax.psum_scatter(w_fc_grad, "sp", scatter_dimension=0, tiled=True),
        lax.psum_scatter(w_proj_grad, "sp", scatter_dimension=0, tiled=True),
    )
    query_total, keyval_total, out_total, fc_total, proj_total = lax.psum(
        (query_share, keyval_share, out_share, fc_share, proj_share), "grp"
    )
    return (
        layer_out,
        input_grad,
        ln1_gain_grad,
        ln1_bias_grad,
        query_total,
        b_query_total,
        keyval_total,
        b_keyval_total,
        out_total,
        bias_out_total,
        ln2_gain_grad,
        ln2_bias_grad,
        fc_total,
        b_fc_total,
        proj_total,
        bias_out_total,
    )


def solution(mesh):
    placed = (
        P(("grp", "sp"), None),
        P("grp", None),
        P(),
        P(),
        P(),
        P(),
        P(),
        P(),
        P(),
        P(),
        P(),
        P(),
        P(),
        P(),
        P(),
        P(),
        P(("grp", "sp"), None),
        P(("grp", "sp"), None),
    )
    def step(*args):
        if fits(mesh, args):
            body = functools.partial(fused_local, mesh.shape["grp"], mesh.shape["sp"])
        else:
            body = local
        return spread(body)(*args)

    def spread(body):
        return jax.shard_map(
            body,
            mesh=mesh,
            in_specs=placed,
            out_specs=(
                P(("grp", "sp"), None),
                P(("grp", "sp"), None),
                P(),
                P(),
                P("sp", None),
                P(),
                P("sp", None),
                P(),
                P("sp", None),
                P(),
                P(),
                P(),
                P("sp", None),
                P(),
                P("sp", None),
                P(),
            ),
            check_vma=False,
        )

    return step
```

```python
import functools
import math

import jax
import jax.numpy as jnp
from jax import lax
from jax.experimental import pallas as pl
from jax.experimental.pallas import tpu as pltpu
from jax.sharding import PartitionSpec as P

H = 12
HD = 64
ROT = 16
MESH = pl.DeviceIdType.MESH
F32 = jnp.float32
BF16 = jnp.bfloat16
NN = (((1,), (0,)), ((), ()))
NT = (((1,), (1,)), ((), ()))
TN = (((0,), (0,)), ((), ()))


def mm(a, b, dims=NN):
    return lax.dot_general(a, b, dims, preferred_element_type=F32)

norm_eps = 1e-05
half_root = 0.7071067811865476
inv_root_tau = 0.3989422804014327
masked_score = -1e30
rotary_base_log = math.log(10000.0)
score_block = 512


def vec_rows(width, ff, pair):
    names = ("ln1_gain", "ln1_bias", "b_query", "b_keyval", "column", "ln2_gain", "ln2_bias", "b_fc")
    sizes = (width, width, width, pair, width, width, width, ff)
    at, rows = 0, {}
    for name, size in zip(names, sizes):
        rows[name] = (at, size // 128)
        at += size // 128
    return rows, at


def fused_kernel(
    dims,
    x_h,
    order_s,
    g1_h,
    b1_h,
    wq_h,
    bq_h,
    wkv_h,
    bkv_h,
    wo_h,
    bo_h,
    g2_h,
    b2_h,
    wfc_h,
    bfc_h,
    wpr_h,
    bpr_h,
    kvg_h,
    og_h,
    o_wp,
    o_wf,
    o_wo,
    o_wq,
    o_wkv,
    o_vec,
    o_lo,
    o_ig,
    vecs,
    bkv_v,
    bfc_v,
    x2,
    og2,
    fi2,
    si2,
    fit,
    sit,
    nrm,
    inv,
    wkv_v,
    wq_v,
    wo_v,
    wfc_v,
    wpr_v,
    kvg_v,
    act_s,
    hg_s,
    mlp_all,
    sec_all,
    mlp_r,
    sec_r,
    wp_part,
    rx_wp,
    wp_s1,
    ry_wp,
    zs_wp,
    rz_wp,
    rzf,
    zf_s0,
    rx_zf,
    zf_s1,
    ry_zf,
    fin_wp,
    wf_part,
    ry_wf,
    rx_wf,
    wf_s1,
    wf_own,
    wf_in,
    zs_wf,
    rz_wf,
    fin_wf,
    kv_all,
    kvt,
    qo,
    bias,
    sbuf,
    dbuf,
    dsp,
    dkv,
    dkv_b,
    rdk,
    dks,
    rdkv,
    kvg2,
    oht,
    qgt,
    ht_r,
    qg2,
    wo_part,
    rx_wo,
    wo_s1,
    ry_wo,
    zs_wo,
    rz_wo,
    fin_wo,
    wq_part,
    ry_wq,
    wq_s1,
    rx_wq,
    zs_wq,
    rz_wq,
    fin_wq,
    vec,
    rvec,
    wkv_part,
    wkv_b,
    rkv,
    sm,
    fin_kv,
    fin_vec,
    lo_v,
    ig_v,
    ctab,
    stab,
    cost,
    sint,
    lsem,
    ssem,
    rsem,
):
    T, D, F, S, NSP, NG = dims
    NZ = NSP // 2
    D2 = D // 2
    Q = F // NSP
    QH = Q // 2
    R = D // NSP
    C2 = D // 2
    pair = 2 * HD
    g = lax.axis_index("grp")
    d = lax.axis_index("sp")
    c = lax.rem(d, 2)
    z = lax.div(d, 2)
    xx = lax.rem(g, 2)
    yy = lax.div(g, 2)
    partner = (g, d + 1 - 2 * c)
    xnb = (g + 1 - 2 * xx, d)
    ynb = (g + 2 - 4 * yy, d)

    def sp_peer(o):
        return (g, lax.rem(d + o, NSP))

    def z_peer(o):
        return (g, 2 * lax.rem(z + o, NZ) + c)

    def xy_peer(o, core):
        return (lax.rem(g + o, NG), 2 * z + core)

    base = {}
    used = [0]

    def take(name, n):
        base[name] = used[0]
        used[0] += n

    for name, n in (
        ("x", 1), ("og", 1), ("kv", NSP), ("mlp", 1), ("sec", 1),
        ("wpx", NZ), ("wpy", NZ), ("wpz", NZ), ("wpg", NG),
        ("wpf", NZ), ("zfx", 1), ("zfy", 1),
        ("wfy", 2), ("wfx", 2), ("wfs", 2), ("wfz", NZ), ("wfg", 2 * NG),
        ("ht", NZ), ("qg", H // 4), ("dk", NZ), ("dkv", NZ), ("kvg", 1),
        ("wox", NZ), ("woy", NZ), ("woz", NZ), ("wog", NG),
        ("wqy", H // 4), ("wqx", H // 4), ("wqz", NZ * (H // 4)), ("wqg", NG),
        ("wkv", NZ), ("vec", NSP), ("sm", NG), ("vg", NSP),
    ):
        take(name, n)

    def rc(name, i, src, dst, to):
        k = base[name] + i
        return pltpu.make_async_remote_copy(
            src_ref=src,
            dst_ref=dst,
            send_sem=ssem.at[k],
            recv_sem=rsem.at[k],
            device_id=to,
            device_id_type=MESH,
        )

    started = []

    def send(copy):
        copy.start()
        started.append(copy)

    lused = [0]

    def lc(src, dst):
        copy = pltpu.make_async_copy(src, dst, lsem.at[lused[0]])
        lused[0] += 1
        copy.start()
        return copy

    def chunk_of(j):
        far_y = lax.div(j, 2) == 0
        far_x = lax.rem(j, 2) == 0
        return 2 * jnp.where(far_y, 1 - yy, yy) + jnp.where(far_x, 1 - xx, xx)

    def chunk_in(j):
        far_y = lax.div(j, 2) == 0
        far_x = lax.rem(j, 2) == 0
        return 2 * jnp.where(far_y, 1 - yy, yy) + jnp.where(far_x, xx, 1 - xx)

    own = pl.ds(0, T)
    other = pl.ds(T, T)
    l_x = lc(x_h, x2.at[own])
    l_og = lc(og_h, og2.at[own])
    l_wkv = lc(wkv_h, wkv_v)
    l_vec = [
        lc(src, vecs.at[i]) for i, src in enumerate((g1_h, b1_h, g2_h, b2_h, bq_h, bo_h, bpr_h))
    ]
    l_bkv = lc(bkv_h, bkv_v.at[0])
    l_bfc = lc(bfc_h, bfc_v.at[0])
    l_mlp = []
    for j in range(NZ):
        q = chunk_of(j)
        cols = pl.ds(pl.multiple_of(Q * (2 * q + c), 128), Q)
        rows = pl.ds(pl.multiple_of(Q * (2 * q + c), 16), Q)
        l_mlp.append((lc(wfc_h.at[:, cols], wfc_v.at[q]), lc(wpr_h.at[rows, :], wpr_v.at[q])))
    l_wq = lc(wq_h, wq_v)
    l_wo = lc(wo_h, wo_v)
    l_kvg = lc(kvg_h, kvg_v)

    barrier = pltpu.get_barrier_semaphore()
    for o in range(1, NSP):
        pl.semaphore_signal(barrier, inc=1, device_id=sp_peer(o), device_id_type=MESH)
    for o in range(1, NG):
        for core in range(2):
            pl.semaphore_signal(barrier, inc=1, device_id=xy_peer(o, core), device_id_type=MESH)
    pl.semaphore_wait(barrier, NSP - 1 + 2 * (NG - 1))

    s_x = rc("x", 0, x_h, x2.at[other], partner)
    send(s_x)
    s_og = rc("og", 0, og_h, og2.at[other], partner)
    send(s_og)

    lane = lax.broadcasted_iota(jnp.int32, (8, T), 1)
    half = lax.broadcasted_iota(jnp.int32, (8, T), 0).astype(F32)
    block = T // 2
    first_block = order_s[0, 2 * d]
    second_block = order_s[0, 2 * d + 1]
    own_pos = jnp.where(
        lane < block, first_block * block + lane, second_block * block + (lane - block)
    )
    frequency = jnp.exp(half * (-2.0 * rotary_base_log / ROT))
    angle = own_pos.astype(F32) * 0.25 * frequency
    cosine, sine = jnp.cos(angle), jnp.sin(angle)
    cost[...] = cosine
    sint[...] = sine
    ones = jnp.ones((HD - ROT, T), F32)
    zeros = jnp.zeros((HD - ROT, T), F32)
    ctab[...] = jnp.concatenate([cosine, cosine, ones] * 2, axis=0).T
    stab[...] = jnp.concatenate([-sine, sine, zeros] * 2, axis=0).T
    lanes = lax.broadcasted_iota(jnp.int32, (128, pair), 1)
    low_half = lax.rem(lanes, HD) < ROT // 2

    def turn(tile, rows, sign):
        mixed = jnp.where(low_half, pltpu.roll(tile, pair - ROT // 2, 1), pltpu.roll(tile, ROT // 2, 1))
        return tile * ctab[rows, :] + (sign * mixed) * stab[rows, :]

    for copy in l_vec:
        copy.wait()
    l_bkv.wait()
    l_bfc.wait()
    g1, b1, g2, b2 = (vecs[i : i + 1, :] for i in range(4))
    vec[...] = jnp.zeros_like(vec)

    def norms(at, keep):
        for i in range(T // 128):
            rows = pl.ds(at + 128 * i, 128)
            v = x2[rows, :].astype(F32)
            centred = v - jnp.mean(v, axis=-1, keepdims=True)
            r = lax.rsqrt(jnp.mean(centred * centred, axis=-1, keepdims=True) + norm_eps)
            n = centred * r
            first = (n * g1 + b1).astype(BF16)
            second = (n * g2 + b2).astype(BF16)
            fi2[rows, :] = first
            si2[rows, :] = second
            fit[:, rows] = first.T
            sit[:, rows] = second.T
            if keep:
                nrm[rows, :] = n
                inv[rows, :] = jnp.broadcast_to(r, (128, 128))

    l_x.wait()
    norms(0, True)

    l_wkv.wait()
    for i in range(T // 128):
        rows = pl.ds(128 * i, 128)
        kv = mm(fi2[rows, :], wkv_v[...]) + bkv_v[...]
        kv = jnp.where(lanes < HD, turn(kv, rows, 1.0), kv)
        kv_all[pl.ds(pl.multiple_of(d * T + 128 * i, 128), 128), :] = kv.astype(BF16)
    mine = pl.ds(pl.multiple_of(d * T, T), T)
    s_kv = [rc("kv", o, kv_all.at[mine], kv_all.at[mine], sp_peer(o)) for o in range(1, NSP)]
    for copy in s_kv:
        send(copy)

    s_x.wait_recv()
    norms(T, False)
    l_og.wait()
    s_og.wait_recv()

    rows_v, _ = vec_rows(D, F, pair)
    for pair_of_copies in l_mlp:
        for copy in pair_of_copies:
            copy.wait()

    def x_half(q):
        far = pl.ds(pl.multiple_of(QH // 2 * (1 - xx), 16), QH // 2)
        return rc("wpx", q, wp_part.at[q, far, :], rx_wp.at[q], xnb)

    def z_half(o):
        q = lax.rem(z + o, NZ)
        return rc("wpf", o, wp_part.at[q, pl.ds(QH, QH), :], rzf.at[o], z_peer(o))

    def y_chunk(q):
        side = lax.rem(q, 2)
        return rc("wfy", side, wf_part.at[q, pl.ds(0, D2), :], ry_wf.at[side], ynb)

    def x_chunk(q):
        side = lax.div(q, 2)
        return rc("wfx", side, wf_part.at[q, pl.ds(D2, D2), :], rx_wf.at[side], xnb)

    def start_z_half(o):
        z_half(o).start()

    def mlp_chunk(j, carry):
        q = chunk_of(j)
        at = pl.ds(pl.multiple_of(Q * (2 * q + c), 128), Q)
        shift = bfc_v[:, at]
        total = jnp.zeros((1, Q), F32)
        for i in range(2 * T // 128):
            rows = pl.ds(128 * i, 128)
            hidden = mm(si2[rows, :], wfc_v[q]) + shift
            erf_part = 1.0 + lax.erf(hidden * half_root)
            act_s[q, rows, :] = (0.5 * hidden * erf_part).astype(BF16)
            slope = 0.5 * erf_part + hidden * jnp.exp(-0.5 * hidden * hidden) * inv_root_tau
            act_grad = mm(og2[rows, :], wpr_v[q], NT)
            hidden_grad = (act_grad * slope).astype(BF16)
            hg_s[q, rows, :] = hidden_grad
            total = total + jnp.sum(hidden_grad.astype(F32), axis=0, keepdims=True)
        for i in range(Q // 128):
            cols = pl.ds(128 * i, 128)
            wp_part[q, cols, :] = mm(act_s[q, :, cols], og2[...], TN).astype(BF16)
        x_half(q).start()
        for o in range(1, NZ):
            pl.when(lax.rem(z + o, NZ) == q)(functools.partial(start_z_half, o))
        for i in range(D // 128):
            rows = pl.ds(128 * i, 128)
            wf_part[q, rows, :] = mm(sit[rows, :], hg_s[q]).astype(BF16)

        @pl.when(j < 2)
        def _():
            y_chunk(q).start()

        @pl.when(lax.rem(j, 2) == 0)
        def _():
            x_chunk(q).start()

        at_row = rows_v["b_fc"][0] + Q // 128 * (2 * q + c)
        for i in range(Q // 128):
            vec[pl.ds(at_row + i, 1), :] = total[:, 128 * i : 128 * (i + 1)]
        return carry

    lax.fori_loop(0, NZ, mlp_chunk, 0)

    def mlp_sums(i, carry):
        at = lax.rem(i + T // 128, 2 * T // 128) * 128
        rows = pl.ds(pl.multiple_of(at, 128), 128)
        out = mm(act_s[0, rows, :], wpr_v[0])
        back = mm(hg_s[0, rows, :], wfc_v[0], NT)
        for q in range(1, NZ):
            out = out + mm(act_s[q, rows, :], wpr_v[q])
            back = back + mm(hg_s[q, rows, :], wfc_v[q], NT)
        mlp_all[rows, :] = out
        sec_all[rows, :] = back
        return carry

    lax.fori_loop(0, 2 * T // 128, mlp_sums, 0)
    s_mlp = rc("mlp", 0, mlp_all.at[other], mlp_r, partner)
    send(s_mlp)
    s_sec = rc("sec", 0, sec_all.at[other], sec_r, partner)
    send(s_sec)

    l_wq.wait()
    l_wo.wait()
    for i in range(T // 128):
        rows = pl.ds(128 * i, 128)
        query = mm(fi2[rows, :], wq_v[...]) + vecs[4:5, :]
        grads = mm(og2[rows, :], wo_v[...], NT)
        for t in range(D // pair):
            q_tile = turn(query[:, pair * t : pair * (t + 1)], rows, 1.0).astype(BF16).astype(F32) * 0.125
            o_tile = grads[:, pair * t : pair * (t + 1)]
            low = lanes < HD
            qo[2 * t, rows, :] = jnp.where(low, q_tile, 0.0).astype(BF16)
            qo[2 * t + 1, rows, :] = jnp.where(low, pltpu.roll(q_tile, HD, 1), 0.0).astype(BF16)
            late = pl.ds(T + 128 * i, 128)
            qo[2 * t, late, :] = jnp.where(low, 0.0, pltpu.roll(o_tile, HD, 1)).astype(BF16)
            qo[2 * t + 1, late, :] = jnp.where(low, 0.0, o_tile).astype(BF16)

    row_in = lax.broadcasted_iota(jnp.int32, (block, T), 0)
    query_pos = jnp.broadcast_to(own_pos[0:1, :], (block, T))
    for j in range(S // block):
        key_pos = order_s[0, j] * block + row_in
        bias[pl.ds(block * j, block), :] = jnp.where(key_pos <= query_pos, 0.0, masked_score)

    for copy in s_kv:
        copy.wait_recv()
    for j in range(S // 256):
        rows = pl.ds(256 * j, 256)
        kvt[:, rows] = kv_all[rows, :].T
        dkv[rows, :] = jnp.zeros((256, pair), F32)

    near_x = pl.ds(pl.multiple_of(QH // 2 * xx, 16), QH // 2)
    near_y = pl.ds(pl.multiple_of(QH // 4 * yy, 16), QH // 4)
    far_y = pl.ds(pl.multiple_of(QH // 4 * (1 - yy), 16), QH // 4)

    def wp_y(q):
        return rc("wpy", q, wp_s1.at[q, far_y, :], ry_wp.at[q], ynb)

    def wp_first(j):
        q = chunk_in(j)
        x_half(q).wait_recv()
        wp_s1[q] = (wp_part[q, near_x, :].astype(F32) + rx_wp[q].astype(F32)).astype(BF16)
        wp_y(q).start()

    def wp_z(o):
        return rc("wpz", o, zs_wp.at[lax.rem(z + o, NZ)], rz_wp.at[o], z_peer(o))

    def wp_second():
        for q in range(NZ):
            wp_y(q).wait_recv()
            zs_wp[q] = (wp_s1[q, near_y, :].astype(F32) + ry_wp[q].astype(F32)).astype(BF16)
        for o in range(1, NZ):
            wp_z(o).start()

    slot_wp = 2 * xx + yy

    def wp_g(o):
        return rc("wpg", o, fin_wp, o_wp.at[slot_wp], xy_peer(o, c))

    l_fin = []

    far_zx = pl.ds(pl.multiple_of(QH // 2 * (1 - xx), 16), QH // 2)
    zf_x = rc("zfx", 0, zf_s0.at[far_zx, :], rx_zf, xnb)
    zf_y = rc("zfy", 0, zf_s1.at[far_y, :], ry_zf, ynb)

    def zf_first():
        total = wp_part[z, QH:, :].astype(F32)
        for o in range(1, NZ):
            z_half(o).wait_recv()
            total = total + rzf[o].astype(F32)
        zf_s0[...] = total.astype(BF16)
        zf_x.start()

    def zf_second():
        zf_x.wait_recv()
        zf_s1[...] = (zf_s0[near_x, :].astype(F32) + rx_zf[...].astype(F32)).astype(BF16)
        zf_y.start()

    def zf_third():
        zf_y.wait_recv()
        fin_wp[1] = (zf_s1[near_y, :].astype(F32) + ry_zf[...].astype(F32)).astype(BF16)

    def wp_third():
        total = zs_wp[z].astype(F32)
        for o in range(1, NZ):
            wp_z(o).wait_recv()
            total = total + rz_wp[o].astype(F32)
        fin_wp[0] = total.astype(BF16)
        for o in range(1, NG):
            wp_g(o).start()
        l_fin.append(lc(fin_wp, o_wp.at[slot_wp]))

    def wf_second_send(part):
        return rc("wfs", part, wf_s1.at[part], wf_in.at[part], ynb if part else xnb)

    def wf_first(part):
        if part:
            q = 2 * (1 - yy) + xx
            x_chunk(2 * (1 - yy) + 1 - xx).wait_recv()
            got = rx_wf[1 - yy]
        else:
            q = 2 * yy + 1 - xx
            y_chunk(2 * (1 - yy) + 1 - xx).wait_recv()
            got = ry_wf[1 - xx]
        wf_s1[part] = (wf_part[q, D2 * part : D2 * (part + 1), :].astype(F32) + got.astype(F32)).astype(BF16)
        wf_second_send(part).start()

    def wf_second(part):
        q = 2 * yy + xx
        if part:
            x_chunk(2 * yy + 1 - xx).wait_recv()
            got = rx_wf[yy]
        else:
            y_chunk(2 * (1 - yy) + xx).wait_recv()
            got = ry_wf[xx]
        wf_own[part] = (wf_part[q, D2 * part : D2 * (part + 1), :].astype(F32) + got.astype(F32)).astype(BF16)

    def wf_z(o):
        rows = pl.ds(pl.multiple_of(2 * R * lax.rem(z + o, NZ), 16), 2 * R)
        return rc("wfz", o, zs_wf.at[rows, :], rz_wf.at[o], z_peer(o))

    def start_wf_z(o):
        wf_z(o).start()

    def wf_third(part):
        wf_second_send(part).wait_recv()
        zs_wf[D2 * part : D2 * (part + 1), :] = (
            wf_own[part].astype(F32) + wf_in[part].astype(F32)
        ).astype(BF16)
        for o in range(1, NZ):
            pl.when(lax.div(lax.rem(z + o, NZ), NZ // 2) == part)(functools.partial(start_wf_z, o))

    slot_wf = 2 * yy + xx

    def wf_g(o, core):
        to = c + core - 2 * c * core
        rows = pl.ds(pl.multiple_of(R * to, 16), R)
        return rc("wfg", 2 * o + core, fin_wf.at[rows, :], o_wf.at[slot_wf, c], xy_peer(o, to))

    def wf_fourth():
        total = zs_wf[pl.ds(pl.multiple_of(2 * R * z, 16), 2 * R), :].astype(F32)
        for o in range(1, NZ):
            wf_z(o).wait_recv()
            total = total + rz_wf[o].astype(F32)
        fin_wf[...] = total.astype(BF16)
        for o in range(NG):
            for core in range(2):
                if o or core:
                    wf_g(o, core).start()
        l_fin.append(lc(fin_wf.at[pl.ds(pl.multiple_of(R * c, 16), R), :], o_wf.at[slot_wf, c]))

    far_rx = pl.ds(pl.multiple_of(R // 2 * (1 - xx), 16), R // 2)
    far_ry = pl.ds(pl.multiple_of(R // 2 * (1 - yy), 16), R // 2)
    near_rx = pl.ds(pl.multiple_of(R // 2 * xx, 16), R // 2)
    near_ry = pl.ds(pl.multiple_of(R // 2 * yy, 16), R // 2)
    far_cy = pl.ds(pl.multiple_of(C2 * (1 - yy), 128), C2)
    near_cy = pl.ds(pl.multiple_of(C2 * yy, 128), C2)
    GC = 4 * HD

    def owner_rows(k, core):
        return pl.ds(pl.multiple_of(2 * R * k + R * core, 16), R)

    def group_cols(m):
        return pl.ds(GC * m, GC)

    def side_cols(m, side):
        return pl.ds(pl.multiple_of(GC * m + GC // 2 * side, 128), GC // 2)

    def r_ht(k):
        return rc("ht", k, oht.at[owner_rows(k, 1 - c), :], ht_r.at[k], partner)

    def r_wox(k):
        return rc("wox", k, wo_part.at[k, far_rx, :], rx_wo.at[k], xnb)

    def r_woy(k):
        return rc("woy", k, wo_s1.at[k, :, far_cy], ry_wo.at[k], ynb)

    def r_woz(o):
        return rc("woz", o, zs_wo.at[lax.rem(z + o, NZ)], rz_wo.at[o], z_peer(o))

    def r_qg(m):
        return rc("qg", m, qg2.at[own, group_cols(m)], qg2.at[other, group_cols(m)], partner)

    def r_wqy(m):
        return rc("wqy", m, wq_part.at[:, far_ry, group_cols(m)], ry_wq.at[:, :, group_cols(m)], ynb)

    def r_wqx(m):
        return rc("wqx", m, wq_s1.at[:, :, side_cols(m, 1 - xx)], rx_wq.at[m], xnb)

    def r_wqz(o, m):
        cols = pl.ds(GC // 2 * m, GC // 2)
        return rc(
            "wqz", NZ * m + o, zs_wq.at[lax.rem(z + o, NZ), :, cols], rz_wq.at[o, :, cols], z_peer(o)
        )

    def ht_send(k):
        r_ht(k).start()

    def wo_a(k):
        r_ht(k).wait_recv()
        total = mm(oht[owner_rows(k, c), :], og2[own, :]) + mm(ht_r[k], og2[other, :])
        wo_part[k] = total.astype(BF16)
        r_wox(k).start()

    def wo_b(k):
        r_wox(k).wait_recv()
        wo_s1[k] = (wo_part[k, near_rx, :].astype(F32) + rx_wo[k].astype(F32)).astype(BF16)
        r_woy(k).start()

    def start_woz(o):
        r_woz(o).start()

    def wo_c(k):
        r_woy(k).wait_recv()
        zs_wo[k] = (wo_s1[k, :, near_cy].astype(F32) + ry_wo[k].astype(F32)).astype(BF16)
        for o in range(1, NZ):
            pl.when(lax.rem(z + o, NZ) == k)(functools.partial(start_woz, o))

    def qg_send(m):
        qg2[own, group_cols(m)] = qgt[group_cols(m), :].T
        r_qg(m).start()

    def wq_a(m):
        r_qg(m).wait_recv()
        for k in range(NZ):
            wq_part[k, :, group_cols(m)] = mm(fit[owner_rows(k, c), :], qg2[:, group_cols(m)]).astype(BF16)
        r_wqy(m).start()

    def wq_b(m):
        r_wqy(m).wait_recv()
        cols = group_cols(m)
        wq_s1[:, :, cols] = (wq_part[:, near_ry, cols].astype(F32) + ry_wq[:, :, cols].astype(F32)).astype(BF16)
        r_wqx(m).start()

    def wq_c(m):
        r_wqx(m).wait_recv()
        mine_cols = side_cols(m, xx)
        zs_wq[:, :, GC // 2 * m : GC // 2 * (m + 1)] = (
            wq_s1[:, :, mine_cols].astype(F32) + rx_wq[m].astype(F32)
        ).astype(BF16)
        for o in range(1, NZ):
            r_wqz(o, m).start()

    def at_head(h):
        for when, what in EVENTS:
            pl.when(h == when)(functools.partial(run_event, what))

    def run_event(what):
        {
            "wp0": lambda: wp_first(0),
            "wp1": lambda: wp_first(1),
            "wp2": lambda: wp_first(2),
            "wp3": lambda: wp_first(3),
            "wp_second": wp_second,
            "ht0": lambda: ht_send(0),
            "ht1": lambda: ht_send(1),
            "ht2": lambda: ht_send(2),
            "woa0": lambda: wo_a(0),
            "woa1": lambda: wo_a(1),
            "woa2": lambda: wo_a(2),
            "wob0": lambda: wo_b(0),
            "wob1": lambda: wo_b(1),
            "woc0": lambda: wo_c(0),
            "qg0": lambda: qg_send(0),
            "qg1": lambda: qg_send(1),
            "wqa0": lambda: wq_a(0),
            "wqa1": lambda: wq_a(1),
            "wqb0": lambda: wq_b(0),
            "wqc0": lambda: wq_c(0),
            "zf_first": zf_first,
            "zf_second": zf_second,
            "zf_third": zf_third,
            "wf_first0": lambda: wf_first(0),
            "wf_second0": lambda: wf_second(0),
            "wf_third0": lambda: wf_third(0),
            "wf_first1": lambda: wf_first(1),
            "wf_second1": lambda: wf_second(1),
            "wf_third1": lambda: wf_third(1),
        }[what]()

    KC = 256

    def head(h, carry):
        at_head(h)
        both = qo[h]
        top = jnp.full((8, T), -3e38, F32)
        for k in range(S // KC):
            rows = pl.ds(KC * k, KC)
            sd = mm(kv_all[rows, :], both, NT)
            score = sd[:, :T] + bias[rows, :]
            sbuf[rows, :] = score
            dbuf[rows, :] = sd[:, T:]
            top = jnp.maximum(top, jnp.max(score.reshape(KC // 8, 8, T), axis=0))
        top = jnp.max(top, axis=0, keepdims=True)
        norm = jnp.zeros((8, T), F32)
        delta = jnp.zeros((8, T), F32)
        for k in range(S // KC):
            rows = pl.ds(KC * k, KC)
            e = jnp.exp(sbuf[rows, :] - top)
            sbuf[rows, :] = e
            norm = norm + jnp.sum(e.reshape(KC // 8, 8, T), axis=0)
            delta = delta + jnp.sum((e * dbuf[rows, :]).reshape(KC // 8, 8, T), axis=0)
        scale = 1.0 / jnp.sum(norm, axis=0, keepdims=True)
        delta = jnp.sum(delta, axis=0, keepdims=True) * scale
        for k in range(S // KC):
            rows = pl.ds(KC * k, KC)
            p = sbuf[rows, :] * scale
            dsp[rows, :T] = (p * (dbuf[rows, :] - delta)).astype(BF16)
            dsp[rows, T:] = p.astype(BF16)
        for k in range(S // KC):
            rows = pl.ds(KC * k, KC)
            dkv[rows, :] += mm(dsp[rows, :], both)
        result = mm(kvt[...], dsp[...])
        rows = pl.ds(pl.multiple_of(HD * h, HD), HD)
        oht[rows, :] = result[HD:, T:].astype(BF16)
        back = result[:HD, :T] * 0.125
        a, b, rest = back[: ROT // 2], back[ROT // 2 : ROT], back[ROT:]
        ct, st = cost[...], sint[...]
        qgt[rows, :] = jnp.concatenate([a * ct + b * st, b * ct - a * st, rest], axis=0).astype(BF16)
        return carry

    lax.fori_loop(0, H, head, 0)

    def block_rows(k, core):
        return pl.ds(pl.multiple_of((2 * k + core) * T, T), T)

    dkv_b[...] = dkv[...].astype(BF16)
    s_dk = []
    for k in range(NZ):
        s_dk.append(rc("dk", k, dkv_b.at[block_rows(k, 1 - c), :], rdk.at[k], partner))
        send(s_dk[-1])

    ht_send(3)
    qg_send(2)

    for copy in s_dk:
        copy.wait_recv()
    s_dkv = []
    for o in range(1, NZ):
        k = lax.rem(z + o, NZ)
        dks[o] = (dkv[block_rows(k, c), :] + rdk[k].astype(F32)).astype(BF16)
        s_dkv.append(rc("dkv", o, dks.at[o], rdkv.at[o], z_peer(o)))
        send(s_dkv[-1])

    def put(name, row):
        at, count = rows_v[name]
        for i in range(count):
            vec[at + i : at + i + 1, :] = row[:, 128 * i : 128 * (i + 1)]

    wo_a(3)
    wq_a(2)
    wq_b(1)
    wo_b(2)
    wo_c(1)

    s_mlp.wait_recv()
    for i in range(T // 128):
        rows = pl.ds(128 * i, 128)
        branch = mm(oht[:, rows], wo_v[...], TN) + vecs[5:6, :]
        mlp = (mlp_all[rows, :] + mlp_r[rows, :]) + vecs[6:7, :]
        lo_v[rows, :] = ((x2[rows, :].astype(F32) + branch) + mlp).astype(BF16)
    l_lo = lc(lo_v, o_lo)

    zf_second()
    wo_b(3)
    wq_b(2)
    wq_c(1)
    wo_c(2)

    s_sec.wait_recv()
    sums = [jnp.zeros((1, D), F32) for _ in range(6)]
    for i in range(T // 128):
        rows = pl.ds(128 * i, 128)
        ig_v[rows, :] = mm(qg2[rows, :], wq_v[...], NT)
        second_grad = sec_all[rows, :] + sec_r[rows, :]
        sec_all[rows, :] = second_grad * g2
        up = og2[rows, :].astype(F32)
        for k, value in enumerate((qg2[rows, :].astype(F32), up, second_grad * nrm[rows, :], second_grad)):
            sums[2 + k] = sums[2 + k] + jnp.sum(value, axis=0, keepdims=True)

    wo_c(3)
    wq_c(2)
    zf_third()
    wp_third()
    wf_fourth()

    l_kvg.wait()
    for copy in s_dkv:
        copy.wait_recv()
    kv_grads = []
    for i in range(T // 128):
        rows = pl.ds(128 * i, 128)
        total = dkv[pl.ds(pl.multiple_of(d * T + 128 * i, 128), 128), :] + rdk[z, rows, :].astype(F32)
        for o in range(1, NZ):
            total = total + rdkv[o, rows, :].astype(F32)
        total = total + kvg_v[rows, :].astype(F32)
        kv_grads.append(jnp.where(lanes < HD, turn(total, rows, -1.0), total).astype(BF16))
        kvg2[rows, :] = kv_grads[-1]
    s_kvg = rc("kvg", 0, kvg2.at[own], kvg2.at[other], partner)
    send(s_kvg)
    put("b_keyval", jnp.sum(jnp.concatenate(kv_grads, axis=0).astype(F32), axis=0, keepdims=True))

    for i in range(T // 128):
        rows = pl.ds(128 * i, 128)
        first_grad = ig_v[rows, :] + mm(kv_grads[i], wkv_v[...], NT)
        n = nrm[rows, :]
        u = first_grad * g1 + sec_all[rows, :]
        back = u - jnp.mean(u, axis=-1, keepdims=True) - n * jnp.mean(u * n, axis=-1, keepdims=True)
        ig_v[rows, :] = og2[rows, :].astype(F32) + inv[rows, 0:1] * back
        for k, value in enumerate((first_grad * n, first_grad)):
            sums[k] = sums[k] + jnp.sum(value, axis=0, keepdims=True)
    l_ig = lc(ig_v, o_ig)
    for name, row in zip(("ln1_gain", "ln1_bias", "b_query", "column", "ln2_gain", "ln2_bias"), sums):
        put(name, row)
    s_vec = []
    for o in range(1, NSP):
        rows = pl.ds(pl.multiple_of(lax.rem(d + o, NSP) * 8, 8), 8)
        s_vec.append(rc("vec", o, vec.at[rows, :], rvec.at[o], sp_peer(o)))
        send(s_vec[-1])

    s_kvg.wait_recv()
    s_wkv = []
    for k in range(NZ):
        rows = pl.ds(pl.multiple_of(2 * R * k + R * c, 16), R)
        wkv_part[k] = mm(fit[rows, :], kvg2[...])
        wkv_b[k] = wkv_part[k].astype(BF16)
    for o in range(1, NZ):
        s_wkv.append(rc("wkv", o, wkv_b.at[lax.rem(z + o, NZ)], rkv.at[o], z_peer(o)))
        send(s_wkv[-1])

    for copy in s_wkv:
        copy.wait_recv()
    total = wkv_part[z]
    for o in range(1, NZ):
        total = total + rkv[o].astype(F32)
    sm[g, :R, :] = total
    for copy in s_vec:
        copy.wait_recv()
    total = vec[pl.ds(pl.multiple_of(d * 8, 8), 8), :]
    for o in range(1, NSP):
        total = total + rvec[o]
    sm[g, R:, :] = total
    s_sm = [rc("sm", o, sm.at[g], sm.at[g], xy_peer(o, c)) for o in range(1, NG)]
    for copy in s_sm:
        send(copy)

    total = zs_wo[z].astype(F32)
    for o in range(1, NZ):
        r_woz(o).wait_recv()
        total = total + rz_wo[o].astype(F32)
    fin_wo[...] = total.astype(BF16)
    s_wog = [rc("wog", o, fin_wo, o_wo.at[xx, yy], xy_peer(o, c)) for o in range(1, NG)]
    for copy in s_wog:
        send(copy)
    l_fo = lc(fin_wo, o_wo.at[xx, yy])
    total = zs_wq[z].astype(F32)
    for o in range(1, NZ):
        for m in range(H // 4):
            r_wqz(o, m).wait_recv()
        total = total + rz_wq[o].astype(F32)
    fin_wq[...] = total.astype(BF16)
    s_wqg = [rc("wqg", o, fin_wq, o_wq.at[yy, xx], xy_peer(o, c)) for o in range(1, NG)]
    for copy in s_wqg:
        send(copy)
    l_fq = lc(fin_wq, o_wq.at[yy, xx])

    for copy in s_sm:
        copy.wait_recv()
    total = sm[0]
    for k in range(1, NG):
        total = total + sm[k]
    fin_kv[...] = total[:R]
    fin_vec[...] = total[R:]
    l_kv = lc(fin_kv, o_wkv)
    mine8 = pl.ds(pl.multiple_of(d * 8, 8), 8)
    s_vg = [rc("vg", o, fin_vec, o_vec.at[mine8, :], sp_peer(o)) for o in range(1, NSP)]
    for copy in s_vg:
        send(copy)
    l_vg = lc(fin_vec, o_vec.at[mine8, :])

    for o in range(1, NG):
        wp_g(o).wait_recv()
    for o in range(NG):
        for core in range(2):
            if o or core:
                wf_g(o, core).wait_recv()
    for copy in s_wog + s_wqg + s_vg:
        copy.wait_recv()
    for copy in started:
        copy.wait_send()
    for q in range(NZ):
        x_half(q).wait_send()
        wp_y(q).wait_send()
    for k in range(2):
        y_chunk(2 * (1 - yy) + k).wait_send()
        x_chunk(2 * k + 1 - xx).wait_send()
        wf_second_send(k).wait_send()
    for k in range(NZ):
        r_ht(k).wait_send()
        r_wox(k).wait_send()
        r_woy(k).wait_send()
    for m in range(H // 4):
        r_qg(m).wait_send()
        r_wqy(m).wait_send()
        r_wqx(m).wait_send()
    for o in range(1, NZ):
        r_woz(o).wait_send()
        for m in range(H // 4):
            r_wqz(o, m).wait_send()
    zf_x.wait_send()
    zf_y.wait_send()
    for o in range(1, NZ):
        z_half(o).wait_send()
        wp_z(o).wait_send()
        wf_z(o).wait_send()
    for o in range(1, NG):
        wp_g(o).wait_send()
    for o in range(NG):
        for core in range(2):
            if o or core:
                wf_g(o, core).wait_send()
    for copy in l_fin + [l_lo, l_ig, l_kv, l_vg, l_fo, l_fq]:
        copy.wait()


EVENTS = (
    (0, "wp0"),
    (2, "wf_first0"),
    (2, "wf_first1"),
    (3, "wp1"),
    (3, "ht0"),
    (4, "woa0"),
    (4, "qg0"),
    (4, "wf_second0"),
    (4, "wp2"),
    (5, "wqa0"),
    (6, "wf_second1"),
    (6, "wp3"),
    (6, "ht1"),
    (7, "woa1"),
    (8, "wf_third1"),
    (8, "wp_second"),
    (8, "qg1"),
    (9, "wqa1"),
    (9, "wob0"),
    (9, "wqb0"),
    (9, "ht2"),
    (10, "wf_third0"),
    (10, "woa2"),
    (11, "zf_first"),
    (11, "woc0"),
    (11, "wqc0"),
    (11, "wob1"),
)


def finish_kernel(
    dims, wp_h, wf_h, wo_h, wq_h, wkv_h, vec_h, lo_h, ig_h,
    layer_out, input_grad, ln1_gain, ln1_bias, w_query, b_query, w_keyval, b_keyval,
    w_attn_out, b_attn_out, ln2_gain, ln2_bias, w_fc, b_fc, w_proj, b_proj,
    wp, wf, wo, wq, wkv, vec, lo, ig, fc_v, proj_v, out_v, query_v, isem, osem,
):
    T, D, F, S, NSP, NG = dims
    Q, R, C2 = F // NSP, D // NSP, D // 2
    arrive = {}
    for i, (name, src, dst) in enumerate(
        (("wf", wf_h, wf), ("wp", wp_h, wp), ("ig", ig_h, ig), ("lo", lo_h, lo), ("vec", vec_h, vec),
         ("wo", wo_h, wo), ("wq", wq_h, wq), ("wkv", wkv_h, wkv))
    ):
        arrive[name] = pltpu.make_async_copy(src, dst, isem.at[i])
        arrive[name].start()
    leave = []

    def put_out(src, dst):
        leave.append(pltpu.make_async_copy(src, dst, osem.at[len(leave)]))
        leave[-1].start()

    arrive["wf"].wait()
    for k in range(NG):
        for core in range(2):
            at = Q * (2 * k + core)
            fc_v[:, at : at + Q] = wf[k, core].astype(F32)
    put_out(fc_v, w_fc)
    arrive["wp"].wait()
    rows = Q // 2 // NG
    for k in range(NG):
        for part in range(2):
            at = Q // 2 * part + rows * k
            proj_v[at : at + rows, :] = wp[k, part].astype(F32)
    put_out(proj_v, w_proj)
    arrive["ig"].wait()
    put_out(ig, input_grad)
    arrive["lo"].wait()
    put_out(lo, layer_out)
    arrive["wo"].wait()
    arrive["wq"].wait()
    for a in range(2):
        for b in range(2):
            rows = slice(R // 2 * a, R // 2 * (a + 1))
            cols = slice(C2 * b, C2 * (b + 1))
            out_v[rows, cols] = wo[a, b].astype(F32)
            for m in range(H // 4):
                at = 4 * HD * m + 2 * HD * b
                query_v[rows, at : at + 2 * HD] = wq[a, b, :, 2 * HD * m : 2 * HD * (m + 1)].astype(F32)
    put_out(out_v, w_attn_out)
    put_out(query_v, w_query)
    arrive["wkv"].wait()
    put_out(wkv, w_keyval)
    arrive["vec"].wait()
    rows_v, _ = vec_rows(D, F, 2 * HD)
    for name, out in (
        ("ln1_gain", ln1_gain), ("ln1_bias", ln1_bias), ("b_query", b_query), ("b_keyval", b_keyval),
        ("column", b_attn_out), ("column", b_proj), ("ln2_gain", ln2_gain), ("ln2_bias", ln2_bias),
        ("b_fc", b_fc),
    ):
        at, count = rows_v[name]
        out[...] = jnp.concatenate([vec[at + i : at + i + 1, :] for i in range(count)], axis=1).reshape(
            128 * count
        )
    for copy in leave:
        copy.wait()


def fused_local(n_grp, n_sp, *args):
    layer_input, block_order = args[0], args[1]
    T, D = layer_input.shape
    F = args[12].shape[1]
    S = T * n_sp
    NZ, NG, NSP = n_sp // 2, n_grp, n_sp
    Q, R, C2, pair = F // n_sp, D // n_sp, D // 2, 2 * HD
    dims = (T, D, F, S, NSP, NG)
    V = pltpu.VMEM
    scratch = [
        V((8, D), F32), V((1, pair), F32), V((1, F), F32),
        V((2 * T, D), BF16), V((2 * T, D), BF16), V((2 * T, D), BF16), V((2 * T, D), BF16),
        V((D, 2 * T), BF16), V((D, 2 * T), BF16), V((T, D), F32), V((T, 128), F32),
        V((D, pair), BF16), V((D, D), BF16), V((D, D), BF16), V((NZ, D, Q), BF16), V((NZ, Q, D), BF16),
        V((T, pair), BF16), V((NZ, 2 * T, Q), BF16), V((NZ, 2 * T, Q), BF16),
        V((2 * T, D), F32), V((2 * T, D), F32), V((T, D), F32), V((T, D), F32),
        V((NZ, Q, D), BF16), V((NZ, Q // 4, D), BF16), V((NZ, Q // 4, D), BF16), V((NZ, Q // 8, D), BF16),
        V((NZ, Q // 8, D), BF16), V((NZ, Q // 8, D), BF16), V((NZ, Q // 2, D), BF16), V((Q // 2, D), BF16),
        V((Q // 4, D), BF16), V((Q // 4, D), BF16), V((Q // 8, D), BF16), V((2, Q // 8, D), BF16),
        V((NZ, D, Q), BF16), V((2, D // 2, Q), BF16), V((2, D // 2, Q), BF16), V((2, D // 2, Q), BF16),
        V((2, D // 2, Q), BF16), V((2, D // 2, Q), BF16), V((D, Q), BF16), V((NZ, 2 * R, Q), BF16), V((2 * R, Q), BF16),
        V((S, pair), BF16), V((pair, S), BF16), V((H, 2 * T, pair), BF16), V((S, T), F32), V((S, T), F32),
        V((S, T), F32), V((S, 2 * T), BF16), V((S, pair), F32), V((S, pair), BF16), V((NZ, T, pair), BF16),
        V((NZ, T, pair), BF16), V((NZ, T, pair), BF16), V((2 * T, pair), BF16),
        V((D, T), BF16), V((D, T), BF16), V((NZ, R, T), BF16), V((2 * T, D), BF16),
        V((NZ, R, D), BF16), V((NZ, R // 2, D), BF16), V((NZ, R // 2, D), BF16), V((NZ, R // 2, C2), BF16),
        V((NZ, R // 2, C2), BF16), V((NZ, R // 2, C2), BF16), V((R // 2, C2), BF16),
        V((NZ, R, D), BF16), V((NZ, R // 2, D), BF16), V((NZ, R // 2, D), BF16),
        V((H // 4, NZ, R // 2, 2 * HD), BF16),
        V((NZ, R // 2, C2), BF16), V((NZ, R // 2, C2), BF16), V((R // 2, C2), BF16),
        V((8 * NSP, 128), F32), V((NSP, 8, 128), F32), V((NZ, R, pair), F32), V((NZ, R, pair), BF16),
        V((NZ, R, pair), BF16), V((NG, R + 8, 128), F32), V((R, 128), F32), V((8, 128), F32),
        V((T, D), BF16), V((T, D), F32), V((T, pair), F32), V((T, pair), F32), V((8, T), F32), V((8, T), F32),
        pltpu.SemaphoreType.DMA((40,)), pltpu.SemaphoreType.DMA((160,)), pltpu.SemaphoreType.DMA((160,)),
    ]
    any_spec = pl.BlockSpec(memory_space=pl.ANY)
    shape = jax.ShapeDtypeStruct
    held = pl.pallas_call(
        functools.partial(fused_kernel, dims),
        out_shape=(
            shape((NG, 2, Q // 8, D), BF16),
            shape((NG, 2, R, Q), BF16),
            shape((2, 2, R // 2, C2), BF16),
            shape((2, 2, R // 2, C2), BF16),
            shape((R, pair), F32),
            shape((8 * NSP, 128), F32),
            shape((T, D), BF16),
            shape((T, D), F32),
        ),
        in_specs=[any_spec, pl.BlockSpec(memory_space=pltpu.SMEM)] + [any_spec] * 16,
        out_specs=(any_spec,) * 8,
        scratch_shapes=scratch,
        compiler_params=pltpu.CompilerParams(
            collective_id=0, has_side_effects=True, vmem_limit_bytes=67043328
        ),
        name="fused_layer",
    )(*args)
    vmem_spec = pl.BlockSpec(memory_space=pltpu.VMEM)
    row = shape((D,), F32)
    return pl.pallas_call(
        functools.partial(finish_kernel, dims),
        out_shape=(
            shape((T, D), BF16), shape((T, D), F32), row, row, shape((R, D), F32), row, shape((R, pair), F32),
            shape((pair,), F32), shape((R, D), F32), row, row, row, shape((R, F), F32), shape((F,), F32),
            shape((Q, D), F32), row,
        ),
        in_specs=[any_spec] * 8,
        out_specs=tuple(any_spec if k in (0, 1, 4, 6, 8, 12, 14) else vmem_spec for k in range(16)),
        scratch_shapes=[
            V((NG, 2, Q // 8, D), BF16), V((NG, 2, R, Q), BF16), V((2, 2, R // 2, C2), BF16),
            V((2, 2, R // 2, C2), BF16), V((R, pair), F32), V((8 * NSP, 128), F32), V((T, D), BF16), V((T, D), F32),
            V((R, F), F32), V((Q, D), F32), V((R, D), F32), V((R, D), F32),
            pltpu.SemaphoreType.DMA((8,)), pltpu.SemaphoreType.DMA((8,)),
        ],
        compiler_params=pltpu.CompilerParams(vmem_limit_bytes=64000000),
        name="finish",
    )(*held)


def fits(mesh, args):
    n_grp, n_sp = mesh.shape["grp"], mesh.shape["sp"]
    tokens, width = args[0].shape
    seqs, blocks = args[1].shape
    ff = args[12].shape[1]
    rows = tokens // (n_grp * n_sp)
    return (
        n_grp == 4
        and n_sp == 2 * n_grp
        and seqs == n_grp
        and blocks == 2 * n_sp
        and rows == 2 * 128
        and width == H * HD
        and width % (32 * n_sp) == 0
        and ff % (128 * n_sp) == 0
        and width % 128 == 0
        and sum(count for _, count in vec_rows(width, ff, 2 * HD)[0].values()) <= 8 * n_sp
    )


def layer_norm(values, gain_row, shift_row):
    centre = jnp.mean(values, axis=-1, keepdims=True)
    centred = values - centre
    spread = jnp.mean(centred * centred, axis=-1, keepdims=True)
    inverse_dev = lax.rsqrt(spread + norm_eps)
    normed = centred * inverse_dev
    return (normed * gain_row + shift_row, normed, inverse_dev)


def norm_back(upstream, normed, inverse_dev, gain_row):
    scaled = upstream * gain_row
    return inverse_dev * (
        scaled
        - jnp.mean(scaled, axis=-1, keepdims=True)
        - normed * jnp.mean(scaled * normed, axis=-1, keepdims=True)
    )


def rotary_tables(position):
    half_rot = ROT // 2
    frequency = jnp.exp(jnp.arange(half_rot, dtype=jnp.float32) * (-2.0 * rotary_base_log / ROT))
    angles = position.astype(jnp.float32)[:, None] * 0.25 * frequency[None, :]
    return (jnp.cos(angles), jnp.sin(angles))


def rotate(values, cosine, sine_table):
    half_rot = ROT // 2
    cos_rows = cosine[:, None, :]
    sin_rows = sine_table[:, None, :]
    lower_half = values[..., :half_rot]
    upper_half = values[..., half_rot:ROT]
    return jnp.concatenate(
        [
            lower_half * cos_rows - upper_half * sin_rows,
            upper_half * cos_rows + lower_half * sin_rows,
            values[..., ROT:],
        ],
        axis=-1,
    )


def rotate_back(values, cosine, sine_table):
    half_rot = ROT // 2
    cos_rows = cosine[:, None, :]
    sin_rows = sine_table[:, None, :]
    lower_half = values[..., :half_rot]
    upper_half = values[..., half_rot:ROT]
    return jnp.concatenate(
        [
            lower_half * cos_rows + upper_half * sin_rows,
            upper_half * cos_rows - lower_half * sin_rows,
            values[..., ROT:],
        ],
        axis=-1,
    )


def key_scores(query_rows, row_pos, kv_sequence, block_index, block_rows):
    key_start = block_index * block_rows
    key_slice = lax.dynamic_slice_in_dim(kv_sequence, key_start, block_rows, 0)
    raw_scores = (
        jnp.einsum("rd,kd->rk", query_rows, key_slice[:, :HD], preferred_element_type=jnp.float32)
        * 0.125
    )
    key_pos = key_start + lax.broadcasted_iota(jnp.int32, (1, block_rows), 1)
    return (jnp.where(key_pos <= row_pos[:, None], raw_scores, masked_score), key_slice)


def attention_forward(query_tiles, tile_pos, kv_sorted):
    pair_count = query_tiles.shape[0]
    pairs_per_seq = pair_count // kv_sorted.shape[0]
    block_rows = min(score_block, kv_sorted.shape[1])

    def one_pair(inputs):
        query_rows, row_pos, pair_index = inputs
        kv_sequence = kv_sorted[pair_index // pairs_per_seq]
        key_blocks = jnp.max(row_pos) // block_rows + 1
        row_count = query_rows.shape[0]

        def max_pass(block_index, carried):
            running_max, running_sum = carried
            masked, key_slice = key_scores(
                query_rows, row_pos, kv_sequence, block_index, block_rows
            )
            new_max = jnp.maximum(running_max, jnp.max(masked, axis=1, keepdims=True))
            running_sum = running_sum * jnp.exp(running_max - new_max) + jnp.sum(
                jnp.exp(masked - new_max), axis=1, keepdims=True
            )
            return (new_max, running_sum)

        start_max = jnp.full((row_count, 1), masked_score, jnp.float32)
        running_max, running_sum = lax.fori_loop(
            0, key_blocks, max_pass, (start_max, jnp.zeros((row_count, 1), jnp.float32))
        )
        log_total = running_max + jnp.log(running_sum)

        def value_pass(block_index, output):
            masked, key_slice = key_scores(
                query_rows, row_pos, kv_sequence, block_index, block_rows
            )
            weights = jnp.exp(masked - log_total).astype(jnp.bfloat16)
            return output + jnp.dot(weights, key_slice[:, HD:], preferred_element_type=jnp.float32)

        output = lax.fori_loop(0, key_blocks, value_pass, jnp.zeros((row_count, HD), jnp.float32))
        return (output, log_total)

    return lax.map(one_pair, (query_tiles, tile_pos, jnp.arange(pair_count, dtype=jnp.int32)))


def attention_backward(query_tiles, tile_pos, grad_tiles, log_totals, kv_sorted):
    pair_count = query_tiles.shape[0]
    pairs_per_seq = pair_count // kv_sorted.shape[0]
    block_rows = min(score_block, kv_sorted.shape[1])
    pair_width = kv_sorted.shape[2]

    def one_pair(key_grads, inputs):
        query_rows, row_pos, grad_rows, log_total, pair_index = inputs
        sequence = pair_index // pairs_per_seq
        kv_sequence = kv_sorted[sequence]
        key_blocks = jnp.max(row_pos) // block_rows + 1
        row_count = query_rows.shape[0]

        def pass_terms(block_index):
            masked, key_slice = key_scores(
                query_rows, row_pos, kv_sequence, block_index, block_rows
            )
            weights = jnp.exp(masked - log_total)
            weight_grads = jnp.einsum(
                "rd,kd->rk", grad_rows, key_slice[:, HD:], preferred_element_type=jnp.float32
            )
            return (weights, weight_grads, key_slice)

        def delta_pass(block_index, row_delta):
            weights, weight_grads, unused_slice = pass_terms(block_index)
            return row_delta + jnp.sum(weights * weight_grads, axis=1, keepdims=True)

        row_delta = lax.fori_loop(0, key_blocks, delta_pass, jnp.zeros((row_count, 1), jnp.float32))

        def grad_pass(block_index, carried):
            query_grad, sequence_grads = carried
            weights, weight_grads, key_slice = pass_terms(block_index)
            score_grad = (weights * (weight_grads - row_delta)).astype(jnp.bfloat16)
            query_grad = (
                query_grad
                + jnp.dot(score_grad, key_slice[:, :HD], preferred_element_type=jnp.float32) * 0.125
            )
            key_part = (
                jnp.einsum("rk,rd->kd", score_grad, query_rows, preferred_element_type=jnp.float32)
                * 0.125
            )
            value_part = jnp.einsum(
                "rk,rd->kd",
                weights.astype(jnp.bfloat16),
                grad_rows,
                preferred_element_type=jnp.float32,
            )
            key_start = block_index * block_rows
            previous = lax.dynamic_slice(
                sequence_grads, (sequence, key_start, 0), (1, block_rows, pair_width)
            )
            updated = previous + jnp.concatenate([key_part, value_part], axis=1)[None]
            return (
                query_grad,
                lax.dynamic_update_slice(sequence_grads, updated, (sequence, key_start, 0)),
            )

        query_grad, key_grads = lax.fori_loop(
            0, key_blocks, grad_pass, (jnp.zeros((row_count, HD), jnp.float32), key_grads)
        )
        return (key_grads, query_grad)

    start_grads = jnp.zeros(kv_sorted.shape, jnp.float32)
    key_grads, query_grads = lax.scan(
        one_pair,
        start_grads,
        (query_tiles, tile_pos, grad_tiles, log_totals, jnp.arange(pair_count, dtype=jnp.int32)),
    )
    return (query_grads, key_grads)


def local(
    layer_input,
    block_order,
    ln1_gain,
    ln1_bias,
    w_query,
    b_query,
    w_keyval,
    b_keyval,
    w_attn_out,
    b_attn_out,
    ln2_gain,
    ln2_bias,
    w_fc,
    b_fc,
    w_proj,
    b_proj,
    kv_grad,
    out_grad,
):
    my_rank = lax.axis_index("sp")
    seq_count = block_order.shape[0]
    block_count = block_order.shape[1]
    token_count = layer_input.shape[0]
    shard_len = token_count // seq_count
    block_len = shard_len // 2
    model_width = layer_input.shape[1]
    pair_width = 2 * HD
    pair_count = 2 * seq_count
    input_float = layer_input.astype(jnp.float32)
    first_in, first_hat, first_inv = layer_norm(input_float, ln1_gain, ln1_bias)
    first_low = first_in.astype(jnp.bfloat16)
    query_pre = jnp.dot(first_low, w_query, preferred_element_type=jnp.float32) + b_query
    keyval_pre = jnp.dot(first_low, w_keyval, preferred_element_type=jnp.float32) + b_keyval
    offsets = jnp.arange(block_len, dtype=jnp.int32)
    own_blocks = lax.dynamic_slice_in_dim(block_order, 2 * my_rank, 2, 1)
    own_pos = (own_blocks[:, :, None] * block_len + offsets[None, None, :]).reshape(token_count)
    cosine, sine_table = rotary_tables(own_pos)
    query_use = (
        rotate(query_pre.reshape(token_count, H, HD), cosine, sine_table)
        .reshape(token_count, model_width)
        .astype(jnp.bfloat16)
    )
    key_rot = rotate(keyval_pre[:, None, :HD], cosine, sine_table)[:, 0, :]
    keyval_use = jnp.concatenate([key_rot, keyval_pre[:, HD:]], axis=1).astype(jnp.bfloat16)
    gathered = lax.all_gather(
        keyval_use.reshape(seq_count, shard_len, pair_width), "sp", axis=1, tiled=True
    )
    seq_len = gathered.shape[1]
    block_sorter = jnp.argsort(block_order, axis=1)
    kv_sorted = jnp.take_along_axis(
        gathered.reshape(seq_count, block_count, block_len, pair_width),
        block_sorter[:, :, None, None],
        axis=1,
    ).reshape(seq_count, seq_len, pair_width)
    row_pos = own_pos.reshape(seq_count, shard_len)
    query_rows = query_use.reshape(seq_count, shard_len, model_width)
    query_tiles = query_rows.reshape(pair_count, block_len * H, HD)
    tile_pos = jnp.repeat(row_pos.reshape(pair_count, block_len), H, axis=1)
    head_rows, log_totals = attention_forward(query_tiles, tile_pos, kv_sorted)
    heads_sorted = head_rows.reshape(seq_count, shard_len, model_width).astype(jnp.bfloat16)
    heads_local = heads_sorted.reshape(token_count, model_width)
    attn_branch = jnp.dot(heads_local, w_attn_out, preferred_element_type=jnp.float32) + b_attn_out
    second_in, second_hat, second_inv = layer_norm(input_float, ln2_gain, ln2_bias)
    second_low = second_in.astype(jnp.bfloat16)
    hidden = jnp.dot(second_low, w_fc, preferred_element_type=jnp.float32) + b_fc
    erf_part = 1.0 + lax.erf(hidden * half_root)
    activated = (0.5 * hidden * erf_part).astype(jnp.bfloat16)
    mlp_branch = jnp.dot(activated, w_proj, preferred_element_type=jnp.float32) + b_proj
    layer_out = (input_float + attn_branch + mlp_branch).astype(jnp.bfloat16)
    upstream = out_grad.astype(jnp.float32)
    column_sum = jnp.sum(upstream, axis=0)
    w_proj_grad = jnp.einsum("tf,td->fd", activated, out_grad, preferred_element_type=jnp.float32)
    act_grad = jnp.einsum("td,fd->tf", out_grad, w_proj, preferred_element_type=jnp.float32)
    gelu_slope = 0.5 * erf_part + hidden * jnp.exp(-0.5 * hidden * hidden) * inv_root_tau
    hidden_grad = (act_grad * gelu_slope).astype(jnp.bfloat16)
    w_fc_grad = jnp.einsum("td,tf->df", second_low, hidden_grad, preferred_element_type=jnp.float32)
    b_fc_grad = jnp.sum(hidden_grad.astype(jnp.float32), axis=0)
    second_grad = jnp.einsum("tf,df->td", hidden_grad, w_fc, preferred_element_type=jnp.float32)
    w_attn_out_grad = jnp.einsum(
        "te,td->ed", heads_local, out_grad, preferred_element_type=jnp.float32
    )
    heads_grad = jnp.einsum(
        "td,ed->te", out_grad, w_attn_out, preferred_element_type=jnp.float32
    ).astype(jnp.bfloat16)
    grad_rows = heads_grad.reshape(seq_count, shard_len, model_width)
    grad_tiles = grad_rows.reshape(pair_count, block_len * H, HD)
    query_tile_grads, sorted_kv_grads = attention_backward(
        query_tiles, tile_pos, grad_tiles, log_totals, kv_sorted
    )
    query_rot_rows = query_tile_grads.reshape(seq_count, shard_len, model_width)
    query_rot_grad = query_rot_rows.reshape(token_count, model_width)
    query_grad = (
        rotate_back(query_rot_grad.reshape(token_count, H, HD), cosine, sine_table)
        .reshape(token_count, model_width)
        .astype(jnp.bfloat16)
    )
    stored_kv_grads = jnp.take_along_axis(
        sorted_kv_grads.reshape(seq_count, block_count, block_len, pair_width),
        block_order[:, :, None, None],
        axis=1,
    ).reshape(seq_count, seq_len, pair_width)
    own_kv_grad = lax.psum_scatter(stored_kv_grads, "sp", scatter_dimension=1, tiled=True).reshape(
        token_count, pair_width
    ) + kv_grad.astype(jnp.float32)
    key_pre_grad = rotate_back(own_kv_grad[:, None, :HD], cosine, sine_table)[:, 0, :]
    keyval_grad = jnp.concatenate([key_pre_grad, own_kv_grad[:, HD:]], axis=1).astype(jnp.bfloat16)
    w_query_grad = jnp.einsum(
        "td,te->de", first_low, query_grad, preferred_element_type=jnp.float32
    )
    b_query_grad = jnp.sum(query_grad.astype(jnp.float32), axis=0)
    w_keyval_grad = jnp.einsum(
        "td,te->de", first_low, keyval_grad, preferred_element_type=jnp.float32
    )
    b_keyval_grad = jnp.sum(keyval_grad.astype(jnp.float32), axis=0)
    first_grad = jnp.einsum(
        "te,de->td", query_grad, w_query, preferred_element_type=jnp.float32
    ) + jnp.einsum("te,de->td", keyval_grad, w_keyval, preferred_element_type=jnp.float32)
    first_back = norm_back(first_grad, first_hat, first_inv, ln1_gain)
    second_back = norm_back(second_grad, second_hat, second_inv, ln2_gain)
    input_grad = upstream + first_back + second_back
    (
        ln1_gain_grad,
        ln1_bias_grad,
        b_query_total,
        b_keyval_total,
        bias_out_total,
        ln2_gain_grad,
        ln2_bias_grad,
        b_fc_total,
    ) = lax.psum(
        (
            jnp.sum(first_grad * first_hat, axis=0),
            jnp.sum(first_grad, axis=0),
            b_query_grad,
            b_keyval_grad,
            column_sum,
            jnp.sum(second_grad * second_hat, axis=0),
            jnp.sum(second_grad, axis=0),
            b_fc_grad,
        ),
        ("grp", "sp"),
    )
    query_share, keyval_share, out_share, fc_share, proj_share = (
        lax.psum_scatter(w_query_grad, "sp", scatter_dimension=0, tiled=True),
        lax.psum_scatter(w_keyval_grad, "sp", scatter_dimension=0, tiled=True),
        lax.psum_scatter(w_attn_out_grad, "sp", scatter_dimension=0, tiled=True),
        lax.psum_scatter(w_fc_grad, "sp", scatter_dimension=0, tiled=True),
        lax.psum_scatter(w_proj_grad, "sp", scatter_dimension=0, tiled=True),
    )
    query_total, keyval_total, out_total, fc_total, proj_total = lax.psum(
        (query_share, keyval_share, out_share, fc_share, proj_share), "grp"
    )
    return (
        layer_out,
        input_grad,
        ln1_gain_grad,
        ln1_bias_grad,
        query_total,
        b_query_total,
        keyval_total,
        b_keyval_total,
        out_total,
        bias_out_total,
        ln2_gain_grad,
        ln2_bias_grad,
        fc_total,
        b_fc_total,
        proj_total,
        bias_out_total,
    )


def solution(mesh):
    placed = (
        P(("grp", "sp"), None),
        P("grp", None),
        P(),
        P(),
        P(),
        P(),
        P(),
        P(),
        P(),
        P(),
        P(),
        P(),
        P(),
        P(),
        P(),
        P(),
        P(("grp", "sp"), None),
        P(("grp", "sp"), None),
    )
    def step(*args):
        if fits(mesh, args):
            body = functools.partial(fused_local, mesh.shape["grp"], mesh.shape["sp"])
        else:
            body = local
        return spread(body)(*args)

    def spread(body):
        return jax.shard_map(
            body,
            mesh=mesh,
            in_specs=placed,
            out_specs=(
                P(("grp", "sp"), None),
                P(("grp", "sp"), None),
                P(),
                P(),
                P("sp", None),
                P(),
                P("sp", None),
                P(),
                P("sp", None),
                P(),
                P(),
                P(),
                P("sp", None),
                P(),
                P("sp", None),
                P(),
            ),
            check_vma=False,
        )

    return step
```

```python
import functools
import math

import jax
import jax.numpy as jnp
from jax import lax
from jax.experimental import pallas as pl
from jax.experimental.pallas import tpu as pltpu
from jax.sharding import PartitionSpec as P

H = 12
HD = 64
ROT = 16
MESH = pl.DeviceIdType.MESH
F32 = jnp.float32
BF16 = jnp.bfloat16
NN = (((1,), (0,)), ((), ()))
NT = (((1,), (1,)), ((), ()))
TN = (((0,), (0,)), ((), ()))


def mm(a, b, dims=NN):
    return lax.dot_general(a, b, dims, preferred_element_type=F32)

norm_eps = 1e-05
half_root = 0.7071067811865476
inv_root_tau = 0.3989422804014327
masked_score = -1e30
rotary_base_log = math.log(10000.0)
score_block = 512


def vec_rows(width, ff, pair):
    names = ("ln1_gain", "ln1_bias", "b_query", "b_keyval", "column", "ln2_gain", "ln2_bias", "b_fc")
    sizes = (width, width, width, pair, width, width, width, ff)
    at, rows = 0, {}
    for name, size in zip(names, sizes):
        rows[name] = (at, size // 128)
        at += size // 128
    return rows, at


def fused_kernel(
    dims,
    x_h,
    order_s,
    g1_h,
    b1_h,
    wq_h,
    bq_h,
    wkv_h,
    bkv_h,
    wo_h,
    bo_h,
    g2_h,
    b2_h,
    wfc_h,
    bfc_h,
    wpr_h,
    bpr_h,
    kvg_h,
    og_h,
    o_wp,
    o_wf,
    o_wo,
    o_wq,
    o_wkv,
    o_vec,
    o_lo,
    o_ig,
    vecs,
    bkv_v,
    bfc_v,
    x2,
    og2,
    fi2,
    si2,
    fit,
    sit,
    nrm,
    inv,
    wkv_v,
    wq_v,
    wo_v,
    wfc_v,
    wpr_v,
    kvg_v,
    act_s,
    hg_s,
    mlp_all,
    sec_all,
    mlp_r,
    sec_r,
    wp_part,
    rx_wp,
    wp_s1,
    ry_wp,
    zs_wp,
    rz_wp,
    rzf,
    zf_pair,
    zf_s0,
    rx_zf,
    zf_s1,
    ry_zf,
    fin_wp,
    wf_part,
    ry_wf,
    rx_wf,
    wf_s1,
    wf_own,
    wf_in,
    zs_wf,
    rz_wf,
    fin_wf,
    kv_all,
    kvt,
    qo,
    bias,
    sbuf,
    dbuf,
    dsp,
    dkv,
    dkv_b,
    rdk,
    dks,
    rdkv,
    kvg2,
    oht,
    qgt,
    ht_r,
    qg2,
    wo_part,
    rx_wo,
    wo_s1,
    ry_wo,
    zs_wo,
    rz_wo,
    fin_wo,
    wq_part,
    ry_wq,
    wq_s1,
    rx_wq,
    zs_wq,
    rz_wq,
    fin_wq,
    vec,
    rvec,
    wkv_part,
    wkv_b,
    rkv,
    sm,
    fin_kv,
    fin_vec,
    lo_v,
    ig_v,
    ctab,
    stab,
    cost,
    sint,
    lsem,
    ssem,
    rsem,
):
    T, D, F, S, NSP, NG = dims
    NZ = NSP // 2
    D2 = D // 2
    Q = F // NSP
    QH = Q // 2
    R = D // NSP
    C2 = D // 2
    pair = 2 * HD
    g = lax.axis_index("grp")
    d = lax.axis_index("sp")
    c = lax.rem(d, 2)
    z = lax.div(d, 2)
    xx = lax.rem(g, 2)
    yy = lax.div(g, 2)
    partner = (g, d + 1 - 2 * c)
    xnb = (g + 1 - 2 * xx, d)
    ynb = (g + 2 - 4 * yy, d)

    def sp_peer(o):
        return (g, lax.rem(d + o, NSP))

    def z_peer(o):
        return (g, 2 * lax.rem(z + o, NZ) + c)

    def xy_peer(o, core):
        return (lax.rem(g + o, NG), 2 * z + core)

    def block_rows(k, core):
        return pl.ds(pl.multiple_of((2 * k + core) * T, T), T)

    mate = z + 1 - 2 * lax.rem(z, 2)
    far = 2 * (1 - lax.div(z, 2))
    outer = jnp.logical_or(z == 0, z == NZ - 1)
    to_mate = (g, 2 * mate + c)

    base = {}
    used = [0]

    def take(name, n):
        base[name] = used[0]
        used[0] += n

    for name, n in (
        ("x", 1), ("og", 1), ("kv", NZ), ("kvp", NZ), ("mlp", 1), ("sec", 1),
        ("wpx", NZ), ("wpy", NZ), ("wpz", NZ), ("wpg", NG),
        ("wpf", 5), ("zfx", 1), ("zfy", 1),
        ("wfy", 2), ("wfx", 2), ("wfs", 2), ("wfz", NZ), ("wfg", 2 * NG),
        ("ht", NZ), ("qg", H // 4), ("dk", NZ), ("dkv", NZ), ("kvg", 1),
        ("wox", NZ), ("woy", NZ), ("woz", NZ), ("wog", NG),
        ("wqy", H // 4), ("wqx", H // 4), ("wqz", NZ * (H // 4)), ("wqg", NG),
        ("wkv", NZ), ("vec", NSP), ("sm", NG), ("vg", NSP),
    ):
        take(name, n)

    def rc(name, i, src, dst, to):
        k = base[name] + i
        return pltpu.make_async_remote_copy(
            src_ref=src,
            dst_ref=dst,
            send_sem=ssem.at[k],
            recv_sem=rsem.at[k],
            device_id=to,
            device_id_type=MESH,
        )

    started = []

    def send(copy):
        copy.start()
        started.append(copy)

    lused = [0]

    def lc(src, dst):
        copy = pltpu.make_async_copy(src, dst, lsem.at[lused[0]])
        lused[0] += 1
        copy.start()
        return copy

    def chunk_of(j):
        far_y = lax.div(j, 2) == 0
        far_x = lax.rem(j, 2) == 0
        return 2 * jnp.where(far_y, 1 - yy, yy) + jnp.where(far_x, 1 - xx, xx)

    def chunk_in(j):
        far_y = lax.div(j, 2) == 0
        far_x = lax.rem(j, 2) == 0
        return 2 * jnp.where(far_y, 1 - yy, yy) + jnp.where(far_x, xx, 1 - xx)

    def chunk_y(j):
        far_y = lax.div(j, 2) == 0
        far_x = lax.rem(j, 2) == 0
        return 2 * jnp.where(far_y, yy, 1 - yy) + jnp.where(far_x, xx, 1 - xx)

    own = pl.ds(0, T)
    other = pl.ds(T, T)
    l_x = lc(x_h, x2.at[own])
    l_og = lc(og_h, og2.at[own])
    l_wkv = lc(wkv_h, wkv_v)
    l_vec = [
        lc(src, vecs.at[i]) for i, src in enumerate((g1_h, b1_h, g2_h, b2_h, bq_h, bo_h, bpr_h))
    ]
    l_bkv = lc(bkv_h, bkv_v.at[0])
    l_bfc = lc(bfc_h, bfc_v.at[0])
    l_mlp = []
    for j in range(NZ):
        q = chunk_of(j)
        cols = pl.ds(pl.multiple_of(Q * (2 * q + c), 128), Q)
        rows = pl.ds(pl.multiple_of(Q * (2 * q + c), 16), Q)
        l_mlp.append((lc(wfc_h.at[:, cols], wfc_v.at[q]), lc(wpr_h.at[rows, :], wpr_v.at[q])))
    l_wq = lc(wq_h, wq_v)
    l_wo = lc(wo_h, wo_v)
    l_kvg = lc(kvg_h, kvg_v)

    barrier = pltpu.get_barrier_semaphore()
    for o in range(1, NSP):
        pl.semaphore_signal(barrier, inc=1, device_id=sp_peer(o), device_id_type=MESH)
    for o in range(1, NG):
        for core in range(2):
            pl.semaphore_signal(barrier, inc=1, device_id=xy_peer(o, core), device_id_type=MESH)
    pl.semaphore_wait(barrier, NSP - 1 + 2 * (NG - 1))

    s_x = rc("x", 0, x_h, x2.at[other], partner)
    send(s_x)
    s_og = rc("og", 0, og_h, og2.at[other], partner)
    send(s_og)

    lane = lax.broadcasted_iota(jnp.int32, (8, T), 1)
    half = lax.broadcasted_iota(jnp.int32, (8, T), 0).astype(F32)
    block = T // 2
    first_block = order_s[0, 2 * d]
    second_block = order_s[0, 2 * d + 1]
    own_pos = jnp.where(
        lane < block, first_block * block + lane, second_block * block + (lane - block)
    )
    frequency = jnp.exp(half * (-2.0 * rotary_base_log / ROT))
    angle = own_pos.astype(F32) * 0.25 * frequency
    cosine, sine = jnp.cos(angle), jnp.sin(angle)
    cost[...] = cosine
    sint[...] = sine
    ones = jnp.ones((HD - ROT, T), F32)
    zeros = jnp.zeros((HD - ROT, T), F32)
    ctab[...] = jnp.concatenate([cosine, cosine, ones] * 2, axis=0).T
    stab[...] = jnp.concatenate([-sine, sine, zeros] * 2, axis=0).T
    lanes = lax.broadcasted_iota(jnp.int32, (128, pair), 1)
    low_half = lax.rem(lanes, HD) < ROT // 2

    def turn(tile, rows, sign):
        mixed = jnp.where(low_half, pltpu.roll(tile, pair - ROT // 2, 1), pltpu.roll(tile, ROT // 2, 1))
        return tile * ctab[rows, :] + (sign * mixed) * stab[rows, :]

    for copy in l_vec:
        copy.wait()
    l_bkv.wait()
    l_bfc.wait()
    g1, b1, g2, b2 = (vecs[i : i + 1, :] for i in range(4))
    vec[...] = jnp.zeros_like(vec)

    def norms(at, keep):
        for i in range(T // 128):
            rows = pl.ds(at + 128 * i, 128)
            v = x2[rows, :].astype(F32)
            centred = v - jnp.mean(v, axis=-1, keepdims=True)
            r = lax.rsqrt(jnp.mean(centred * centred, axis=-1, keepdims=True) + norm_eps)
            n = centred * r
            first = (n * g1 + b1).astype(BF16)
            second = (n * g2 + b2).astype(BF16)
            fi2[rows, :] = first
            si2[rows, :] = second
            fit[:, rows] = first.T
            sit[:, rows] = second.T
            if keep:
                nrm[rows, :] = n
                inv[rows, :] = jnp.broadcast_to(r, (128, 128))

    l_x.wait()
    norms(0, True)

    l_wkv.wait()
    for i in range(T // 128):
        rows = pl.ds(128 * i, 128)
        kv = mm(fi2[rows, :], wkv_v[...]) + bkv_v[...]
        kv = jnp.where(lanes < HD, turn(kv, rows, 1.0), kv)
        kv_all[pl.ds(pl.multiple_of(d * T + 128 * i, 128), 128), :] = kv.astype(BF16)
    mine = kv_all.at[block_rows(z, c)]
    s_kv = [rc("kv", o, mine, mine, z_peer(o)) for o in range(1, NZ)]
    for copy in s_kv:
        send(copy)

    def kv_pass(k):
        return rc("kvp", k, kv_all.at[block_rows(k, c)], kv_all.at[block_rows(k, c)], partner)

    s_x.wait_recv()
    norms(T, False)
    l_og.wait()
    s_og.wait_recv()

    rows_v, _ = vec_rows(D, F, pair)
    for pair_of_copies in l_mlp:
        for copy in pair_of_copies:
            copy.wait()

    def x_half(q):
        far = pl.ds(pl.multiple_of(QH // 2 * (1 - xx), 16), QH // 2)
        return rc("wpx", q, wp_part.at[q, far, :], rx_wp.at[q], xnb)

    def z_half(q, slot):
        return rc("wpf", slot, wp_part.at[q, pl.ds(QH, QH), :], rzf.at[slot], to_mate)

    def z_pair(side):
        return rc("wpf", 3 + side, zf_pair.at[side], rzf.at[3], (g, 2 * (far + side) + c))

    z_got = rc("wpf", 3 + lax.rem(z, 2), zf_pair.at[0], rzf.at[3], (g, 2 * far + c))

    def y_chunk(q):
        side = lax.rem(q, 2)
        return rc("wfy", side, wf_part.at[q, pl.ds(0, D2), :], ry_wf.at[side], ynb)

    def x_chunk(q):
        side = lax.div(q, 2)
        return rc("wfx", side, wf_part.at[q, pl.ds(D2, D2), :], rx_wf.at[side], xnb)

    def mlp_chunk(j, carry):
        q = chunk_of(j)
        at = pl.ds(pl.multiple_of(Q * (2 * q + c), 128), Q)
        shift = bfc_v[:, at]
        total = jnp.zeros((1, Q), F32)
        for i in range(2 * T // 128):
            rows = pl.ds(128 * i, 128)
            hidden = mm(si2[rows, :], wfc_v[q]) + shift
            erf_part = 1.0 + lax.erf(hidden * half_root)
            act_s[q, rows, :] = (0.5 * hidden * erf_part).astype(BF16)
            slope = 0.5 * erf_part + hidden * jnp.exp(-0.5 * hidden * hidden) * inv_root_tau
            act_grad = mm(og2[rows, :], wpr_v[q], NT)
            hidden_grad = (act_grad * slope).astype(BF16)
            hg_s[q, rows, :] = hidden_grad
            total = total + jnp.sum(hidden_grad.astype(F32), axis=0, keepdims=True)
        for i in range(Q // 128):
            cols = pl.ds(128 * i, 128)
            wp_part[q, cols, :] = mm(act_s[q, :, cols], og2[...], TN).astype(BF16)
        x_half(q).start()

        @pl.when(q == mate)
        def _():
            z_half(q, 0).start()

        @pl.when(jnp.logical_and(outer, lax.div(q, 2) != lax.div(z, 2)))
        def _():
            z_half(q, 1 + lax.rem(q, 2)).start()

        for i in range(D // 128):
            rows = pl.ds(128 * i, 128)
            wf_part[q, rows, :] = mm(sit[rows, :], hg_s[q]).astype(BF16)

        @pl.when(j < 2)
        def _():
            y_chunk(q).start()

        @pl.when(lax.rem(j, 2) == 0)
        def _():
            x_chunk(q).start()

        at_row = rows_v["b_fc"][0] + Q // 128 * (2 * q + c)
        for i in range(Q // 128):
            vec[pl.ds(at_row + i, 1), :] = total[:, 128 * i : 128 * (i + 1)]
        return carry

    lax.fori_loop(0, NZ, mlp_chunk, 0)
    for copy in s_kv:
        copy.wait_recv()
    for k in range(NZ):
        send(kv_pass(k))

    def mlp_sums(i, carry):
        at = lax.rem(i + T // 128, 2 * T // 128) * 128
        rows = pl.ds(pl.multiple_of(at, 128), 128)
        out = mm(act_s[0, rows, :], wpr_v[0])
        back = mm(hg_s[0, rows, :], wfc_v[0], NT)
        for q in range(1, NZ):
            out = out + mm(act_s[q, rows, :], wpr_v[q])
            back = back + mm(hg_s[q, rows, :], wfc_v[q], NT)
        mlp_all[rows, :] = out
        sec_all[rows, :] = back
        return carry

    lax.fori_loop(0, 2 * T // 128, mlp_sums, 0)
    s_mlp = rc("mlp", 0, mlp_all.at[other], mlp_r, partner)
    send(s_mlp)
    s_sec = rc("sec", 0, sec_all.at[other], sec_r, partner)
    send(s_sec)

    l_wq.wait()
    l_wo.wait()
    for i in range(T // 128):
        rows = pl.ds(128 * i, 128)
        query = mm(fi2[rows, :], wq_v[...]) + vecs[4:5, :]
        grads = mm(og2[rows, :], wo_v[...], NT)
        for t in range(D // pair):
            q_tile = turn(query[:, pair * t : pair * (t + 1)], rows, 1.0).astype(BF16).astype(F32) * 0.125
            o_tile = grads[:, pair * t : pair * (t + 1)]
            low = lanes < HD
            qo[2 * t, rows, :] = jnp.where(low, q_tile, 0.0).astype(BF16)
            qo[2 * t + 1, rows, :] = jnp.where(low, pltpu.roll(q_tile, HD, 1), 0.0).astype(BF16)
            late = pl.ds(T + 128 * i, 128)
            qo[2 * t, late, :] = jnp.where(low, 0.0, pltpu.roll(o_tile, HD, 1)).astype(BF16)
            qo[2 * t + 1, late, :] = jnp.where(low, 0.0, o_tile).astype(BF16)

    row_in = lax.broadcasted_iota(jnp.int32, (block, T), 0)
    query_pos = jnp.broadcast_to(own_pos[0:1, :], (block, T))
    for j in range(S // block):
        key_pos = order_s[0, j] * block + row_in
        bias[pl.ds(block * j, block), :] = jnp.where(key_pos <= query_pos, 0.0, masked_score)

    for k in range(NZ):
        kv_pass(k).wait_recv()
    for j in range(S // 256):
        rows = pl.ds(256 * j, 256)
        kvt[:, rows] = kv_all[rows, :].T
        dkv[rows, :] = jnp.zeros((256, pair), F32)

    near_x = pl.ds(pl.multiple_of(QH // 2 * xx, 16), QH // 2)
    near_y = pl.ds(pl.multiple_of(QH // 4 * yy, 16), QH // 4)
    far_y = pl.ds(pl.multiple_of(QH // 4 * (1 - yy), 16), QH // 4)

    def wp_y(q):
        return rc("wpy", q, wp_s1.at[q, far_y, :], ry_wp.at[q], ynb)

    def wp_first(j):
        q = chunk_in(j)
        x_half(q).wait_recv()
        wp_s1[q] = (wp_part[q, near_x, :].astype(F32) + rx_wp[q].astype(F32)).astype(BF16)
        wp_y(q).start()

    def wp_z(o):
        return rc("wpz", o, zs_wp.at[lax.rem(z + o, NZ)], rz_wp.at[o], z_peer(o))

    def start_wp_z(o):
        wp_z(o).start()

    def wp_second(j):
        q = chunk_y(j)
        wp_y(q).wait_recv()
        zs_wp[q] = (wp_s1[q, near_y, :].astype(F32) + ry_wp[q].astype(F32)).astype(BF16)
        for o in range(1, NZ):
            pl.when(lax.rem(z + o, NZ) == q)(functools.partial(start_wp_z, o))

    slot_wp = 2 * xx + yy

    def wp_g(o):
        return rc("wpg", o, fin_wp, o_wp.at[slot_wp], xy_peer(o, c))

    l_fin = []

    far_zx = pl.ds(pl.multiple_of(QH // 2 * (1 - xx), 16), QH // 2)
    zf_x = rc("zfx", 0, zf_s0.at[far_zx, :], rx_zf, xnb)
    zf_y = rc("zfy", 0, zf_s1.at[far_y, :], ry_zf, ynb)

    def zf_mid():
        @pl.when(jnp.logical_not(outer))
        def _():
            for side in range(2):
                z_half(far + side, 1 + side).wait_recv()
                total = wp_part[far + side, QH:, :].astype(F32) + rzf[1 + side].astype(F32)
                zf_pair[side] = total.astype(BF16)
                z_pair(side).start()

    def zf_first():
        total = wp_part[z, QH:, :].astype(F32)
        z_half(mate, 0).wait_recv()
        z_got.wait_recv()
        total = total + rzf[0].astype(F32) + rzf[3].astype(F32)
        zf_s0[...] = total.astype(BF16)
        zf_x.start()

    def zf_second():
        zf_x.wait_recv()
        zf_s1[...] = (zf_s0[near_x, :].astype(F32) + rx_zf[...].astype(F32)).astype(BF16)
        zf_y.start()

    def zf_third():
        zf_y.wait_recv()
        fin_wp[1] = (zf_s1[near_y, :].astype(F32) + ry_zf[...].astype(F32)).astype(BF16)

    def wp_third():
        total = zs_wp[z].astype(F32)
        for o in range(1, NZ):
            wp_z(o).wait_recv()
            total = total + rz_wp[o].astype(F32)
        fin_wp[0] = total.astype(BF16)
        for o in range(1, NG):
            wp_g(o).start()
        l_fin.append(lc(fin_wp, o_wp.at[slot_wp]))

    def wf_second_send(part):
        return rc("wfs", part, wf_s1.at[part], wf_in.at[part], ynb if part else xnb)

    def wf_first(part):
        if part:
            q = 2 * (1 - yy) + xx
            x_chunk(2 * (1 - yy) + 1 - xx).wait_recv()
            got = rx_wf[1 - yy]
        else:
            q = 2 * yy + 1 - xx
            y_chunk(2 * (1 - yy) + 1 - xx).wait_recv()
            got = ry_wf[1 - xx]
        wf_s1[part] = (wf_part[q, D2 * part : D2 * (part + 1), :].astype(F32) + got.astype(F32)).astype(BF16)
        wf_second_send(part).start()

    def wf_second(part):
        q = 2 * yy + xx
        if part:
            x_chunk(2 * yy + 1 - xx).wait_recv()
            got = rx_wf[yy]
        else:
            y_chunk(2 * (1 - yy) + xx).wait_recv()
            got = ry_wf[xx]
        wf_own[part] = (wf_part[q, D2 * part : D2 * (part + 1), :].astype(F32) + got.astype(F32)).astype(BF16)

    def wf_z(o):
        rows = pl.ds(pl.multiple_of(2 * R * lax.rem(z + o, NZ), 16), 2 * R)
        return rc("wfz", o, zs_wf.at[rows, :], rz_wf.at[o], z_peer(o))

    def start_wf_z(o):
        wf_z(o).start()

    def wf_third(part):
        wf_second_send(part).wait_recv()
        zs_wf[D2 * part : D2 * (part + 1), :] = (
            wf_own[part].astype(F32) + wf_in[part].astype(F32)
        ).astype(BF16)
        for o in range(1, NZ):
            pl.when(lax.div(lax.rem(z + o, NZ), NZ // 2) == part)(functools.partial(start_wf_z, o))

    slot_wf = 2 * yy + xx

    def wf_g(o, core):
        to = c + core - 2 * c * core
        rows = pl.ds(pl.multiple_of(R * to, 16), R)
        return rc("wfg", 2 * o + core, fin_wf.at[rows, :], o_wf.at[slot_wf, c], xy_peer(o, to))

    def wf_fourth():
        total = zs_wf[pl.ds(pl.multiple_of(2 * R * z, 16), 2 * R), :].astype(F32)
        for o in range(1, NZ):
            wf_z(o).wait_recv()
            total = total + rz_wf[o].astype(F32)
        fin_wf[...] = total.astype(BF16)
        for o in range(NG):
            for core in range(2):
                if o or core:
                    wf_g(o, core).start()
        l_fin.append(lc(fin_wf.at[pl.ds(pl.multiple_of(R * c, 16), R), :], o_wf.at[slot_wf, c]))

    far_rx = pl.ds(pl.multiple_of(R // 2 * (1 - xx), 16), R // 2)
    far_ry = pl.ds(pl.multiple_of(R // 2 * (1 - yy), 16), R // 2)
    near_rx = pl.ds(pl.multiple_of(R // 2 * xx, 16), R // 2)
    near_ry = pl.ds(pl.multiple_of(R // 2 * yy, 16), R // 2)
    far_cy = pl.ds(pl.multiple_of(C2 * (1 - yy), 128), C2)
    near_cy = pl.ds(pl.multiple_of(C2 * yy, 128), C2)
    GC = 4 * HD

    def owner_rows(k, core):
        return pl.ds(pl.multiple_of(2 * R * k + R * core, 16), R)

    def group_cols(m):
        return pl.ds(GC * m, GC)

    def side_cols(m, side):
        return pl.ds(pl.multiple_of(GC * m + GC // 2 * side, 128), GC // 2)

    def r_ht(k):
        return rc("ht", k, oht.at[owner_rows(k, 1 - c), :], ht_r.at[k], partner)

    def r_wox(k):
        return rc("wox", k, wo_part.at[k, far_rx, :], rx_wo.at[k], xnb)

    def r_woy(k):
        return rc("woy", k, wo_s1.at[k, :, far_cy], ry_wo.at[k], ynb)

    def r_woz(o):
        return rc("woz", o, zs_wo.at[lax.rem(z + o, NZ)], rz_wo.at[o], z_peer(o))

    def r_qg(m):
        return rc("qg", m, qg2.at[own, group_cols(m)], qg2.at[other, group_cols(m)], partner)

    def r_wqy(m):
        return rc("wqy", m, wq_part.at[:, far_ry, group_cols(m)], ry_wq.at[:, :, group_cols(m)], ynb)

    def r_wqx(m):
        return rc("wqx", m, wq_s1.at[:, :, side_cols(m, 1 - xx)], rx_wq.at[m], xnb)

    def r_wqz(o, m):
        cols = pl.ds(GC // 2 * m, GC // 2)
        return rc(
            "wqz", NZ * m + o, zs_wq.at[lax.rem(z + o, NZ), :, cols], rz_wq.at[o, :, cols], z_peer(o)
        )

    def ht_send(k):
        r_ht(k).start()

    def wo_a(k):
        r_ht(k).wait_recv()
        total = mm(oht[owner_rows(k, c), :], og2[own, :]) + mm(ht_r[k], og2[other, :])
        wo_part[k] = total.astype(BF16)
        r_wox(k).start()

    def wo_b(k):
        r_wox(k).wait_recv()
        wo_s1[k] = (wo_part[k, near_rx, :].astype(F32) + rx_wo[k].astype(F32)).astype(BF16)
        r_woy(k).start()

    def start_woz(o):
        r_woz(o).start()

    def wo_c(k):
        r_woy(k).wait_recv()
        zs_wo[k] = (wo_s1[k, :, near_cy].astype(F32) + ry_wo[k].astype(F32)).astype(BF16)
        for o in range(1, NZ):
            pl.when(lax.rem(z + o, NZ) == k)(functools.partial(start_woz, o))

    def qg_send(m):
        qg2[own, group_cols(m)] = qgt[group_cols(m), :].T
        r_qg(m).start()

    def wq_a(m):
        r_qg(m).wait_recv()
        for k in range(NZ):
            wq_part[k, :, group_cols(m)] = mm(fit[owner_rows(k, c), :], qg2[:, group_cols(m)]).astype(BF16)
        r_wqy(m).start()

    def wq_b(m):
        r_wqy(m).wait_recv()
        cols = group_cols(m)
        wq_s1[:, :, cols] = (wq_part[:, near_ry, cols].astype(F32) + ry_wq[:, :, cols].astype(F32)).astype(BF16)
        r_wqx(m).start()

    def wq_c(m):
        r_wqx(m).wait_recv()
        mine_cols = side_cols(m, xx)
        zs_wq[:, :, GC // 2 * m : GC // 2 * (m + 1)] = (
            wq_s1[:, :, mine_cols].astype(F32) + rx_wq[m].astype(F32)
        ).astype(BF16)
        for o in range(1, NZ):
            r_wqz(o, m).start()

    def at_head(h):
        for when, what in EVENTS:
            pl.when(h == when)(functools.partial(run_event, what))

    def run_event(what):
        {
            "wp0": lambda: wp_first(0),
            "wp1": lambda: wp_first(1),
            "wp2": lambda: wp_first(2),
            "wp3": lambda: wp_first(3),
            "wpy0": lambda: wp_second(0),
            "wpy1": lambda: wp_second(1),
            "wpy2": lambda: wp_second(2),
            "wpy3": lambda: wp_second(3),
            "zf_mid": zf_mid,
            "ht0": lambda: ht_send(0),
            "ht1": lambda: ht_send(1),
            "ht2": lambda: ht_send(2),
            "woa0": lambda: wo_a(0),
            "woa1": lambda: wo_a(1),
            "woa2": lambda: wo_a(2),
            "wob0": lambda: wo_b(0),
            "wob1": lambda: wo_b(1),
            "woc0": lambda: wo_c(0),
            "qg0": lambda: qg_send(0),
            "qg1": lambda: qg_send(1),
            "wqa0": lambda: wq_a(0),
            "wqa1": lambda: wq_a(1),
            "wqb0": lambda: wq_b(0),
            "wqc0": lambda: wq_c(0),
            "zf_first": zf_first,
            "zf_second": zf_second,
            "zf_third": zf_third,
            "wf_first0": lambda: wf_first(0),
            "wf_second0": lambda: wf_second(0),
            "wf_third0": lambda: wf_third(0),
            "wf_first1": lambda: wf_first(1),
            "wf_second1": lambda: wf_second(1),
            "wf_third1": lambda: wf_third(1),
        }[what]()

    KC = 256

    def head(h, carry):
        at_head(h)
        both = qo[h]
        top = jnp.full((8, T), -3e38, F32)
        for k in range(S // KC):
            rows = pl.ds(KC * k, KC)
            sd = mm(kv_all[rows, :], both, NT)
            score = sd[:, :T] + bias[rows, :]
            sbuf[rows, :] = score
            dbuf[rows, :] = sd[:, T:]
            top = jnp.maximum(top, jnp.max(score.reshape(KC // 8, 8, T), axis=0))
        top = jnp.max(top, axis=0, keepdims=True)
        norm = jnp.zeros((8, T), F32)
        delta = jnp.zeros((8, T), F32)
        for k in range(S // KC):
            rows = pl.ds(KC * k, KC)
            e = jnp.exp(sbuf[rows, :] - top)
            sbuf[rows, :] = e
            norm = norm + jnp.sum(e.reshape(KC // 8, 8, T), axis=0)
            delta = delta + jnp.sum((e * dbuf[rows, :]).reshape(KC // 8, 8, T), axis=0)
        scale = 1.0 / jnp.sum(norm, axis=0, keepdims=True)
        delta = jnp.sum(delta, axis=0, keepdims=True) * scale
        for k in range(S // KC):
            rows = pl.ds(KC * k, KC)
            p = sbuf[rows, :] * scale
            dsp[rows, :T] = (p * (dbuf[rows, :] - delta)).astype(BF16)
            dsp[rows, T:] = p.astype(BF16)
        for k in range(S // KC):
            rows = pl.ds(KC * k, KC)
            dkv[rows, :] += mm(dsp[rows, :], both)
        result = mm(kvt[...], dsp[...])
        rows = pl.ds(pl.multiple_of(HD * h, HD), HD)
        oht[rows, :] = result[HD:, T:].astype(BF16)
        back = result[:HD, :T] * 0.125
        a, b, rest = back[: ROT // 2], back[ROT // 2 : ROT], back[ROT:]
        ct, st = cost[...], sint[...]
        qgt[rows, :] = jnp.concatenate([a * ct + b * st, b * ct - a * st, rest], axis=0).astype(BF16)
        return carry

    lax.fori_loop(0, H, head, 0)

    dkv_b[...] = dkv[...].astype(BF16)
    s_dk = []
    for k in range(NZ):
        s_dk.append(rc("dk", k, dkv_b.at[block_rows(k, 1 - c), :], rdk.at[k], partner))
        send(s_dk[-1])

    ht_send(3)
    qg_send(2)

    for copy in s_dk:
        copy.wait_recv()
    s_dkv = []
    for o in range(1, NZ):
        k = lax.rem(z + o, NZ)
        dks[o] = (dkv[block_rows(k, c), :] + rdk[k].astype(F32)).astype(BF16)
        s_dkv.append(rc("dkv", o, dks.at[o], rdkv.at[o], z_peer(o)))
        send(s_dkv[-1])

    def put(name, row):
        at, count = rows_v[name]
        for i in range(count):
            vec[at + i : at + i + 1, :] = row[:, 128 * i : 128 * (i + 1)]

    wo_a(3)
    wq_a(2)
    wq_b(1)
    wo_b(2)
    wo_c(1)

    s_mlp.wait_recv()
    for i in range(T // 128):
        rows = pl.ds(128 * i, 128)
        branch = mm(oht[:, rows], wo_v[...], TN) + vecs[5:6, :]
        mlp = (mlp_all[rows, :] + mlp_r[rows, :]) + vecs[6:7, :]
        lo_v[rows, :] = ((x2[rows, :].astype(F32) + branch) + mlp).astype(BF16)
    l_lo = lc(lo_v, o_lo)

    s_sec.wait_recv()
    sums = [jnp.zeros((1, D), F32) for _ in range(6)]
    for i in range(T // 128):
        rows = pl.ds(128 * i, 128)
        ig_v[rows, :] = mm(qg2[rows, :], wq_v[...], NT)
        second_grad = sec_all[rows, :] + sec_r[rows, :]
        sec_all[rows, :] = second_grad * g2
        up = og2[rows, :].astype(F32)
        for k, value in enumerate((qg2[rows, :].astype(F32), up, second_grad * nrm[rows, :], second_grad)):
            sums[2 + k] = sums[2 + k] + jnp.sum(value, axis=0, keepdims=True)

    wo_b(3)
    wq_b(2)
    zf_second()
    wq_c(1)
    wo_c(2)

    l_kvg.wait()
    for copy in s_dkv:
        copy.wait_recv()
    kv_grads = []
    for i in range(T // 128):
        rows = pl.ds(128 * i, 128)
        total = dkv[pl.ds(pl.multiple_of(d * T + 128 * i, 128), 128), :] + rdk[z, rows, :].astype(F32)
        for o in range(1, NZ):
            total = total + rdkv[o, rows, :].astype(F32)
        total = total + kvg_v[rows, :].astype(F32)
        kv_grads.append(jnp.where(lanes < HD, turn(total, rows, -1.0), total).astype(BF16))
        kvg2[rows, :] = kv_grads[-1]
    s_kvg = rc("kvg", 0, kvg2.at[own], kvg2.at[other], partner)
    send(s_kvg)
    put("b_keyval", jnp.sum(jnp.concatenate(kv_grads, axis=0).astype(F32), axis=0, keepdims=True))

    for i in range(T // 128):
        rows = pl.ds(128 * i, 128)
        first_grad = ig_v[rows, :] + mm(kv_grads[i], wkv_v[...], NT)
        n = nrm[rows, :]
        u = first_grad * g1 + sec_all[rows, :]
        back = u - jnp.mean(u, axis=-1, keepdims=True) - n * jnp.mean(u * n, axis=-1, keepdims=True)
        ig_v[rows, :] = og2[rows, :].astype(F32) + inv[rows, 0:1] * back
        for k, value in enumerate((first_grad * n, first_grad)):
            sums[k] = sums[k] + jnp.sum(value, axis=0, keepdims=True)
    l_ig = lc(ig_v, o_ig)
    for name, row in zip(("ln1_gain", "ln1_bias", "b_query", "column", "ln2_gain", "ln2_bias"), sums):
        put(name, row)
    s_vec = []
    for o in range(1, NSP):
        rows = pl.ds(pl.multiple_of(lax.rem(d + o, NSP) * 8, 8), 8)
        s_vec.append(rc("vec", o, vec.at[rows, :], rvec.at[o], sp_peer(o)))
        send(s_vec[-1])

    s_kvg.wait_recv()
    s_wkv = []
    for k in range(NZ):
        rows = pl.ds(pl.multiple_of(2 * R * k + R * c, 16), R)
        wkv_part[k] = mm(fit[rows, :], kvg2[...])
        wkv_b[k] = wkv_part[k].astype(BF16)
    for o in range(1, NZ):
        s_wkv.append(rc("wkv", o, wkv_b.at[lax.rem(z + o, NZ)], rkv.at[o], z_peer(o)))
        send(s_wkv[-1])

    wo_c(3)
    wq_c(2)
    zf_third()
    wp_third()
    wf_fourth()

    for copy in s_wkv:
        copy.wait_recv()
    total = wkv_part[z]
    for o in range(1, NZ):
        total = total + rkv[o].astype(F32)
    sm[g, :R, :] = total
    for copy in s_vec:
        copy.wait_recv()
    total = vec[pl.ds(pl.multiple_of(d * 8, 8), 8), :]
    for o in range(1, NSP):
        total = total + rvec[o]
    sm[g, R:, :] = total
    s_sm = [rc("sm", o, sm.at[g], sm.at[g], xy_peer(o, c)) for o in range(1, NG)]
    for copy in s_sm:
        send(copy)

    total = zs_wo[z].astype(F32)
    for o in range(1, NZ):
        r_woz(o).wait_recv()
        total = total + rz_wo[o].astype(F32)
    fin_wo[...] = total.astype(BF16)
    s_wog = [rc("wog", o, fin_wo, o_wo.at[xx, yy], xy_peer(o, c)) for o in range(1, NG)]
    for copy in s_wog:
        send(copy)
    l_fo = lc(fin_wo, o_wo.at[xx, yy])
    total = zs_wq[z].astype(F32)
    for o in range(1, NZ):
        for m in range(H // 4):
            r_wqz(o, m).wait_recv()
        total = total + rz_wq[o].astype(F32)
    fin_wq[...] = total.astype(BF16)
    s_wqg = [rc("wqg", o, fin_wq, o_wq.at[yy, xx], xy_peer(o, c)) for o in range(1, NG)]
    for copy in s_wqg:
        send(copy)
    l_fq = lc(fin_wq, o_wq.at[yy, xx])

    for copy in s_sm:
        copy.wait_recv()
    total = sm[0]
    for k in range(1, NG):
        total = total + sm[k]
    fin_kv[...] = total[:R]
    fin_vec[...] = total[R:]
    l_kv = lc(fin_kv, o_wkv)
    mine8 = pl.ds(pl.multiple_of(d * 8, 8), 8)
    s_vg = [rc("vg", o, fin_vec, o_vec.at[mine8, :], sp_peer(o)) for o in range(1, NSP)]
    for copy in s_vg:
        send(copy)
    l_vg = lc(fin_vec, o_vec.at[mine8, :])

    for o in range(1, NG):
        wp_g(o).wait_recv()
    for o in range(NG):
        for core in range(2):
            if o or core:
                wf_g(o, core).wait_recv()
    for copy in s_wog + s_wqg + s_vg:
        copy.wait_recv()
    for copy in started:
        copy.wait_send()
    for q in range(NZ):
        x_half(q).wait_send()
        wp_y(q).wait_send()
    for k in range(2):
        y_chunk(2 * (1 - yy) + k).wait_send()
        x_chunk(2 * k + 1 - xx).wait_send()
        wf_second_send(k).wait_send()
    for k in range(NZ):
        r_ht(k).wait_send()
        r_wox(k).wait_send()
        r_woy(k).wait_send()
    for m in range(H // 4):
        r_qg(m).wait_send()
        r_wqy(m).wait_send()
        r_wqx(m).wait_send()
    for o in range(1, NZ):
        r_woz(o).wait_send()
        for m in range(H // 4):
            r_wqz(o, m).wait_send()
    z_half(mate, 0).wait_send()

    @pl.when(outer)
    def _():
        for side in range(2):
            z_half(far + side, 1 + side).wait_send()

    @pl.when(jnp.logical_not(outer))
    def _():
        for side in range(2):
            z_pair(side).wait_send()

    zf_x.wait_send()
    zf_y.wait_send()
    for o in range(1, NZ):
        wp_z(o).wait_send()
        wf_z(o).wait_send()
    for o in range(1, NG):
        wp_g(o).wait_send()
    for o in range(NG):
        for core in range(2):
            if o or core:
                wf_g(o, core).wait_send()
    for copy in l_fin + [l_lo, l_ig, l_kv, l_vg, l_fo, l_fq]:
        copy.wait()


EVENTS = (
    (0, "wp0"),
    (1, "wf_first0"),
    (2, "wf_first1"),
    (2, "wp1"),
    (3, "zf_mid"),
    (3, "wf_second0"),
    (4, "wp2"),
    (4, "ht0"),
    (5, "wpy0"),
    (5, "woa0"),
    (5, "qg0"),
    (6, "wf_second1"),
    (6, "wp3"),
    (6, "wqa0"),
    (7, "wpy1"),
    (7, "wpy2"),
    (7, "wf_third1"),
    (7, "ht1"),
    (8, "wpy3"),
    (8, "woa1"),
    (8, "qg1"),
    (9, "wf_third0"),
    (9, "wqa1"),
    (9, "wob0"),
    (9, "wqb0"),
    (9, "ht2"),
    (10, "woa2"),
    (10, "zf_first"),
    (11, "woc0"),
    (11, "wqc0"),
    (11, "wob1"),
)


def finish_kernel(
    dims, wp_h, wf_h, wo_h, wq_h, wkv_h, vec_h, lo_h, ig_h,
    layer_out, input_grad, ln1_gain, ln1_bias, w_query, b_query, w_keyval, b_keyval,
    w_attn_out, b_attn_out, ln2_gain, ln2_bias, w_fc, b_fc, w_proj, b_proj,
    wp, wf, wo, wq, wkv, vec, lo, ig, fc_v, proj_v, out_v, query_v, isem, osem,
):
    T, D, F, S, NSP, NG = dims
    Q, R, C2 = F // NSP, D // NSP, D // 2
    arrive = {}
    for i, (name, src, dst) in enumerate(
        (("wf", wf_h, wf), ("wp", wp_h, wp), ("ig", ig_h, ig), ("lo", lo_h, lo), ("vec", vec_h, vec),
         ("wo", wo_h, wo), ("wq", wq_h, wq), ("wkv", wkv_h, wkv))
    ):
        arrive[name] = pltpu.make_async_copy(src, dst, isem.at[i])
        arrive[name].start()
    leave = []

    def put_out(src, dst):
        leave.append(pltpu.make_async_copy(src, dst, osem.at[len(leave)]))
        leave[-1].start()

    arrive["wf"].wait()
    for k in range(NG):
        for core in range(2):
            at = Q * (2 * k + core)
            fc_v[:, at : at + Q] = wf[k, core].astype(F32)
    put_out(fc_v, w_fc)
    arrive["wp"].wait()
    rows = Q // 2 // NG
    for k in range(NG):
        for part in range(2):
            at = Q // 2 * part + rows * k
            proj_v[at : at + rows, :] = wp[k, part].astype(F32)
    put_out(proj_v, w_proj)
    arrive["ig"].wait()
    put_out(ig, input_grad)
    arrive["lo"].wait()
    put_out(lo, layer_out)
    arrive["wo"].wait()
    arrive["wq"].wait()
    for a in range(2):
        for b in range(2):
            rows = slice(R // 2 * a, R // 2 * (a + 1))
            cols = slice(C2 * b, C2 * (b + 1))
            out_v[rows, cols] = wo[a, b].astype(F32)
            for m in range(H // 4):
                at = 4 * HD * m + 2 * HD * b
                query_v[rows, at : at + 2 * HD] = wq[a, b, :, 2 * HD * m : 2 * HD * (m + 1)].astype(F32)
    put_out(out_v, w_attn_out)
    put_out(query_v, w_query)
    arrive["wkv"].wait()
    put_out(wkv, w_keyval)
    arrive["vec"].wait()
    rows_v, _ = vec_rows(D, F, 2 * HD)
    for name, out in (
        ("ln1_gain", ln1_gain), ("ln1_bias", ln1_bias), ("b_query", b_query), ("b_keyval", b_keyval),
        ("column", b_attn_out), ("column", b_proj), ("ln2_gain", ln2_gain), ("ln2_bias", ln2_bias),
        ("b_fc", b_fc),
    ):
        at, count = rows_v[name]
        out[...] = jnp.concatenate([vec[at + i : at + i + 1, :] for i in range(count)], axis=1).reshape(
            128 * count
        )
    for copy in leave:
        copy.wait()


def fused_local(n_grp, n_sp, *args):
    layer_input, block_order = args[0], args[1]
    T, D = layer_input.shape
    F = args[12].shape[1]
    S = T * n_sp
    NZ, NG, NSP = n_sp // 2, n_grp, n_sp
    Q, R, C2, pair = F // n_sp, D // n_sp, D // 2, 2 * HD
    dims = (T, D, F, S, NSP, NG)
    V = pltpu.VMEM
    scratch = [
        V((8, D), F32), V((1, pair), F32), V((1, F), F32),
        V((2 * T, D), BF16), V((2 * T, D), BF16), V((2 * T, D), BF16), V((2 * T, D), BF16),
        V((D, 2 * T), BF16), V((D, 2 * T), BF16), V((T, D), F32), V((T, 128), F32),
        V((D, pair), BF16), V((D, D), BF16), V((D, D), BF16), V((NZ, D, Q), BF16), V((NZ, Q, D), BF16),
        V((T, pair), BF16), V((NZ, 2 * T, Q), BF16), V((NZ, 2 * T, Q), BF16),
        V((2 * T, D), F32), V((2 * T, D), F32), V((T, D), F32), V((T, D), F32),
        V((NZ, Q, D), BF16), V((NZ, Q // 4, D), BF16), V((NZ, Q // 4, D), BF16), V((NZ, Q // 8, D), BF16),
        V((NZ, Q // 8, D), BF16), V((NZ, Q // 8, D), BF16), V((NZ, Q // 2, D), BF16), V((2, Q // 2, D), BF16),
        V((Q // 2, D), BF16),
        V((Q // 4, D), BF16), V((Q // 4, D), BF16), V((Q // 8, D), BF16), V((2, Q // 8, D), BF16),
        V((NZ, D, Q), BF16), V((2, D // 2, Q), BF16), V((2, D // 2, Q), BF16), V((2, D // 2, Q), BF16),
        V((2, D // 2, Q), BF16), V((2, D // 2, Q), BF16), V((D, Q), BF16), V((NZ, 2 * R, Q), BF16), V((2 * R, Q), BF16),
        V((S, pair), BF16), V((pair, S), BF16), V((H, 2 * T, pair), BF16), V((S, T), F32), V((S, T), F32),
        V((S, T), F32), V((S, 2 * T), BF16), V((S, pair), F32), V((S, pair), BF16), V((NZ, T, pair), BF16),
        V((NZ, T, pair), BF16), V((NZ, T, pair), BF16), V((2 * T, pair), BF16),
        V((D, T), BF16), V((D, T), BF16), V((NZ, R, T), BF16), V((2 * T, D), BF16),
        V((NZ, R, D), BF16), V((NZ, R // 2, D), BF16), V((NZ, R // 2, D), BF16), V((NZ, R // 2, C2), BF16),
        V((NZ, R // 2, C2), BF16), V((NZ, R // 2, C2), BF16), V((R // 2, C2), BF16),
        V((NZ, R, D), BF16), V((NZ, R // 2, D), BF16), V((NZ, R // 2, D), BF16),
        V((H // 4, NZ, R // 2, 2 * HD), BF16),
        V((NZ, R // 2, C2), BF16), V((NZ, R // 2, C2), BF16), V((R // 2, C2), BF16),
        V((8 * NSP, 128), F32), V((NSP, 8, 128), F32), V((NZ, R, pair), F32), V((NZ, R, pair), BF16),
        V((NZ, R, pair), BF16), V((NG, R + 8, 128), F32), V((R, 128), F32), V((8, 128), F32),
        V((T, D), BF16), V((T, D), F32), V((T, pair), F32), V((T, pair), F32), V((8, T), F32), V((8, T), F32),
        pltpu.SemaphoreType.DMA((40,)), pltpu.SemaphoreType.DMA((160,)), pltpu.SemaphoreType.DMA((160,)),
    ]
    any_spec = pl.BlockSpec(memory_space=pl.ANY)
    shape = jax.ShapeDtypeStruct
    held = pl.pallas_call(
        functools.partial(fused_kernel, dims),
        out_shape=(
            shape((NG, 2, Q // 8, D), BF16),
            shape((NG, 2, R, Q), BF16),
            shape((2, 2, R // 2, C2), BF16),
            shape((2, 2, R // 2, C2), BF16),
            shape((R, pair), F32),
            shape((8 * NSP, 128), F32),
            shape((T, D), BF16),
            shape((T, D), F32),
        ),
        in_specs=[any_spec, pl.BlockSpec(memory_space=pltpu.SMEM)] + [any_spec] * 16,
        out_specs=(any_spec,) * 8,
        scratch_shapes=scratch,
        compiler_params=pltpu.CompilerParams(
            collective_id=0, has_side_effects=True, vmem_limit_bytes=67043328
        ),
        name="fused_layer",
    )(*args)
    vmem_spec = pl.BlockSpec(memory_space=pltpu.VMEM)
    row = shape((D,), F32)
    return pl.pallas_call(
        functools.partial(finish_kernel, dims),
        out_shape=(
            shape((T, D), BF16), shape((T, D), F32), row, row, shape((R, D), F32), row, shape((R, pair), F32),
            shape((pair,), F32), shape((R, D), F32), row, row, row, shape((R, F), F32), shape((F,), F32),
            shape((Q, D), F32), row,
        ),
        in_specs=[any_spec] * 8,
        out_specs=tuple(any_spec if k in (0, 1, 4, 6, 8, 12, 14) else vmem_spec for k in range(16)),
        scratch_shapes=[
            V((NG, 2, Q // 8, D), BF16), V((NG, 2, R, Q), BF16), V((2, 2, R // 2, C2), BF16),
            V((2, 2, R // 2, C2), BF16), V((R, pair), F32), V((8 * NSP, 128), F32), V((T, D), BF16), V((T, D), F32),
            V((R, F), F32), V((Q, D), F32), V((R, D), F32), V((R, D), F32),
            pltpu.SemaphoreType.DMA((8,)), pltpu.SemaphoreType.DMA((8,)),
        ],
        compiler_params=pltpu.CompilerParams(vmem_limit_bytes=64000000),
        name="finish",
    )(*held)


def fits(mesh, args):
    n_grp, n_sp = mesh.shape["grp"], mesh.shape["sp"]
    tokens, width = args[0].shape
    seqs, blocks = args[1].shape
    ff = args[12].shape[1]
    rows = tokens // (n_grp * n_sp)
    return (
        n_grp == 4
        and n_sp == 2 * n_grp
        and seqs == n_grp
        and blocks == 2 * n_sp
        and rows == 2 * 128
        and width == H * HD
        and width % (32 * n_sp) == 0
        and ff % (128 * n_sp) == 0
        and width % 128 == 0
        and sum(count for _, count in vec_rows(width, ff, 2 * HD)[0].values()) <= 8 * n_sp
    )


def layer_norm(values, gain_row, shift_row):
    centre = jnp.mean(values, axis=-1, keepdims=True)
    centred = values - centre
    spread = jnp.mean(centred * centred, axis=-1, keepdims=True)
    inverse_dev = lax.rsqrt(spread + norm_eps)
    normed = centred * inverse_dev
    return (normed * gain_row + shift_row, normed, inverse_dev)


def norm_back(upstream, normed, inverse_dev, gain_row):
    scaled = upstream * gain_row
    return inverse_dev * (
        scaled
        - jnp.mean(scaled, axis=-1, keepdims=True)
        - normed * jnp.mean(scaled * normed, axis=-1, keepdims=True)
    )


def rotary_tables(position):
    half_rot = ROT // 2
    frequency = jnp.exp(jnp.arange(half_rot, dtype=jnp.float32) * (-2.0 * rotary_base_log / ROT))
    angles = position.astype(jnp.float32)[:, None] * 0.25 * frequency[None, :]
    return (jnp.cos(angles), jnp.sin(angles))


def rotate(values, cosine, sine_table):
    half_rot = ROT // 2
    cos_rows = cosine[:, None, :]
    sin_rows = sine_table[:, None, :]
    lower_half = values[..., :half_rot]
    upper_half = values[..., half_rot:ROT]
    return jnp.concatenate(
        [
            lower_half * cos_rows - upper_half * sin_rows,
            upper_half * cos_rows + lower_half * sin_rows,
            values[..., ROT:],
        ],
        axis=-1,
    )


def rotate_back(values, cosine, sine_table):
    half_rot = ROT // 2
    cos_rows = cosine[:, None, :]
    sin_rows = sine_table[:, None, :]
    lower_half = values[..., :half_rot]
    upper_half = values[..., half_rot:ROT]
    return jnp.concatenate(
        [
            lower_half * cos_rows + upper_half * sin_rows,
            upper_half * cos_rows - lower_half * sin_rows,
            values[..., ROT:],
        ],
        axis=-1,
    )


def key_scores(query_rows, row_pos, kv_sequence, block_index, block_rows):
    key_start = block_index * block_rows
    key_slice = lax.dynamic_slice_in_dim(kv_sequence, key_start, block_rows, 0)
    raw_scores = (
        jnp.einsum("rd,kd->rk", query_rows, key_slice[:, :HD], preferred_element_type=jnp.float32)
        * 0.125
    )
    key_pos = key_start + lax.broadcasted_iota(jnp.int32, (1, block_rows), 1)
    return (jnp.where(key_pos <= row_pos[:, None], raw_scores, masked_score), key_slice)


def attention_forward(query_tiles, tile_pos, kv_sorted):
    pair_count = query_tiles.shape[0]
    pairs_per_seq = pair_count // kv_sorted.shape[0]
    block_rows = min(score_block, kv_sorted.shape[1])

    def one_pair(inputs):
        query_rows, row_pos, pair_index = inputs
        kv_sequence = kv_sorted[pair_index // pairs_per_seq]
        key_blocks = jnp.max(row_pos) // block_rows + 1
        row_count = query_rows.shape[0]

        def max_pass(block_index, carried):
            running_max, running_sum = carried
            masked, key_slice = key_scores(
                query_rows, row_pos, kv_sequence, block_index, block_rows
            )
            new_max = jnp.maximum(running_max, jnp.max(masked, axis=1, keepdims=True))
            running_sum = running_sum * jnp.exp(running_max - new_max) + jnp.sum(
                jnp.exp(masked - new_max), axis=1, keepdims=True
            )
            return (new_max, running_sum)

        start_max = jnp.full((row_count, 1), masked_score, jnp.float32)
        running_max, running_sum = lax.fori_loop(
            0, key_blocks, max_pass, (start_max, jnp.zeros((row_count, 1), jnp.float32))
        )
        log_total = running_max + jnp.log(running_sum)

        def value_pass(block_index, output):
            masked, key_slice = key_scores(
                query_rows, row_pos, kv_sequence, block_index, block_rows
            )
            weights = jnp.exp(masked - log_total).astype(jnp.bfloat16)
            return output + jnp.dot(weights, key_slice[:, HD:], preferred_element_type=jnp.float32)

        output = lax.fori_loop(0, key_blocks, value_pass, jnp.zeros((row_count, HD), jnp.float32))
        return (output, log_total)

    return lax.map(one_pair, (query_tiles, tile_pos, jnp.arange(pair_count, dtype=jnp.int32)))


def attention_backward(query_tiles, tile_pos, grad_tiles, log_totals, kv_sorted):
    pair_count = query_tiles.shape[0]
    pairs_per_seq = pair_count // kv_sorted.shape[0]
    block_rows = min(score_block, kv_sorted.shape[1])
    pair_width = kv_sorted.shape[2]

    def one_pair(key_grads, inputs):
        query_rows, row_pos, grad_rows, log_total, pair_index = inputs
        sequence = pair_index // pairs_per_seq
        kv_sequence = kv_sorted[sequence]
        key_blocks = jnp.max(row_pos) // block_rows + 1
        row_count = query_rows.shape[0]

        def pass_terms(block_index):
            masked, key_slice = key_scores(
                query_rows, row_pos, kv_sequence, block_index, block_rows
            )
            weights = jnp.exp(masked - log_total)
            weight_grads = jnp.einsum(
                "rd,kd->rk", grad_rows, key_slice[:, HD:], preferred_element_type=jnp.float32
            )
            return (weights, weight_grads, key_slice)

        def delta_pass(block_index, row_delta):
            weights, weight_grads, unused_slice = pass_terms(block_index)
            return row_delta + jnp.sum(weights * weight_grads, axis=1, keepdims=True)

        row_delta = lax.fori_loop(0, key_blocks, delta_pass, jnp.zeros((row_count, 1), jnp.float32))

        def grad_pass(block_index, carried):
            query_grad, sequence_grads = carried
            weights, weight_grads, key_slice = pass_terms(block_index)
            score_grad = (weights * (weight_grads - row_delta)).astype(jnp.bfloat16)
            query_grad = (
                query_grad
                + jnp.dot(score_grad, key_slice[:, :HD], preferred_element_type=jnp.float32) * 0.125
            )
            key_part = (
                jnp.einsum("rk,rd->kd", score_grad, query_rows, preferred_element_type=jnp.float32)
                * 0.125
            )
            value_part = jnp.einsum(
                "rk,rd->kd",
                weights.astype(jnp.bfloat16),
                grad_rows,
                preferred_element_type=jnp.float32,
            )
            key_start = block_index * block_rows
            previous = lax.dynamic_slice(
                sequence_grads, (sequence, key_start, 0), (1, block_rows, pair_width)
            )
            updated = previous + jnp.concatenate([key_part, value_part], axis=1)[None]
            return (
                query_grad,
                lax.dynamic_update_slice(sequence_grads, updated, (sequence, key_start, 0)),
            )

        query_grad, key_grads = lax.fori_loop(
            0, key_blocks, grad_pass, (jnp.zeros((row_count, HD), jnp.float32), key_grads)
        )
        return (key_grads, query_grad)

    start_grads = jnp.zeros(kv_sorted.shape, jnp.float32)
    key_grads, query_grads = lax.scan(
        one_pair,
        start_grads,
        (query_tiles, tile_pos, grad_tiles, log_totals, jnp.arange(pair_count, dtype=jnp.int32)),
    )
    return (query_grads, key_grads)


def local(
    layer_input,
    block_order,
    ln1_gain,
    ln1_bias,
    w_query,
    b_query,
    w_keyval,
    b_keyval,
    w_attn_out,
    b_attn_out,
    ln2_gain,
    ln2_bias,
    w_fc,
    b_fc,
    w_proj,
    b_proj,
    kv_grad,
    out_grad,
):
    my_rank = lax.axis_index("sp")
    seq_count = block_order.shape[0]
    block_count = block_order.shape[1]
    token_count = layer_input.shape[0]
    shard_len = token_count // seq_count
    block_len = shard_len // 2
    model_width = layer_input.shape[1]
    pair_width = 2 * HD
    pair_count = 2 * seq_count
    input_float = layer_input.astype(jnp.float32)
    first_in, first_hat, first_inv = layer_norm(input_float, ln1_gain, ln1_bias)
    first_low = first_in.astype(jnp.bfloat16)
    query_pre = jnp.dot(first_low, w_query, preferred_element_type=jnp.float32) + b_query
    keyval_pre = jnp.dot(first_low, w_keyval, preferred_element_type=jnp.float32) + b_keyval
    offsets = jnp.arange(block_len, dtype=jnp.int32)
    own_blocks = lax.dynamic_slice_in_dim(block_order, 2 * my_rank, 2, 1)
    own_pos = (own_blocks[:, :, None] * block_len + offsets[None, None, :]).reshape(token_count)
    cosine, sine_table = rotary_tables(own_pos)
    query_use = (
        rotate(query_pre.reshape(token_count, H, HD), cosine, sine_table)
        .reshape(token_count, model_width)
        .astype(jnp.bfloat16)
    )
    key_rot = rotate(keyval_pre[:, None, :HD], cosine, sine_table)[:, 0, :]
    keyval_use = jnp.concatenate([key_rot, keyval_pre[:, HD:]], axis=1).astype(jnp.bfloat16)
    gathered = lax.all_gather(
        keyval_use.reshape(seq_count, shard_len, pair_width), "sp", axis=1, tiled=True
    )
    seq_len = gathered.shape[1]
    block_sorter = jnp.argsort(block_order, axis=1)
    kv_sorted = jnp.take_along_axis(
        gathered.reshape(seq_count, block_count, block_len, pair_width),
        block_sorter[:, :, None, None],
        axis=1,
    ).reshape(seq_count, seq_len, pair_width)
    row_pos = own_pos.reshape(seq_count, shard_len)
    query_rows = query_use.reshape(seq_count, shard_len, model_width)
    query_tiles = query_rows.reshape(pair_count, block_len * H, HD)
    tile_pos = jnp.repeat(row_pos.reshape(pair_count, block_len), H, axis=1)
    head_rows, log_totals = attention_forward(query_tiles, tile_pos, kv_sorted)
    heads_sorted = head_rows.reshape(seq_count, shard_len, model_width).astype(jnp.bfloat16)
    heads_local = heads_sorted.reshape(token_count, model_width)
    attn_branch = jnp.dot(heads_local, w_attn_out, preferred_element_type=jnp.float32) + b_attn_out
    second_in, second_hat, second_inv = layer_norm(input_float, ln2_gain, ln2_bias)
    second_low = second_in.astype(jnp.bfloat16)
    hidden = jnp.dot(second_low, w_fc, preferred_element_type=jnp.float32) + b_fc
    erf_part = 1.0 + lax.erf(hidden * half_root)
    activated = (0.5 * hidden * erf_part).astype(jnp.bfloat16)
    mlp_branch = jnp.dot(activated, w_proj, preferred_element_type=jnp.float32) + b_proj
    layer_out = (input_float + attn_branch + mlp_branch).astype(jnp.bfloat16)
    upstream = out_grad.astype(jnp.float32)
    column_sum = jnp.sum(upstream, axis=0)
    w_proj_grad = jnp.einsum("tf,td->fd", activated, out_grad, preferred_element_type=jnp.float32)
    act_grad = jnp.einsum("td,fd->tf", out_grad, w_proj, preferred_element_type=jnp.float32)
    gelu_slope = 0.5 * erf_part + hidden * jnp.exp(-0.5 * hidden * hidden) * inv_root_tau
    hidden_grad = (act_grad * gelu_slope).astype(jnp.bfloat16)
    w_fc_grad = jnp.einsum("td,tf->df", second_low, hidden_grad, preferred_element_type=jnp.float32)
    b_fc_grad = jnp.sum(hidden_grad.astype(jnp.float32), axis=0)
    second_grad = jnp.einsum("tf,df->td", hidden_grad, w_fc, preferred_element_type=jnp.float32)
    w_attn_out_grad = jnp.einsum(
        "te,td->ed", heads_local, out_grad, preferred_element_type=jnp.float32
    )
    heads_grad = jnp.einsum(
        "td,ed->te", out_grad, w_attn_out, preferred_element_type=jnp.float32
    ).astype(jnp.bfloat16)
    grad_rows = heads_grad.reshape(seq_count, shard_len, model_width)
    grad_tiles = grad_rows.reshape(pair_count, block_len * H, HD)
    query_tile_grads, sorted_kv_grads = attention_backward(
        query_tiles, tile_pos, grad_tiles, log_totals, kv_sorted
    )
    query_rot_rows = query_tile_grads.reshape(seq_count, shard_len, model_width)
    query_rot_grad = query_rot_rows.reshape(token_count, model_width)
    query_grad = (
        rotate_back(query_rot_grad.reshape(token_count, H, HD), cosine, sine_table)
        .reshape(token_count, model_width)
        .astype(jnp.bfloat16)
    )
    stored_kv_grads = jnp.take_along_axis(
        sorted_kv_grads.reshape(seq_count, block_count, block_len, pair_width),
        block_order[:, :, None, None],
        axis=1,
    ).reshape(seq_count, seq_len, pair_width)
    own_kv_grad = lax.psum_scatter(stored_kv_grads, "sp", scatter_dimension=1, tiled=True).reshape(
        token_count, pair_width
    ) + kv_grad.astype(jnp.float32)
    key_pre_grad = rotate_back(own_kv_grad[:, None, :HD], cosine, sine_table)[:, 0, :]
    keyval_grad = jnp.concatenate([key_pre_grad, own_kv_grad[:, HD:]], axis=1).astype(jnp.bfloat16)
    w_query_grad = jnp.einsum(
        "td,te->de", first_low, query_grad, preferred_element_type=jnp.float32
    )
    b_query_grad = jnp.sum(query_grad.astype(jnp.float32), axis=0)
    w_keyval_grad = jnp.einsum(
        "td,te->de", first_low, keyval_grad, preferred_element_type=jnp.float32
    )
    b_keyval_grad = jnp.sum(keyval_grad.astype(jnp.float32), axis=0)
    first_grad = jnp.einsum(
        "te,de->td", query_grad, w_query, preferred_element_type=jnp.float32
    ) + jnp.einsum("te,de->td", keyval_grad, w_keyval, preferred_element_type=jnp.float32)
    first_back = norm_back(first_grad, first_hat, first_inv, ln1_gain)
    second_back = norm_back(second_grad, second_hat, second_inv, ln2_gain)
    input_grad = upstream + first_back + second_back
    (
        ln1_gain_grad,
        ln1_bias_grad,
        b_query_total,
        b_keyval_total,
        bias_out_total,
        ln2_gain_grad,
        ln2_bias_grad,
        b_fc_total,
    ) = lax.psum(
        (
            jnp.sum(first_grad * first_hat, axis=0),
            jnp.sum(first_grad, axis=0),
            b_query_grad,
            b_keyval_grad,
            column_sum,
            jnp.sum(second_grad * second_hat, axis=0),
            jnp.sum(second_grad, axis=0),
            b_fc_grad,
        ),
        ("grp", "sp"),
    )
    query_share, keyval_share, out_share, fc_share, proj_share = (
        lax.psum_scatter(w_query_grad, "sp", scatter_dimension=0, tiled=True),
        lax.psum_scatter(w_keyval_grad, "sp", scatter_dimension=0, tiled=True),
        lax.psum_scatter(w_attn_out_grad, "sp", scatter_dimension=0, tiled=True),
        lax.psum_scatter(w_fc_grad, "sp", scatter_dimension=0, tiled=True),
        lax.psum_scatter(w_proj_grad, "sp", scatter_dimension=0, tiled=True),
    )
    query_total, keyval_total, out_total, fc_total, proj_total = lax.psum(
        (query_share, keyval_share, out_share, fc_share, proj_share), "grp"
    )
    return (
        layer_out,
        input_grad,
        ln1_gain_grad,
        ln1_bias_grad,
        query_total,
        b_query_total,
        keyval_total,
        b_keyval_total,
        out_total,
        bias_out_total,
        ln2_gain_grad,
        ln2_bias_grad,
        fc_total,
        b_fc_total,
        proj_total,
        bias_out_total,
    )


def solution(mesh):
    placed = (
        P(("grp", "sp"), None),
        P("grp", None),
        P(),
        P(),
        P(),
        P(),
        P(),
        P(),
        P(),
        P(),
        P(),
        P(),
        P(),
        P(),
        P(),
        P(),
        P(("grp", "sp"), None),
        P(("grp", "sp"), None),
    )
    def step(*args):
        if fits(mesh, args):
            body = functools.partial(fused_local, mesh.shape["grp"], mesh.shape["sp"])
        else:
            body = local
        return spread(body)(*args)

    def spread(body):
        return jax.shard_map(
            body,
            mesh=mesh,
            in_specs=placed,
            out_specs=(
                P(("grp", "sp"), None),
                P(("grp", "sp"), None),
                P(),
                P(),
                P("sp", None),
                P(),
                P("sp", None),
                P(),
                P("sp", None),
                P(),
                P(),
                P(),
                P("sp", None),
                P(),
                P("sp", None),
                P(),
            ),
            check_vma=False,
        )

    return step
```

```python
import functools
import math

import jax
import jax.numpy as jnp
from jax import lax
from jax.experimental import pallas as pl
from jax.experimental.pallas import tpu as pltpu
from jax.sharding import PartitionSpec as P

H = 12
HD = 64
ROT = 16
MESH = pl.DeviceIdType.MESH
F32 = jnp.float32
BF16 = jnp.bfloat16
NN = (((1,), (0,)), ((), ()))
NT = (((1,), (1,)), ((), ()))
TN = (((0,), (0,)), ((), ()))


def mm(a, b, dims=NN):
    return lax.dot_general(a, b, dims, preferred_element_type=F32)

norm_eps = 1e-05
half_root = 0.7071067811865476
inv_root_tau = 0.3989422804014327
masked_score = -1e30
rotary_base_log = math.log(10000.0)
score_block = 512


def vec_rows(width, ff, pair):
    names = ("ln1_gain", "ln1_bias", "b_query", "b_keyval", "column", "ln2_gain", "ln2_bias", "b_fc")
    sizes = (width, width, width, pair, width, width, width, ff)
    at, rows = 0, {}
    for name, size in zip(names, sizes):
        rows[name] = (at, size // 128)
        at += size // 128
    return rows, at


def fused_kernel(
    dims,
    x_h,
    order_s,
    g1_h,
    b1_h,
    wq_h,
    bq_h,
    wkv_h,
    bkv_h,
    wo_h,
    bo_h,
    g2_h,
    b2_h,
    wfc_h,
    bfc_h,
    wpr_h,
    bpr_h,
    kvg_h,
    og_h,
    o_wp,
    o_wf,
    o_wo,
    o_wq,
    o_wkv,
    o_vec,
    o_lo,
    o_ig,
    vecs,
    bkv_v,
    bfc_v,
    x2,
    og2,
    fi2,
    si2,
    fit,
    sit,
    nrm,
    inv,
    wkv_v,
    wq_v,
    wo_v,
    wfc_v,
    wpr_v,
    kvg_v,
    act_s,
    hg_s,
    mlp_all,
    sec_all,
    mlp_r,
    sec_r,
    wp_part,
    rx_wp,
    wp_s1,
    ry_wp,
    zs_wp,
    rz_wp,
    rzf,
    zf_pair,
    zf_s0,
    rx_zf,
    zf_s1,
    ry_zf,
    fin_wp,
    wf_part,
    ry_wf,
    rx_wf,
    wf_s1,
    wf_own,
    wf_in,
    zs_wf,
    rz_wf,
    fin_wf,
    kv_all,
    kvt,
    qo,
    bias,
    sbuf,
    dbuf,
    dsp,
    dkv,
    dkv_b,
    rdk,
    dks,
    rdkv,
    kvg2,
    oht,
    qgt,
    ht_r,
    qg2,
    wo_part,
    rx_wo,
    wo_s1,
    ry_wo,
    zs_wo,
    rz_wo,
    fin_wo,
    wq_part,
    ry_wq,
    wq_s1,
    rx_wq,
    zs_wq,
    rz_wq,
    fin_wq,
    vec,
    rvec,
    wkv_part,
    wkv_b,
    rkv,
    sm,
    fin_kv,
    fin_vec,
    lo_v,
    ig_v,
    ctab,
    stab,
    cost,
    sint,
    lsem,
    ssem,
    rsem,
):
    T, D, F, S, NSP, NG = dims
    NZ = NSP // 2
    D2 = D // 2
    Q = F // NSP
    QH = Q // 2
    R = D // NSP
    C2 = D // 2
    pair = 2 * HD
    g = lax.axis_index("grp")
    d = lax.axis_index("sp")
    c = lax.rem(d, 2)
    z = lax.div(d, 2)
    xx = lax.rem(g, 2)
    yy = lax.div(g, 2)
    partner = (g, d + 1 - 2 * c)
    xnb = (g + 1 - 2 * xx, d)
    ynb = (g + 2 - 4 * yy, d)

    def sp_peer(o):
        return (g, lax.rem(d + o, NSP))

    def z_peer(o):
        return (g, 2 * lax.rem(z + o, NZ) + c)

    def xy_peer(o, core):
        return (lax.rem(g + o, NG), 2 * z + core)

    def block_rows(k, core):
        return pl.ds(pl.multiple_of((2 * k + core) * T, T), T)

    mate = z + 1 - 2 * lax.rem(z, 2)
    far = 2 * (1 - lax.div(z, 2))
    outer = jnp.logical_or(z == 0, z == NZ - 1)
    to_mate = (g, 2 * mate + c)

    base = {}
    used = [0]

    def take(name, n):
        base[name] = used[0]
        used[0] += n

    for name, n in (
        ("x", 1), ("og", 1), ("kv", NZ), ("kvp", NZ), ("mlp", 1), ("sec", 1),
        ("wpx", NZ), ("wpy", NZ), ("wpz", NZ), ("wpg", NG),
        ("wpf", 5), ("zfx", 1), ("zfy", 1),
        ("wfy", 2), ("wfx", 2), ("wfs", 2), ("wfz", NZ), ("wfg", 2 * NG),
        ("ht", NZ), ("qg", H // 4), ("dk", NZ), ("dkv", NZ), ("kvg", 1),
        ("wox", NZ), ("woy", NZ), ("woz", NZ), ("wog", NG),
        ("wqy", H // 4), ("wqx", H // 4), ("wqz", NZ * (H // 4)), ("wqg", NG),
        ("wkv", NZ), ("vec", NSP), ("sm", NG), ("vg", NSP),
    ):
        take(name, n)

    def rc(name, i, src, dst, to):
        k = base[name] + i
        return pltpu.make_async_remote_copy(
            src_ref=src,
            dst_ref=dst,
            send_sem=ssem.at[k],
            recv_sem=rsem.at[k],
            device_id=to,
            device_id_type=MESH,
        )

    started = []

    def send(copy):
        copy.start()
        started.append(copy)

    lused = [0]

    def lc(src, dst):
        copy = pltpu.make_async_copy(src, dst, lsem.at[lused[0]])
        lused[0] += 1
        copy.start()
        return copy

    def chunk_of(j):
        far_y = lax.div(j, 2) == 0
        far_x = lax.rem(j, 2) == 0
        return 2 * jnp.where(far_y, 1 - yy, yy) + jnp.where(far_x, 1 - xx, xx)

    def chunk_in(j):
        far_y = lax.div(j, 2) == 0
        far_x = lax.rem(j, 2) == 0
        return 2 * jnp.where(far_y, 1 - yy, yy) + jnp.where(far_x, xx, 1 - xx)

    def chunk_y(j):
        far_y = lax.div(j, 2) == 0
        far_x = lax.rem(j, 2) == 0
        return 2 * jnp.where(far_y, yy, 1 - yy) + jnp.where(far_x, xx, 1 - xx)

    own = pl.ds(0, T)
    other = pl.ds(T, T)
    l_x = lc(x_h, x2.at[own])
    l_og = lc(og_h, og2.at[own])
    l_wkv = lc(wkv_h, wkv_v)
    l_vec = [
        lc(src, vecs.at[i]) for i, src in enumerate((g1_h, b1_h, g2_h, b2_h, bq_h, bo_h, bpr_h))
    ]
    l_bkv = lc(bkv_h, bkv_v.at[0])
    l_bfc = lc(bfc_h, bfc_v.at[0])
    l_mlp = []
    for j in range(NZ):
        q = chunk_of(j)
        cols = pl.ds(pl.multiple_of(Q * (2 * q + c), 128), Q)
        rows = pl.ds(pl.multiple_of(Q * (2 * q + c), 16), Q)
        l_mlp.append((lc(wfc_h.at[:, cols], wfc_v.at[q]), lc(wpr_h.at[rows, :], wpr_v.at[q])))
    l_wq = lc(wq_h, wq_v)
    l_wo = lc(wo_h, wo_v)
    l_kvg = lc(kvg_h, kvg_v)

    barrier = pltpu.get_barrier_semaphore()
    for o in range(1, NSP):
        pl.semaphore_signal(barrier, inc=1, device_id=sp_peer(o), device_id_type=MESH)
    for o in range(1, NG):
        for core in range(2):
            pl.semaphore_signal(barrier, inc=1, device_id=xy_peer(o, core), device_id_type=MESH)
    pl.semaphore_wait(barrier, NSP - 1 + 2 * (NG - 1))

    s_x = rc("x", 0, x_h, x2.at[other], partner)
    send(s_x)
    s_og = rc("og", 0, og_h, og2.at[other], partner)
    send(s_og)

    lane = lax.broadcasted_iota(jnp.int32, (8, T), 1)
    half = lax.broadcasted_iota(jnp.int32, (8, T), 0).astype(F32)
    block = T // 2
    first_block = order_s[0, 2 * d]
    second_block = order_s[0, 2 * d + 1]
    own_pos = jnp.where(
        lane < block, first_block * block + lane, second_block * block + (lane - block)
    )
    frequency = jnp.exp(half * (-2.0 * rotary_base_log / ROT))
    angle = own_pos.astype(F32) * 0.25 * frequency
    cosine, sine = jnp.cos(angle), jnp.sin(angle)
    cost[...] = cosine
    sint[...] = sine
    ones = jnp.ones((HD - ROT, T), F32)
    zeros = jnp.zeros((HD - ROT, T), F32)
    ctab[...] = jnp.concatenate([cosine, cosine, ones] * 2, axis=0).T
    stab[...] = jnp.concatenate([-sine, sine, zeros] * 2, axis=0).T
    lanes = lax.broadcasted_iota(jnp.int32, (128, pair), 1)
    low_half = lax.rem(lanes, HD) < ROT // 2

    def turn(tile, rows, sign):
        mixed = jnp.where(low_half, pltpu.roll(tile, pair - ROT // 2, 1), pltpu.roll(tile, ROT // 2, 1))
        return tile * ctab[rows, :] + (sign * mixed) * stab[rows, :]

    for copy in l_vec:
        copy.wait()
    l_bkv.wait()
    l_bfc.wait()
    g1, b1, g2, b2 = (vecs[i : i + 1, :] for i in range(4))
    vec[...] = jnp.zeros_like(vec)

    def norms(at, keep):
        for i in range(T // 128):
            rows = pl.ds(at + 128 * i, 128)
            v = x2[rows, :].astype(F32)
            centred = v - jnp.mean(v, axis=-1, keepdims=True)
            r = lax.rsqrt(jnp.mean(centred * centred, axis=-1, keepdims=True) + norm_eps)
            n = centred * r
            first = (n * g1 + b1).astype(BF16)
            second = (n * g2 + b2).astype(BF16)
            fi2[rows, :] = first
            si2[rows, :] = second
            fit[:, rows] = first.T
            sit[:, rows] = second.T
            if keep:
                nrm[rows, :] = n
                inv[rows, :] = jnp.broadcast_to(r, (128, 128))

    l_x.wait()
    norms(0, True)

    l_wkv.wait()
    for i in range(T // 128):
        rows = pl.ds(128 * i, 128)
        kv = mm(fi2[rows, :], wkv_v[...]) + bkv_v[...]
        kv = jnp.where(lanes < HD, turn(kv, rows, 1.0), kv)
        kv_all[pl.ds(pl.multiple_of(d * T + 128 * i, 128), 128), :] = kv.astype(BF16)
    mine = kv_all.at[block_rows(z, c)]
    s_kv = [rc("kv", o, mine, mine, z_peer(o)) for o in range(1, NZ)]
    for copy in s_kv:
        send(copy)

    def kv_pass(k):
        return rc("kvp", k, kv_all.at[block_rows(k, c)], kv_all.at[block_rows(k, c)], partner)

    s_x.wait_recv()
    norms(T, False)
    l_og.wait()
    s_og.wait_recv()

    rows_v, _ = vec_rows(D, F, pair)
    for pair_of_copies in l_mlp:
        for copy in pair_of_copies:
            copy.wait()

    def x_half(q):
        far = pl.ds(pl.multiple_of(QH // 2 * (1 - xx), 16), QH // 2)
        return rc("wpx", q, wp_part.at[q, far, :], rx_wp.at[q], xnb)

    def z_half(q, slot):
        return rc("wpf", slot, wp_part.at[q, pl.ds(QH, QH), :], rzf.at[slot], to_mate)

    def z_pair(side):
        return rc("wpf", 3 + side, zf_pair.at[side], rzf.at[3], (g, 2 * (far + side) + c))

    z_got = rc("wpf", 3 + lax.rem(z, 2), zf_pair.at[0], rzf.at[3], (g, 2 * far + c))

    def y_chunk(q):
        side = lax.rem(q, 2)
        return rc("wfy", side, wf_part.at[q, pl.ds(0, D2), :], ry_wf.at[side], ynb)

    def x_chunk(q):
        side = lax.div(q, 2)
        return rc("wfx", side, wf_part.at[q, pl.ds(D2, D2), :], rx_wf.at[side], xnb)

    def mlp_chunk(j, carry):
        q = chunk_of(j)
        at = pl.ds(pl.multiple_of(Q * (2 * q + c), 128), Q)
        shift = bfc_v[:, at]
        total = jnp.zeros((1, Q), F32)
        for i in range(2 * T // 128):
            rows = pl.ds(128 * i, 128)
            hidden = mm(si2[rows, :], wfc_v[q]) + shift
            erf_part = 1.0 + lax.erf(hidden * half_root)
            act_s[q, rows, :] = (0.5 * hidden * erf_part).astype(BF16)
            slope = 0.5 * erf_part + hidden * jnp.exp(-0.5 * hidden * hidden) * inv_root_tau
            act_grad = mm(og2[rows, :], wpr_v[q], NT)
            hidden_grad = (act_grad * slope).astype(BF16)
            hg_s[q, rows, :] = hidden_grad
            total = total + jnp.sum(hidden_grad.astype(F32), axis=0, keepdims=True)
        for i in range(Q // 128):
            cols = pl.ds(128 * i, 128)
            wp_part[q, cols, :] = mm(act_s[q, :, cols], og2[...], TN).astype(BF16)
        x_half(q).start()

        @pl.when(q == mate)
        def _():
            z_half(q, 0).start()

        @pl.when(jnp.logical_and(outer, lax.div(q, 2) != lax.div(z, 2)))
        def _():
            z_half(q, 1 + lax.rem(q, 2)).start()

        for i in range(D // 128):
            rows = pl.ds(128 * i, 128)
            wf_part[q, rows, :] = mm(sit[rows, :], hg_s[q]).astype(BF16)

        @pl.when(j < 2)
        def _():
            y_chunk(q).start()

        @pl.when(lax.rem(j, 2) == 0)
        def _():
            x_chunk(q).start()

        at_row = rows_v["b_fc"][0] + Q // 128 * (2 * q + c)
        for i in range(Q // 128):
            vec[pl.ds(at_row + i, 1), :] = total[:, 128 * i : 128 * (i + 1)]
        return carry

    lax.fori_loop(0, NZ, mlp_chunk, 0)
    for copy in s_kv:
        copy.wait_recv()
    for k in range(NZ):
        send(kv_pass(k))

    def mlp_sums(i, carry):
        at = lax.rem(i + T // 128, 2 * T // 128) * 128
        rows = pl.ds(pl.multiple_of(at, 128), 128)
        out = mm(act_s[0, rows, :], wpr_v[0])
        back = mm(hg_s[0, rows, :], wfc_v[0], NT)
        for q in range(1, NZ):
            out = out + mm(act_s[q, rows, :], wpr_v[q])
            back = back + mm(hg_s[q, rows, :], wfc_v[q], NT)
        mlp_all[rows, :] = out
        sec_all[rows, :] = back
        return carry

    lax.fori_loop(0, 2 * T // 128, mlp_sums, 0)
    s_mlp = rc("mlp", 0, mlp_all.at[other], mlp_r, partner)
    send(s_mlp)
    s_sec = rc("sec", 0, sec_all.at[other], sec_r, partner)
    send(s_sec)

    l_wq.wait()
    l_wo.wait()
    for i in range(T // 128):
        rows = pl.ds(128 * i, 128)
        query = mm(fi2[rows, :], wq_v[...]) + vecs[4:5, :]
        grads = mm(og2[rows, :], wo_v[...], NT)
        for t in range(D // pair):
            q_tile = turn(query[:, pair * t : pair * (t + 1)], rows, 1.0).astype(BF16).astype(F32) * 0.125
            o_tile = grads[:, pair * t : pair * (t + 1)]
            low = lanes < HD
            qo[2 * t, rows, :] = jnp.where(low, q_tile, 0.0).astype(BF16)
            qo[2 * t + 1, rows, :] = jnp.where(low, pltpu.roll(q_tile, HD, 1), 0.0).astype(BF16)
            late = pl.ds(T + 128 * i, 128)
            qo[2 * t, late, :] = jnp.where(low, 0.0, pltpu.roll(o_tile, HD, 1)).astype(BF16)
            qo[2 * t + 1, late, :] = jnp.where(low, 0.0, o_tile).astype(BF16)

    row_in = lax.broadcasted_iota(jnp.int32, (block, T), 0)
    query_pos = jnp.broadcast_to(own_pos[0:1, :], (block, T))
    for j in range(S // block):
        key_pos = order_s[0, j] * block + row_in
        bias[pl.ds(block * j, block), :] = jnp.where(key_pos <= query_pos, 0.0, masked_score)

    for k in range(NZ):
        kv_pass(k).wait_recv()
    for j in range(S // 256):
        rows = pl.ds(256 * j, 256)
        kvt[:, rows] = kv_all[rows, :].T
        dkv[rows, :] = jnp.zeros((256, pair), F32)

    near_x = pl.ds(pl.multiple_of(QH // 2 * xx, 16), QH // 2)
    near_y = pl.ds(pl.multiple_of(QH // 4 * yy, 16), QH // 4)
    far_y = pl.ds(pl.multiple_of(QH // 4 * (1 - yy), 16), QH // 4)

    def wp_y(q):
        return rc("wpy", q, wp_s1.at[q, far_y, :], ry_wp.at[q], ynb)

    def wp_first(j):
        q = chunk_in(j)
        x_half(q).wait_recv()
        wp_s1[q] = (wp_part[q, near_x, :].astype(F32) + rx_wp[q].astype(F32)).astype(BF16)
        wp_y(q).start()

    def wp_z(o):
        return rc("wpz", o, zs_wp.at[lax.rem(z + o, NZ)], rz_wp.at[o], z_peer(o))

    def start_wp_z(o):
        wp_z(o).start()

    def wp_second(j):
        q = chunk_y(j)
        wp_y(q).wait_recv()
        zs_wp[q] = (wp_s1[q, near_y, :].astype(F32) + ry_wp[q].astype(F32)).astype(BF16)
        for o in range(1, NZ):
            pl.when(lax.rem(z + o, NZ) == q)(functools.partial(start_wp_z, o))

    slot_wp = 2 * xx + yy

    def wp_g(o):
        return rc("wpg", o, fin_wp, o_wp.at[slot_wp], xy_peer(o, c))

    l_fin = []

    far_zx = pl.ds(pl.multiple_of(QH // 2 * (1 - xx), 16), QH // 2)
    zf_x = rc("zfx", 0, zf_s0.at[far_zx, :], rx_zf, xnb)
    zf_y = rc("zfy", 0, zf_s1.at[far_y, :], ry_zf, ynb)

    def zf_mid():
        @pl.when(jnp.logical_not(outer))
        def _():
            for side in range(2):
                z_half(far + side, 1 + side).wait_recv()
                total = wp_part[far + side, QH:, :].astype(F32) + rzf[1 + side].astype(F32)
                zf_pair[side] = total.astype(BF16)
                z_pair(side).start()

    def zf_first():
        total = wp_part[z, QH:, :].astype(F32)
        z_half(mate, 0).wait_recv()
        z_got.wait_recv()
        total = total + rzf[0].astype(F32) + rzf[3].astype(F32)
        zf_s0[...] = total.astype(BF16)
        zf_x.start()

    def zf_second():
        zf_x.wait_recv()
        zf_s1[...] = (zf_s0[near_x, :].astype(F32) + rx_zf[...].astype(F32)).astype(BF16)
        zf_y.start()

    def zf_third():
        zf_y.wait_recv()
        fin_wp[1] = (zf_s1[near_y, :].astype(F32) + ry_zf[...].astype(F32)).astype(BF16)

    def wp_third():
        total = zs_wp[z].astype(F32)
        for o in range(1, NZ):
            wp_z(o).wait_recv()
            total = total + rz_wp[o].astype(F32)
        fin_wp[0] = total.astype(BF16)
        for o in range(1, NG):
            wp_g(o).start()
        l_fin.append(lc(fin_wp, o_wp.at[slot_wp]))

    def wf_second_send(part):
        return rc("wfs", part, wf_s1.at[part], wf_in.at[part], ynb if part else xnb)

    def wf_first(part):
        if part:
            q = 2 * (1 - yy) + xx
            x_chunk(2 * (1 - yy) + 1 - xx).wait_recv()
            got = rx_wf[1 - yy]
        else:
            q = 2 * yy + 1 - xx
            y_chunk(2 * (1 - yy) + 1 - xx).wait_recv()
            got = ry_wf[1 - xx]
        wf_s1[part] = (wf_part[q, D2 * part : D2 * (part + 1), :].astype(F32) + got.astype(F32)).astype(BF16)
        wf_second_send(part).start()

    def wf_second(part):
        q = 2 * yy + xx
        if part:
            x_chunk(2 * yy + 1 - xx).wait_recv()
            got = rx_wf[yy]
        else:
            y_chunk(2 * (1 - yy) + xx).wait_recv()
            got = ry_wf[xx]
        wf_own[part] = (wf_part[q, D2 * part : D2 * (part + 1), :].astype(F32) + got.astype(F32)).astype(BF16)

    def wf_z(o):
        rows = pl.ds(pl.multiple_of(2 * R * lax.rem(z + o, NZ), 16), 2 * R)
        return rc("wfz", o, zs_wf.at[rows, :], rz_wf.at[o], z_peer(o))

    def start_wf_z(o):
        wf_z(o).start()

    def wf_third(part):
        wf_second_send(part).wait_recv()
        zs_wf[D2 * part : D2 * (part + 1), :] = (
            wf_own[part].astype(F32) + wf_in[part].astype(F32)
        ).astype(BF16)
        for o in range(1, NZ):
            pl.when(lax.div(lax.rem(z + o, NZ), NZ // 2) == part)(functools.partial(start_wf_z, o))

    slot_wf = 2 * yy + xx

    def wf_g(o, core):
        to = c + core - 2 * c * core
        rows = pl.ds(pl.multiple_of(R * to, 16), R)
        return rc("wfg", 2 * o + core, fin_wf.at[rows, :], o_wf.at[slot_wf, c], xy_peer(o, to))

    def wf_fourth():
        total = zs_wf[pl.ds(pl.multiple_of(2 * R * z, 16), 2 * R), :].astype(F32)
        for o in range(1, NZ):
            wf_z(o).wait_recv()
            total = total + rz_wf[o].astype(F32)
        fin_wf[...] = total.astype(BF16)
        for o in range(NG):
            for core in range(2):
                if o or core:
                    wf_g(o, core).start()
        l_fin.append(lc(fin_wf.at[pl.ds(pl.multiple_of(R * c, 16), R), :], o_wf.at[slot_wf, c]))

    far_rx = pl.ds(pl.multiple_of(R // 2 * (1 - xx), 16), R // 2)
    far_ry = pl.ds(pl.multiple_of(R // 2 * (1 - yy), 16), R // 2)
    near_rx = pl.ds(pl.multiple_of(R // 2 * xx, 16), R // 2)
    near_ry = pl.ds(pl.multiple_of(R // 2 * yy, 16), R // 2)
    far_cy = pl.ds(pl.multiple_of(C2 * (1 - yy), 128), C2)
    near_cy = pl.ds(pl.multiple_of(C2 * yy, 128), C2)
    GC = 4 * HD

    def owner_rows(k, core):
        return pl.ds(pl.multiple_of(2 * R * k + R * core, 16), R)

    def group_cols(m):
        return pl.ds(GC * m, GC)

    def side_cols(m, side):
        return pl.ds(pl.multiple_of(GC * m + GC // 2 * side, 128), GC // 2)

    def r_ht(k):
        return rc("ht", k, oht.at[owner_rows(k, 1 - c), :], ht_r.at[k], partner)

    def r_wox(k):
        return rc("wox", k, wo_part.at[k, far_rx, :], rx_wo.at[k], xnb)

    def r_woy(k):
        return rc("woy", k, wo_s1.at[k, :, far_cy], ry_wo.at[k], ynb)

    def r_woz(o):
        return rc("woz", o, zs_wo.at[lax.rem(z + o, NZ)], rz_wo.at[o], z_peer(o))

    def r_qg(m):
        return rc("qg", m, qg2.at[own, group_cols(m)], qg2.at[other, group_cols(m)], partner)

    def r_wqy(m):
        return rc("wqy", m, wq_part.at[:, far_ry, group_cols(m)], ry_wq.at[:, :, group_cols(m)], ynb)

    def r_wqx(m):
        return rc("wqx", m, wq_s1.at[:, :, side_cols(m, 1 - xx)], rx_wq.at[m], xnb)

    def r_wqz(o, m):
        cols = pl.ds(GC // 2 * m, GC // 2)
        return rc(
            "wqz", NZ * m + o, zs_wq.at[lax.rem(z + o, NZ), :, cols], rz_wq.at[o, :, cols], z_peer(o)
        )

    def ht_send(k):
        r_ht(k).start()

    def wo_a(k):
        r_ht(k).wait_recv()
        total = mm(oht[owner_rows(k, c), :], og2[own, :]) + mm(ht_r[k], og2[other, :])
        wo_part[k] = total.astype(BF16)
        r_wox(k).start()

    def wo_b(k):
        r_wox(k).wait_recv()
        wo_s1[k] = (wo_part[k, near_rx, :].astype(F32) + rx_wo[k].astype(F32)).astype(BF16)
        r_woy(k).start()

    def start_woz(o):
        r_woz(o).start()

    def wo_c(k):
        r_woy(k).wait_recv()
        zs_wo[k] = (wo_s1[k, :, near_cy].astype(F32) + ry_wo[k].astype(F32)).astype(BF16)
        for o in range(1, NZ):
            pl.when(lax.rem(z + o, NZ) == k)(functools.partial(start_woz, o))

    def qg_send(m):
        qg2[own, group_cols(m)] = qgt[group_cols(m), :].T
        r_qg(m).start()

    def wq_a(m):
        r_qg(m).wait_recv()
        for k in range(NZ):
            wq_part[k, :, group_cols(m)] = mm(fit[owner_rows(k, c), :], qg2[:, group_cols(m)]).astype(BF16)
        r_wqy(m).start()

    def wq_b(m):
        r_wqy(m).wait_recv()
        cols = group_cols(m)
        wq_s1[:, :, cols] = (wq_part[:, near_ry, cols].astype(F32) + ry_wq[:, :, cols].astype(F32)).astype(BF16)
        r_wqx(m).start()

    def wq_c(m):
        r_wqx(m).wait_recv()
        mine_cols = side_cols(m, xx)
        zs_wq[:, :, GC // 2 * m : GC // 2 * (m + 1)] = (
            wq_s1[:, :, mine_cols].astype(F32) + rx_wq[m].astype(F32)
        ).astype(BF16)
        for o in range(1, NZ):
            r_wqz(o, m).start()

    def at_head(h):
        for when, what in EVENTS:
            pl.when(h == when)(functools.partial(run_event, what))

    def run_event(what):
        {
            "wp0": lambda: wp_first(0),
            "wp1": lambda: wp_first(1),
            "wp2": lambda: wp_first(2),
            "wp3": lambda: wp_first(3),
            "wpy0": lambda: wp_second(0),
            "wpy1": lambda: wp_second(1),
            "wpy2": lambda: wp_second(2),
            "wpy3": lambda: wp_second(3),
            "zf_mid": zf_mid,
            "ht0": lambda: ht_send(0),
            "ht1": lambda: ht_send(1),
            "ht2": lambda: ht_send(2),
            "woa0": lambda: wo_a(0),
            "woa1": lambda: wo_a(1),
            "woa2": lambda: wo_a(2),
            "wob0": lambda: wo_b(0),
            "wob1": lambda: wo_b(1),
            "woc0": lambda: wo_c(0),
            "qg0": lambda: qg_send(0),
            "qg1": lambda: qg_send(1),
            "wqa0": lambda: wq_a(0),
            "wqa1": lambda: wq_a(1),
            "wqb0": lambda: wq_b(0),
            "wqc0": lambda: wq_c(0),
            "zf_first": zf_first,
            "zf_second": zf_second,
            "zf_third": zf_third,
            "wf_first0": lambda: wf_first(0),
            "wf_second0": lambda: wf_second(0),
            "wf_third0": lambda: wf_third(0),
            "wf_first1": lambda: wf_first(1),
            "wf_second1": lambda: wf_second(1),
            "wf_third1": lambda: wf_third(1),
        }[what]()

    KC = 256

    def head(h, carry):
        at_head(h)
        both = qo[h]
        top = jnp.full((8, T), -3e38, F32)
        for k in range(S // KC):
            rows = pl.ds(KC * k, KC)
            sd = mm(kv_all[rows, :], both, NT)
            score = sd[:, :T] + bias[rows, :]
            sbuf[rows, :] = score
            dbuf[rows, :] = sd[:, T:]
            top = jnp.maximum(top, jnp.max(score.reshape(KC // 8, 8, T), axis=0))
        top = jnp.max(top, axis=0, keepdims=True)
        norm = jnp.zeros((8, T), F32)
        delta = jnp.zeros((8, T), F32)
        for k in range(S // KC):
            rows = pl.ds(KC * k, KC)
            e = jnp.exp(sbuf[rows, :] - top)
            sbuf[rows, :] = e
            norm = norm + jnp.sum(e.reshape(KC // 8, 8, T), axis=0)
            delta = delta + jnp.sum((e * dbuf[rows, :]).reshape(KC // 8, 8, T), axis=0)
        scale = 1.0 / jnp.sum(norm, axis=0, keepdims=True)
        delta = jnp.sum(delta, axis=0, keepdims=True) * scale
        for k in range(S // KC):
            rows = pl.ds(KC * k, KC)
            p = sbuf[rows, :] * scale
            dsp[rows, :T] = (p * (dbuf[rows, :] - delta)).astype(BF16)
            dsp[rows, T:] = p.astype(BF16)
        for k in range(S // KC):
            rows = pl.ds(KC * k, KC)
            dkv[rows, :] += mm(dsp[rows, :], both)
        result = mm(kvt[...], dsp[...])
        rows = pl.ds(pl.multiple_of(HD * h, HD), HD)
        oht[rows, :] = result[HD:, T:].astype(BF16)
        back = result[:HD, :T] * 0.125
        a, b, rest = back[: ROT // 2], back[ROT // 2 : ROT], back[ROT:]
        ct, st = cost[...], sint[...]
        qgt[rows, :] = jnp.concatenate([a * ct + b * st, b * ct - a * st, rest], axis=0).astype(BF16)
        return carry

    lax.fori_loop(0, H, head, 0)

    dkv_b[...] = dkv[...].astype(BF16)
    s_dk = []
    for k in range(NZ):
        s_dk.append(rc("dk", k, dkv_b.at[block_rows(k, 1 - c), :], rdk.at[k], partner))
        send(s_dk[-1])

    ht_send(3)
    qg_send(2)

    for copy in s_dk:
        copy.wait_recv()
    s_dkv = []
    for o in range(1, NZ):
        k = lax.rem(z + o, NZ)
        dks[o] = (dkv[block_rows(k, c), :] + rdk[k].astype(F32)).astype(BF16)
        s_dkv.append(rc("dkv", o, dks.at[o], rdkv.at[o], z_peer(o)))
        send(s_dkv[-1])

    def put(name, row):
        at, count = rows_v[name]
        for i in range(count):
            vec[at + i : at + i + 1, :] = row[:, 128 * i : 128 * (i + 1)]

    wo_a(3)
    wq_a(2)
    wq_b(1)
    wo_b(2)
    wo_c(1)

    s_mlp.wait_recv()
    for i in range(T // 128):
        rows = pl.ds(128 * i, 128)
        branch = mm(oht[:, rows], wo_v[...], TN) + vecs[5:6, :]
        mlp = (mlp_all[rows, :] + mlp_r[rows, :]) + vecs[6:7, :]
        lo_v[rows, :] = ((x2[rows, :].astype(F32) + branch) + mlp).astype(BF16)
    l_lo = lc(lo_v, o_lo)

    zf_second()
    wo_b(3)
    wq_b(2)
    wf_fourth()
    zf_third()
    wp_third()

    s_sec.wait_recv()
    sums = [jnp.zeros((1, D), F32) for _ in range(6)]
    for i in range(T // 128):
        rows = pl.ds(128 * i, 128)
        ig_v[rows, :] = mm(qg2[rows, :], wq_v[...], NT)
        second_grad = sec_all[rows, :] + sec_r[rows, :]
        sec_all[rows, :] = second_grad * g2
        up = og2[rows, :].astype(F32)
        for k, value in enumerate((qg2[rows, :].astype(F32), up, second_grad * nrm[rows, :], second_grad)):
            sums[2 + k] = sums[2 + k] + jnp.sum(value, axis=0, keepdims=True)

    wq_c(1)
    wo_c(2)

    l_kvg.wait()
    for copy in s_dkv:
        copy.wait_recv()
    kv_grads = []
    for i in range(T // 128):
        rows = pl.ds(128 * i, 128)
        total = dkv[pl.ds(pl.multiple_of(d * T + 128 * i, 128), 128), :] + rdk[z, rows, :].astype(F32)
        for o in range(1, NZ):
            total = total + rdkv[o, rows, :].astype(F32)
        total = total + kvg_v[rows, :].astype(F32)
        kv_grads.append(jnp.where(lanes < HD, turn(total, rows, -1.0), total).astype(BF16))
        kvg2[rows, :] = kv_grads[-1]
    s_kvg = rc("kvg", 0, kvg2.at[own], kvg2.at[other], partner)
    send(s_kvg)
    put("b_keyval", jnp.sum(jnp.concatenate(kv_grads, axis=0).astype(F32), axis=0, keepdims=True))

    for i in range(T // 128):
        rows = pl.ds(128 * i, 128)
        first_grad = ig_v[rows, :] + mm(kv_grads[i], wkv_v[...], NT)
        n = nrm[rows, :]
        u = first_grad * g1 + sec_all[rows, :]
        back = u - jnp.mean(u, axis=-1, keepdims=True) - n * jnp.mean(u * n, axis=-1, keepdims=True)
        ig_v[rows, :] = og2[rows, :].astype(F32) + inv[rows, 0:1] * back
        for k, value in enumerate((first_grad * n, first_grad)):
            sums[k] = sums[k] + jnp.sum(value, axis=0, keepdims=True)
    l_ig = lc(ig_v, o_ig)
    for name, row in zip(("ln1_gain", "ln1_bias", "b_query", "column", "ln2_gain", "ln2_bias"), sums):
        put(name, row)
    s_vec = []
    for o in range(1, NSP):
        rows = pl.ds(pl.multiple_of(lax.rem(d + o, NSP) * 8, 8), 8)
        s_vec.append(rc("vec", o, vec.at[rows, :], rvec.at[o], sp_peer(o)))
        send(s_vec[-1])

    s_kvg.wait_recv()
    s_wkv = []
    for k in range(NZ):
        rows = pl.ds(pl.multiple_of(2 * R * k + R * c, 16), R)
        wkv_part[k] = mm(fit[rows, :], kvg2[...])
        wkv_b[k] = wkv_part[k].astype(BF16)
    for o in range(1, NZ):
        s_wkv.append(rc("wkv", o, wkv_b.at[lax.rem(z + o, NZ)], rkv.at[o], z_peer(o)))
        send(s_wkv[-1])

    wo_c(3)
    wq_c(2)

    for copy in s_wkv:
        copy.wait_recv()
    total = wkv_part[z]
    for o in range(1, NZ):
        total = total + rkv[o].astype(F32)
    sm[g, :R, :] = total
    for copy in s_vec:
        copy.wait_recv()
    total = vec[pl.ds(pl.multiple_of(d * 8, 8), 8), :]
    for o in range(1, NSP):
        total = total + rvec[o]
    sm[g, R:, :] = total
    s_sm = [rc("sm", o, sm.at[g], sm.at[g], xy_peer(o, c)) for o in range(1, NG)]
    for copy in s_sm:
        send(copy)

    total = zs_wo[z].astype(F32)
    for o in range(1, NZ):
        r_woz(o).wait_recv()
        total = total + rz_wo[o].astype(F32)
    fin_wo[...] = total.astype(BF16)
    s_wog = [rc("wog", o, fin_wo, o_wo.at[xx, yy], xy_peer(o, c)) for o in range(1, NG)]
    for copy in s_wog:
        send(copy)
    l_fo = lc(fin_wo, o_wo.at[xx, yy])
    total = zs_wq[z].astype(F32)
    for o in range(1, NZ):
        for m in range(H // 4):
            r_wqz(o, m).wait_recv()
        total = total + rz_wq[o].astype(F32)
    fin_wq[...] = total.astype(BF16)
    s_wqg = [rc("wqg", o, fin_wq, o_wq.at[yy, xx], xy_peer(o, c)) for o in range(1, NG)]
    for copy in s_wqg:
        send(copy)
    l_fq = lc(fin_wq, o_wq.at[yy, xx])

    for copy in s_sm:
        copy.wait_recv()
    total = sm[0]
    for k in range(1, NG):
        total = total + sm[k]
    fin_kv[...] = total[:R]
    fin_vec[...] = total[R:]
    l_kv = lc(fin_kv, o_wkv)
    mine8 = pl.ds(pl.multiple_of(d * 8, 8), 8)
    s_vg = [rc("vg", o, fin_vec, o_vec.at[mine8, :], sp_peer(o)) for o in range(1, NSP)]
    for copy in s_vg:
        send(copy)
    l_vg = lc(fin_vec, o_vec.at[mine8, :])

    for o in range(1, NG):
        wp_g(o).wait_recv()
    for o in range(NG):
        for core in range(2):
            if o or core:
                wf_g(o, core).wait_recv()
    for copy in s_wog + s_wqg + s_vg:
        copy.wait_recv()
    for copy in started:
        copy.wait_send()
    for q in range(NZ):
        x_half(q).wait_send()
        wp_y(q).wait_send()
    for k in range(2):
        y_chunk(2 * (1 - yy) + k).wait_send()
        x_chunk(2 * k + 1 - xx).wait_send()
        wf_second_send(k).wait_send()
    for k in range(NZ):
        r_ht(k).wait_send()
        r_wox(k).wait_send()
        r_woy(k).wait_send()
    for m in range(H // 4):
        r_qg(m).wait_send()
        r_wqy(m).wait_send()
        r_wqx(m).wait_send()
    for o in range(1, NZ):
        r_woz(o).wait_send()
        for m in range(H // 4):
            r_wqz(o, m).wait_send()
    z_half(mate, 0).wait_send()

    @pl.when(outer)
    def _():
        for side in range(2):
            z_half(far + side, 1 + side).wait_send()

    @pl.when(jnp.logical_not(outer))
    def _():
        for side in range(2):
            z_pair(side).wait_send()

    zf_x.wait_send()
    zf_y.wait_send()
    for o in range(1, NZ):
        wp_z(o).wait_send()
        wf_z(o).wait_send()
    for o in range(1, NG):
        wp_g(o).wait_send()
    for o in range(NG):
        for core in range(2):
            if o or core:
                wf_g(o, core).wait_send()
    for copy in l_fin + [l_lo, l_ig, l_kv, l_vg, l_fo, l_fq]:
        copy.wait()


EVENTS = (
    (0, "wp0"),
    (1, "wf_first0"),
    (2, "wf_first1"),
    (2, "wp1"),
    (3, "zf_mid"),
    (3, "wf_second0"),
    (4, "wp2"),
    (4, "ht0"),
    (5, "wpy0"),
    (5, "woa0"),
    (5, "qg0"),
    (6, "wf_second1"),
    (6, "wp3"),
    (6, "wqa0"),
    (7, "wpy1"),
    (7, "wpy2"),
    (7, "wf_third1"),
    (7, "ht1"),
    (8, "wpy3"),
    (8, "woa1"),
    (8, "qg1"),
    (9, "wf_third0"),
    (9, "wqa1"),
    (9, "wob0"),
    (9, "wqb0"),
    (9, "ht2"),
    (10, "woa2"),
    (10, "zf_first"),
    (11, "woc0"),
    (11, "wqc0"),
    (11, "wob1"),
)


def finish_kernel(
    dims, wp_h, wf_h, wo_h, wq_h, wkv_h, vec_h, lo_h, ig_h,
    layer_out, input_grad, ln1_gain, ln1_bias, w_query, b_query, w_keyval, b_keyval,
    w_attn_out, b_attn_out, ln2_gain, ln2_bias, w_fc, b_fc, w_proj, b_proj,
    wp, wf, wo, wq, wkv, vec, lo, ig, fc_v, proj_v, out_v, query_v, isem, osem,
):
    T, D, F, S, NSP, NG = dims
    Q, R, C2 = F // NSP, D // NSP, D // 2
    arrive = {}
    for i, (name, src, dst) in enumerate(
        (("wf", wf_h, wf), ("wp", wp_h, wp), ("ig", ig_h, ig), ("lo", lo_h, lo), ("vec", vec_h, vec),
         ("wo", wo_h, wo), ("wq", wq_h, wq), ("wkv", wkv_h, wkv))
    ):
        arrive[name] = pltpu.make_async_copy(src, dst, isem.at[i])
        arrive[name].start()
    leave = []

    def put_out(src, dst):
        leave.append(pltpu.make_async_copy(src, dst, osem.at[len(leave)]))
        leave[-1].start()

    arrive["wf"].wait()
    for k in range(NG):
        for core in range(2):
            at = Q * (2 * k + core)
            fc_v[:, at : at + Q] = wf[k, core].astype(F32)
    put_out(fc_v, w_fc)
    arrive["wp"].wait()
    rows = Q // 2 // NG
    for k in range(NG):
        for part in range(2):
            at = Q // 2 * part + rows * k
            proj_v[at : at + rows, :] = wp[k, part].astype(F32)
    put_out(proj_v, w_proj)
    arrive["ig"].wait()
    put_out(ig, input_grad)
    arrive["lo"].wait()
    put_out(lo, layer_out)
    arrive["wo"].wait()
    arrive["wq"].wait()
    for a in range(2):
        for b in range(2):
            rows = slice(R // 2 * a, R // 2 * (a + 1))
            cols = slice(C2 * b, C2 * (b + 1))
            out_v[rows, cols] = wo[a, b].astype(F32)
            for m in range(H // 4):
                at = 4 * HD * m + 2 * HD * b
                query_v[rows, at : at + 2 * HD] = wq[a, b, :, 2 * HD * m : 2 * HD * (m + 1)].astype(F32)
    put_out(out_v, w_attn_out)
    put_out(query_v, w_query)
    arrive["wkv"].wait()
    put_out(wkv, w_keyval)
    arrive["vec"].wait()
    rows_v, _ = vec_rows(D, F, 2 * HD)
    for name, out in (
        ("ln1_gain", ln1_gain), ("ln1_bias", ln1_bias), ("b_query", b_query), ("b_keyval", b_keyval),
        ("column", b_attn_out), ("column", b_proj), ("ln2_gain", ln2_gain), ("ln2_bias", ln2_bias),
        ("b_fc", b_fc),
    ):
        at, count = rows_v[name]
        out[...] = jnp.concatenate([vec[at + i : at + i + 1, :] for i in range(count)], axis=1).reshape(
            128 * count
        )
    for copy in leave:
        copy.wait()


def fused_local(n_grp, n_sp, *args):
    layer_input, block_order = args[0], args[1]
    T, D = layer_input.shape
    F = args[12].shape[1]
    S = T * n_sp
    NZ, NG, NSP = n_sp // 2, n_grp, n_sp
    Q, R, C2, pair = F // n_sp, D // n_sp, D // 2, 2 * HD
    dims = (T, D, F, S, NSP, NG)
    V = pltpu.VMEM
    scratch = [
        V((8, D), F32), V((1, pair), F32), V((1, F), F32),
        V((2 * T, D), BF16), V((2 * T, D), BF16), V((2 * T, D), BF16), V((2 * T, D), BF16),
        V((D, 2 * T), BF16), V((D, 2 * T), BF16), V((T, D), F32), V((T, 128), F32),
        V((D, pair), BF16), V((D, D), BF16), V((D, D), BF16), V((NZ, D, Q), BF16), V((NZ, Q, D), BF16),
        V((T, pair), BF16), V((NZ, 2 * T, Q), BF16), V((NZ, 2 * T, Q), BF16),
        V((2 * T, D), F32), V((2 * T, D), F32), V((T, D), F32), V((T, D), F32),
        V((NZ, Q, D), BF16), V((NZ, Q // 4, D), BF16), V((NZ, Q // 4, D), BF16), V((NZ, Q // 8, D), BF16),
        V((NZ, Q // 8, D), BF16), V((NZ, Q // 8, D), BF16), V((NZ, Q // 2, D), BF16), V((2, Q // 2, D), BF16),
        V((Q // 2, D), BF16),
        V((Q // 4, D), BF16), V((Q // 4, D), BF16), V((Q // 8, D), BF16), V((2, Q // 8, D), BF16),
        V((NZ, D, Q), BF16), V((2, D // 2, Q), BF16), V((2, D // 2, Q), BF16), V((2, D // 2, Q), BF16),
        V((2, D // 2, Q), BF16), V((2, D // 2, Q), BF16), V((D, Q), BF16), V((NZ, 2 * R, Q), BF16), V((2 * R, Q), BF16),
        V((S, pair), BF16), V((pair, S), BF16), V((H, 2 * T, pair), BF16), V((S, T), F32), V((S, T), F32),
        V((S, T), F32), V((S, 2 * T), BF16), V((S, pair), F32), V((S, pair), BF16), V((NZ, T, pair), BF16),
        V((NZ, T, pair), BF16), V((NZ, T, pair), BF16), V((2 * T, pair), BF16),
        V((D, T), BF16), V((D, T), BF16), V((NZ, R, T), BF16), V((2 * T, D), BF16),
        V((NZ, R, D), BF16), V((NZ, R // 2, D), BF16), V((NZ, R // 2, D), BF16), V((NZ, R // 2, C2), BF16),
        V((NZ, R // 2, C2), BF16), V((NZ, R // 2, C2), BF16), V((R // 2, C2), BF16),
        V((NZ, R, D), BF16), V((NZ, R // 2, D), BF16), V((NZ, R // 2, D), BF16),
        V((H // 4, NZ, R // 2, 2 * HD), BF16),
        V((NZ, R // 2, C2), BF16), V((NZ, R // 2, C2), BF16), V((R // 2, C2), BF16),
        V((8 * NSP, 128), F32), V((NSP, 8, 128), F32), V((NZ, R, pair), F32), V((NZ, R, pair), BF16),
        V((NZ, R, pair), BF16), V((NG, R + 8, 128), F32), V((R, 128), F32), V((8, 128), F32),
        V((T, D), BF16), V((T, D), F32), V((T, pair), F32), V((T, pair), F32), V((8, T), F32), V((8, T), F32),
        pltpu.SemaphoreType.DMA((40,)), pltpu.SemaphoreType.DMA((160,)), pltpu.SemaphoreType.DMA((160,)),
    ]
    any_spec = pl.BlockSpec(memory_space=pl.ANY)
    shape = jax.ShapeDtypeStruct
    held = pl.pallas_call(
        functools.partial(fused_kernel, dims),
        out_shape=(
            shape((NG, 2, Q // 8, D), BF16),
            shape((NG, 2, R, Q), BF16),
            shape((2, 2, R // 2, C2), BF16),
            shape((2, 2, R // 2, C2), BF16),
            shape((R, pair), F32),
            shape((8 * NSP, 128), F32),
            shape((T, D), BF16),
            shape((T, D), F32),
        ),
        in_specs=[any_spec, pl.BlockSpec(memory_space=pltpu.SMEM)] + [any_spec] * 16,
        out_specs=(any_spec,) * 8,
        scratch_shapes=scratch,
        compiler_params=pltpu.CompilerParams(
            collective_id=0, has_side_effects=True, vmem_limit_bytes=67043328
        ),
        name="fused_layer",
    )(*args)
    vmem_spec = pl.BlockSpec(memory_space=pltpu.VMEM)
    row = shape((D,), F32)
    return pl.pallas_call(
        functools.partial(finish_kernel, dims),
        out_shape=(
            shape((T, D), BF16), shape((T, D), F32), row, row, shape((R, D), F32), row, shape((R, pair), F32),
            shape((pair,), F32), shape((R, D), F32), row, row, row, shape((R, F), F32), shape((F,), F32),
            shape((Q, D), F32), row,
        ),
        in_specs=[any_spec] * 8,
        out_specs=tuple(any_spec if k in (0, 1, 4, 6, 8, 12, 14) else vmem_spec for k in range(16)),
        scratch_shapes=[
            V((NG, 2, Q // 8, D), BF16), V((NG, 2, R, Q), BF16), V((2, 2, R // 2, C2), BF16),
            V((2, 2, R // 2, C2), BF16), V((R, pair), F32), V((8 * NSP, 128), F32), V((T, D), BF16), V((T, D), F32),
            V((R, F), F32), V((Q, D), F32), V((R, D), F32), V((R, D), F32),
            pltpu.SemaphoreType.DMA((8,)), pltpu.SemaphoreType.DMA((8,)),
        ],
        compiler_params=pltpu.CompilerParams(vmem_limit_bytes=64000000),
        name="finish",
    )(*held)


def fits(mesh, args):
    n_grp, n_sp = mesh.shape["grp"], mesh.shape["sp"]
    tokens, width = args[0].shape
    seqs, blocks = args[1].shape
    ff = args[12].shape[1]
    rows = tokens // (n_grp * n_sp)
    return (
        n_grp == 4
        and n_sp == 2 * n_grp
        and seqs == n_grp
        and blocks == 2 * n_sp
        and rows == 2 * 128
        and width == H * HD
        and width % (32 * n_sp) == 0
        and ff % (128 * n_sp) == 0
        and width % 128 == 0
        and sum(count for _, count in vec_rows(width, ff, 2 * HD)[0].values()) <= 8 * n_sp
    )


def layer_norm(values, gain_row, shift_row):
    centre = jnp.mean(values, axis=-1, keepdims=True)
    centred = values - centre
    spread = jnp.mean(centred * centred, axis=-1, keepdims=True)
    inverse_dev = lax.rsqrt(spread + norm_eps)
    normed = centred * inverse_dev
    return (normed * gain_row + shift_row, normed, inverse_dev)


def norm_back(upstream, normed, inverse_dev, gain_row):
    scaled = upstream * gain_row
    return inverse_dev * (
        scaled
        - jnp.mean(scaled, axis=-1, keepdims=True)
        - normed * jnp.mean(scaled * normed, axis=-1, keepdims=True)
    )


def rotary_tables(position):
    half_rot = ROT // 2
    frequency = jnp.exp(jnp.arange(half_rot, dtype=jnp.float32) * (-2.0 * rotary_base_log / ROT))
    angles = position.astype(jnp.float32)[:, None] * 0.25 * frequency[None, :]
    return (jnp.cos(angles), jnp.sin(angles))


def rotate(values, cosine, sine_table):
    half_rot = ROT // 2
    cos_rows = cosine[:, None, :]
    sin_rows = sine_table[:, None, :]
    lower_half = values[..., :half_rot]
    upper_half = values[..., half_rot:ROT]
    return jnp.concatenate(
        [
            lower_half * cos_rows - upper_half * sin_rows,
            upper_half * cos_rows + lower_half * sin_rows,
            values[..., ROT:],
        ],
        axis=-1,
    )


def rotate_back(values, cosine, sine_table):
    half_rot = ROT // 2
    cos_rows = cosine[:, None, :]
    sin_rows = sine_table[:, None, :]
    lower_half = values[..., :half_rot]
    upper_half = values[..., half_rot:ROT]
    return jnp.concatenate(
        [
            lower_half * cos_rows + upper_half * sin_rows,
            upper_half * cos_rows - lower_half * sin_rows,
            values[..., ROT:],
        ],
        axis=-1,
    )


def key_scores(query_rows, row_pos, kv_sequence, block_index, block_rows):
    key_start = block_index * block_rows
    key_slice = lax.dynamic_slice_in_dim(kv_sequence, key_start, block_rows, 0)
    raw_scores = (
        jnp.einsum("rd,kd->rk", query_rows, key_slice[:, :HD], preferred_element_type=jnp.float32)
        * 0.125
    )
    key_pos = key_start + lax.broadcasted_iota(jnp.int32, (1, block_rows), 1)
    return (jnp.where(key_pos <= row_pos[:, None], raw_scores, masked_score), key_slice)


def attention_forward(query_tiles, tile_pos, kv_sorted):
    pair_count = query_tiles.shape[0]
    pairs_per_seq = pair_count // kv_sorted.shape[0]
    block_rows = min(score_block, kv_sorted.shape[1])

    def one_pair(inputs):
        query_rows, row_pos, pair_index = inputs
        kv_sequence = kv_sorted[pair_index // pairs_per_seq]
        key_blocks = jnp.max(row_pos) // block_rows + 1
        row_count = query_rows.shape[0]

        def max_pass(block_index, carried):
            running_max, running_sum = carried
            masked, key_slice = key_scores(
                query_rows, row_pos, kv_sequence, block_index, block_rows
            )
            new_max = jnp.maximum(running_max, jnp.max(masked, axis=1, keepdims=True))
            running_sum = running_sum * jnp.exp(running_max - new_max) + jnp.sum(
                jnp.exp(masked - new_max), axis=1, keepdims=True
            )
            return (new_max, running_sum)

        start_max = jnp.full((row_count, 1), masked_score, jnp.float32)
        running_max, running_sum = lax.fori_loop(
            0, key_blocks, max_pass, (start_max, jnp.zeros((row_count, 1), jnp.float32))
        )
        log_total = running_max + jnp.log(running_sum)

        def value_pass(block_index, output):
            masked, key_slice = key_scores(
                query_rows, row_pos, kv_sequence, block_index, block_rows
            )
            weights = jnp.exp(masked - log_total).astype(jnp.bfloat16)
            return output + jnp.dot(weights, key_slice[:, HD:], preferred_element_type=jnp.float32)

        output = lax.fori_loop(0, key_blocks, value_pass, jnp.zeros((row_count, HD), jnp.float32))
        return (output, log_total)

    return lax.map(one_pair, (query_tiles, tile_pos, jnp.arange(pair_count, dtype=jnp.int32)))


def attention_backward(query_tiles, tile_pos, grad_tiles, log_totals, kv_sorted):
    pair_count = query_tiles.shape[0]
    pairs_per_seq = pair_count // kv_sorted.shape[0]
    block_rows = min(score_block, kv_sorted.shape[1])
    pair_width = kv_sorted.shape[2]

    def one_pair(key_grads, inputs):
        query_rows, row_pos, grad_rows, log_total, pair_index = inputs
        sequence = pair_index // pairs_per_seq
        kv_sequence = kv_sorted[sequence]
        key_blocks = jnp.max(row_pos) // block_rows + 1
        row_count = query_rows.shape[0]

        def pass_terms(block_index):
            masked, key_slice = key_scores(
                query_rows, row_pos, kv_sequence, block_index, block_rows
            )
            weights = jnp.exp(masked - log_total)
            weight_grads = jnp.einsum(
                "rd,kd->rk", grad_rows, key_slice[:, HD:], preferred_element_type=jnp.float32
            )
            return (weights, weight_grads, key_slice)

        def delta_pass(block_index, row_delta):
            weights, weight_grads, unused_slice = pass_terms(block_index)
            return row_delta + jnp.sum(weights * weight_grads, axis=1, keepdims=True)

        row_delta = lax.fori_loop(0, key_blocks, delta_pass, jnp.zeros((row_count, 1), jnp.float32))

        def grad_pass(block_index, carried):
            query_grad, sequence_grads = carried
            weights, weight_grads, key_slice = pass_terms(block_index)
            score_grad = (weights * (weight_grads - row_delta)).astype(jnp.bfloat16)
            query_grad = (
                query_grad
                + jnp.dot(score_grad, key_slice[:, :HD], preferred_element_type=jnp.float32) * 0.125
            )
            key_part = (
                jnp.einsum("rk,rd->kd", score_grad, query_rows, preferred_element_type=jnp.float32)
                * 0.125
            )
            value_part = jnp.einsum(
                "rk,rd->kd",
                weights.astype(jnp.bfloat16),
                grad_rows,
                preferred_element_type=jnp.float32,
            )
            key_start = block_index * block_rows
            previous = lax.dynamic_slice(
                sequence_grads, (sequence, key_start, 0), (1, block_rows, pair_width)
            )
            updated = previous + jnp.concatenate([key_part, value_part], axis=1)[None]
            return (
                query_grad,
                lax.dynamic_update_slice(sequence_grads, updated, (sequence, key_start, 0)),
            )

        query_grad, key_grads = lax.fori_loop(
            0, key_blocks, grad_pass, (jnp.zeros((row_count, HD), jnp.float32), key_grads)
        )
        return (key_grads, query_grad)

    start_grads = jnp.zeros(kv_sorted.shape, jnp.float32)
    key_grads, query_grads = lax.scan(
        one_pair,
        start_grads,
        (query_tiles, tile_pos, grad_tiles, log_totals, jnp.arange(pair_count, dtype=jnp.int32)),
    )
    return (query_grads, key_grads)


def local(
    layer_input,
    block_order,
    ln1_gain,
    ln1_bias,
    w_query,
    b_query,
    w_keyval,
    b_keyval,
    w_attn_out,
    b_attn_out,
    ln2_gain,
    ln2_bias,
    w_fc,
    b_fc,
    w_proj,
    b_proj,
    kv_grad,
    out_grad,
):
    my_rank = lax.axis_index("sp")
    seq_count = block_order.shape[0]
    block_count = block_order.shape[1]
    token_count = layer_input.shape[0]
    shard_len = token_count // seq_count
    block_len = shard_len // 2
    model_width = layer_input.shape[1]
    pair_width = 2 * HD
    pair_count = 2 * seq_count
    input_float = layer_input.astype(jnp.float32)
    first_in, first_hat, first_inv = layer_norm(input_float, ln1_gain, ln1_bias)
    first_low = first_in.astype(jnp.bfloat16)
    query_pre = jnp.dot(first_low, w_query, preferred_element_type=jnp.float32) + b_query
    keyval_pre = jnp.dot(first_low, w_keyval, preferred_element_type=jnp.float32) + b_keyval
    offsets = jnp.arange(block_len, dtype=jnp.int32)
    own_blocks = lax.dynamic_slice_in_dim(block_order, 2 * my_rank, 2, 1)
    own_pos = (own_blocks[:, :, None] * block_len + offsets[None, None, :]).reshape(token_count)
    cosine, sine_table = rotary_tables(own_pos)
    query_use = (
        rotate(query_pre.reshape(token_count, H, HD), cosine, sine_table)
        .reshape(token_count, model_width)
        .astype(jnp.bfloat16)
    )
    key_rot = rotate(keyval_pre[:, None, :HD], cosine, sine_table)[:, 0, :]
    keyval_use = jnp.concatenate([key_rot, keyval_pre[:, HD:]], axis=1).astype(jnp.bfloat16)
    gathered = lax.all_gather(
        keyval_use.reshape(seq_count, shard_len, pair_width), "sp", axis=1, tiled=True
    )
    seq_len = gathered.shape[1]
    block_sorter = jnp.argsort(block_order, axis=1)
    kv_sorted = jnp.take_along_axis(
        gathered.reshape(seq_count, block_count, block_len, pair_width),
        block_sorter[:, :, None, None],
        axis=1,
    ).reshape(seq_count, seq_len, pair_width)
    row_pos = own_pos.reshape(seq_count, shard_len)
    query_rows = query_use.reshape(seq_count, shard_len, model_width)
    query_tiles = query_rows.reshape(pair_count, block_len * H, HD)
    tile_pos = jnp.repeat(row_pos.reshape(pair_count, block_len), H, axis=1)
    head_rows, log_totals = attention_forward(query_tiles, tile_pos, kv_sorted)
    heads_sorted = head_rows.reshape(seq_count, shard_len, model_width).astype(jnp.bfloat16)
    heads_local = heads_sorted.reshape(token_count, model_width)
    attn_branch = jnp.dot(heads_local, w_attn_out, preferred_element_type=jnp.float32) + b_attn_out
    second_in, second_hat, second_inv = layer_norm(input_float, ln2_gain, ln2_bias)
    second_low = second_in.astype(jnp.bfloat16)
    hidden = jnp.dot(second_low, w_fc, preferred_element_type=jnp.float32) + b_fc
    erf_part = 1.0 + lax.erf(hidden * half_root)
    activated = (0.5 * hidden * erf_part).astype(jnp.bfloat16)
    mlp_branch = jnp.dot(activated, w_proj, preferred_element_type=jnp.float32) + b_proj
    layer_out = (input_float + attn_branch + mlp_branch).astype(jnp.bfloat16)
    upstream = out_grad.astype(jnp.float32)
    column_sum = jnp.sum(upstream, axis=0)
    w_proj_grad = jnp.einsum("tf,td->fd", activated, out_grad, preferred_element_type=jnp.float32)
    act_grad = jnp.einsum("td,fd->tf", out_grad, w_proj, preferred_element_type=jnp.float32)
    gelu_slope = 0.5 * erf_part + hidden * jnp.exp(-0.5 * hidden * hidden) * inv_root_tau
    hidden_grad = (act_grad * gelu_slope).astype(jnp.bfloat16)
    w_fc_grad = jnp.einsum("td,tf->df", second_low, hidden_grad, preferred_element_type=jnp.float32)
    b_fc_grad = jnp.sum(hidden_grad.astype(jnp.float32), axis=0)
    second_grad = jnp.einsum("tf,df->td", hidden_grad, w_fc, preferred_element_type=jnp.float32)
    w_attn_out_grad = jnp.einsum(
        "te,td->ed", heads_local, out_grad, preferred_element_type=jnp.float32
    )
    heads_grad = jnp.einsum(
        "td,ed->te", out_grad, w_attn_out, preferred_element_type=jnp.float32
    ).astype(jnp.bfloat16)
    grad_rows = heads_grad.reshape(seq_count, shard_len, model_width)
    grad_tiles = grad_rows.reshape(pair_count, block_len * H, HD)
    query_tile_grads, sorted_kv_grads = attention_backward(
        query_tiles, tile_pos, grad_tiles, log_totals, kv_sorted
    )
    query_rot_rows = query_tile_grads.reshape(seq_count, shard_len, model_width)
    query_rot_grad = query_rot_rows.reshape(token_count, model_width)
    query_grad = (
        rotate_back(query_rot_grad.reshape(token_count, H, HD), cosine, sine_table)
        .reshape(token_count, model_width)
        .astype(jnp.bfloat16)
    )
    stored_kv_grads = jnp.take_along_axis(
        sorted_kv_grads.reshape(seq_count, block_count, block_len, pair_width),
        block_order[:, :, None, None],
        axis=1,
    ).reshape(seq_count, seq_len, pair_width)
    own_kv_grad = lax.psum_scatter(stored_kv_grads, "sp", scatter_dimension=1, tiled=True).reshape(
        token_count, pair_width
    ) + kv_grad.astype(jnp.float32)
    key_pre_grad = rotate_back(own_kv_grad[:, None, :HD], cosine, sine_table)[:, 0, :]
    keyval_grad = jnp.concatenate([key_pre_grad, own_kv_grad[:, HD:]], axis=1).astype(jnp.bfloat16)
    w_query_grad = jnp.einsum(
        "td,te->de", first_low, query_grad, preferred_element_type=jnp.float32
    )
    b_query_grad = jnp.sum(query_grad.astype(jnp.float32), axis=0)
    w_keyval_grad = jnp.einsum(
        "td,te->de", first_low, keyval_grad, preferred_element_type=jnp.float32
    )
    b_keyval_grad = jnp.sum(keyval_grad.astype(jnp.float32), axis=0)
    first_grad = jnp.einsum(
        "te,de->td", query_grad, w_query, preferred_element_type=jnp.float32
    ) + jnp.einsum("te,de->td", keyval_grad, w_keyval, preferred_element_type=jnp.float32)
    first_back = norm_back(first_grad, first_hat, first_inv, ln1_gain)
    second_back = norm_back(second_grad, second_hat, second_inv, ln2_gain)
    input_grad = upstream + first_back + second_back
    (
        ln1_gain_grad,
        ln1_bias_grad,
        b_query_total,
        b_keyval_total,
        bias_out_total,
        ln2_gain_grad,
        ln2_bias_grad,
        b_fc_total,
    ) = lax.psum(
        (
            jnp.sum(first_grad * first_hat, axis=0),
            jnp.sum(first_grad, axis=0),
            b_query_grad,
            b_keyval_grad,
            column_sum,
            jnp.sum(second_grad * second_hat, axis=0),
            jnp.sum(second_grad, axis=0),
            b_fc_grad,
        ),
        ("grp", "sp"),
    )
    query_share, keyval_share, out_share, fc_share, proj_share = (
        lax.psum_scatter(w_query_grad, "sp", scatter_dimension=0, tiled=True),
        lax.psum_scatter(w_keyval_grad, "sp", scatter_dimension=0, tiled=True),
        lax.psum_scatter(w_attn_out_grad, "sp", scatter_dimension=0, tiled=True),
        lax.psum_scatter(w_fc_grad, "sp", scatter_dimension=0, tiled=True),
        lax.psum_scatter(w_proj_grad, "sp", scatter_dimension=0, tiled=True),
    )
    query_total, keyval_total, out_total, fc_total, proj_total = lax.psum(
        (query_share, keyval_share, out_share, fc_share, proj_share), "grp"
    )
    return (
        layer_out,
        input_grad,
        ln1_gain_grad,
        ln1_bias_grad,
        query_total,
        b_query_total,
        keyval_total,
        b_keyval_total,
        out_total,
        bias_out_total,
        ln2_gain_grad,
        ln2_bias_grad,
        fc_total,
        b_fc_total,
        proj_total,
        bias_out_total,
    )


def solution(mesh):
    placed = (
        P(("grp", "sp"), None),
        P("grp", None),
        P(),
        P(),
        P(),
        P(),
        P(),
        P(),
        P(),
        P(),
        P(),
        P(),
        P(),
        P(),
        P(),
        P(),
        P(("grp", "sp"), None),
        P(("grp", "sp"), None),
    )
    def step(*args):
        if fits(mesh, args):
            body = functools.partial(fused_local, mesh.shape["grp"], mesh.shape["sp"])
        else:
            body = local
        return spread(body)(*args)

    def spread(body):
        return jax.shard_map(
            body,
            mesh=mesh,
            in_specs=placed,
            out_specs=(
                P(("grp", "sp"), None),
                P(("grp", "sp"), None),
                P(),
                P(),
                P("sp", None),
                P(),
                P("sp", None),
                P(),
                P("sp", None),
                P(),
                P(),
                P(),
                P("sp", None),
                P(),
                P("sp", None),
                P(),
            ),
            check_vma=False,
        )

    return step
```
